8 devices in a mesh: dp: 1 (over z), sp: 8 (over y, x, core).
Axes of the slice: x: 2, y: 2, z: 1, core: 2. Of those that a mesh axis runs over, the one named last changes fastest.
Arguments:
- hidden: bfloat16 [32, 7168], P('dp')
- ckv_cache: bfloat16 [32, 16384, 512], P('dp', 'sp')
- kpe_cache: bfloat16 [32, 16384, 64], P('dp', 'sp')
- cache_len: int32 [32], P('dp')
- w_dq: bfloat16 [7168, 1536], replicated
- q_gain: bfloat16 [1536], replicated
- w_uq: bfloat16 [1536, 12288], replicated
- w_dkv: bfloat16 [7168, 576], replicated
- kv_gain: bfloat16 [512], replicated
- w_uk: bfloat16 [64, 128, 512], replicated
- w_uv: bfloat16 [64, 128, 512], replicated
- w_out: bfloat16 [8192, 7168], replicated
Outputs:
- output 1: bfloat16 [32, 7168], P('dp')
- output 2: bfloat16 [32, 16384, 512], P('dp', 'sp')
- output 3: bfloat16 [32, 16384, 64], P('dp', 'sp')
- output 4: bfloat16 [32, 576], P('dp')
All inputs are finite; a program needn't handle non-finite values.
Results may differ from the reference program's by a relative error of at most 0.0112965.
Values sent between devices are 32-bit elements.
A program may use at most 1.5 GiB of HBM per device.

```python
import jax
import jax.numpy as jnp
from jax import lax

D_MODEL = 7168
N_HEADS = 64
Q_LORA = 1536
KV_LORA = 512
ROPE_DIM = 64
NOPE_DIM = 128
V_DIM = 128
N_SEQS = 32
SHARD_LEN = 2048
SEQ_LEN = 16384
ROPE_THETA = 10000
N_ANCHORS = 17
EPS = 1e-6
QK_DIM = NOPE_DIM + ROPE_DIM


def rms_norm(vector, norm_gain):
    mean_sq = jnp.mean(vector * vector, axis=-1, keepdims=True)
    return vector * lax.rsqrt(mean_sq + EPS) * norm_gain.astype(jnp.float32)


def rope_tables(cache_len):
    inv_freq = jnp.power(float(ROPE_THETA), -2.0 * jnp.arange(ROPE_DIM // 2, dtype=jnp.float32) / ROPE_DIM)
    rope_angle = cache_len.astype(jnp.float32)[:, None] * inv_freq[None, :]
    return jnp.cos(rope_angle), jnp.sin(rope_angle)


def rotate(vector, cos_t, sin_t):
    half_dim = vector.shape[-1] // 2
    first_half = vector[..., :half_dim]
    second_half = vector[..., half_dim:]
    return jnp.concatenate([first_half * cos_t - second_half * sin_t, second_half * cos_t + first_half * sin_t], axis=-1)


def setup_inputs(seed: int = 0, part: int = 0) -> dict:
    part_key = jax.random.fold_in(jax.random.key(seed), part)
    hid_key, cache_key, len_key = jax.random.split(part_key, 3)
    shared = jax.random.split(jax.random.key(seed + 1), 8)
    pos_frac = jnp.arange(SEQ_LEN, dtype=jnp.float32) * ((N_ANCHORS - 1) / (SEQ_LEN - 1))
    interp = jnp.maximum(0.0, 1.0 - jnp.abs(pos_frac[:, None] - jnp.arange(N_ANCHORS, dtype=jnp.float32)[None, :]))

    def draw_seq(seq_idx):
        noise_key, anchor_key, pe_key = jax.random.split(jax.random.fold_in(cache_key, seq_idx), 3)
        base_noise = jax.random.normal(noise_key, (SEQ_LEN, KV_LORA), jnp.float32)
        anchors = jax.random.normal(anchor_key, (N_ANCHORS, KV_LORA), jnp.float32)
        latent = 0.8 * base_noise + 0.6 * jnp.dot(interp, anchors)
        rope_part = 1.5 * jax.random.normal(pe_key, (SEQ_LEN, ROPE_DIM), jnp.float32)
        return latent.astype(jnp.bfloat16), rope_part.astype(jnp.bfloat16)

    ckv_cache, kpe_cache = lax.map(draw_seq, jnp.arange(N_SEQS))
    long_key, short_key = jax.random.split(len_key)
    long_len = SEQ_LEN - 1 - jax.random.randint(long_key, (N_SEQS,), 0, SHARD_LEN)
    short_len = jax.random.randint(short_key, (N_SEQS,), SEQ_LEN // 2, SEQ_LEN)
    cache_len = jnp.where(jnp.arange(N_SEQS) % 2 == 0, long_len, short_len).astype(jnp.int32)

    def normal_weight(key_in, arr_shape, fan_in, gain_mul):
        return (jax.random.normal(key_in, arr_shape, jnp.float32) * (gain_mul * fan_in ** -0.5)).astype(jnp.bfloat16)

    hidden = jax.random.normal(hid_key, (N_SEQS, D_MODEL), jnp.float32).astype(jnp.bfloat16)
    return {
        'hidden': hidden,
        'ckv_cache': ckv_cache,
        'kpe_cache': kpe_cache,
        'cache_len': cache_len,
        'w_dq': normal_weight(shared[0], (D_MODEL, Q_LORA), D_MODEL, 1.0),
        'q_gain': jax.random.uniform(shared[1], (Q_LORA,), jnp.float32, minval=0.5, maxval=1.5).astype(jnp.bfloat16),
        'w_uq': normal_weight(shared[2], (Q_LORA, N_HEADS * QK_DIM), Q_LORA, 1.0),
        'w_dkv': normal_weight(shared[3], (D_MODEL, KV_LORA + ROPE_DIM), D_MODEL, 1.0),
        'kv_gain': jax.random.uniform(shared[4], (KV_LORA,), jnp.float32, minval=0.5, maxval=1.5).astype(jnp.bfloat16),
        'w_uk': normal_weight(shared[5], (N_HEADS, NOPE_DIM, KV_LORA), NOPE_DIM, 1.0),
        'w_uv': normal_weight(shared[6], (N_HEADS, V_DIM, KV_LORA), KV_LORA, 5.0),
        'w_out': normal_weight(shared[7], (N_HEADS * V_DIM, D_MODEL), N_HEADS * V_DIM, 1.0),
    }


def reference(hidden, ckv_cache, kpe_cache, cache_len, w_dq, q_gain, w_uq, w_dkv, kv_gain, w_uk, w_uv, w_out):
    score_scale = QK_DIM ** -0.5
    cq_raw = jnp.dot(hidden, w_dq, preferred_element_type=jnp.float32)
    c_q = rms_norm(cq_raw, q_gain).astype(jnp.bfloat16)
    q_full = jnp.dot(c_q, w_uq, preferred_element_type=jnp.float32).astype(jnp.bfloat16)
    q_full = q_full.reshape(N_SEQS, N_HEADS, QK_DIM)
    cos_t, sin_t = rope_tables(cache_len)
    q_pe = rotate(q_full[:, :, NOPE_DIM:].astype(jnp.float32), cos_t[:, None, :], sin_t[:, None, :]).astype(jnp.bfloat16)
    q_lat = jnp.einsum('bhn,hnc->bhc', q_full[:, :, :NOPE_DIM].astype(jnp.float32), w_uk.astype(jnp.float32)).astype(jnp.bfloat16)
    kv_raw = jnp.dot(hidden, w_dkv, preferred_element_type=jnp.float32)
    c_kv = rms_norm(kv_raw[:, :KV_LORA], kv_gain).astype(jnp.bfloat16)
    k_pe = rotate(kv_raw[:, KV_LORA:], cos_t, sin_t).astype(jnp.bfloat16)
    positions = jnp.arange(SEQ_LEN, dtype=jnp.int32)
    new_slot = (positions[None, :] == cache_len[:, None])[:, :, None]
    ckv_out = jnp.where(new_slot, c_kv[:, None, :], ckv_cache)
    kpe_out = jnp.where(new_slot, k_pe[:, None, :], kpe_cache)

    def attend_one(seq_args):
        q_lat_b, q_pe_b, ckv_b, kpe_b, len_b = seq_args
        ckv_f = ckv_b.astype(jnp.float32)
        scores = jnp.einsum('hc,tc->ht', q_lat_b.astype(jnp.float32), ckv_f) + jnp.einsum('hr,tr->ht', q_pe_b.astype(jnp.float32), kpe_b.astype(jnp.float32))
        scores = jnp.where(positions[None, :] <= len_b, scores * score_scale, -jnp.inf)
        attn_probs = jax.nn.softmax(scores, axis=-1)
        return jnp.einsum('ht,tc->hc', attn_probs, ckv_f)

    o_lat = lax.map(attend_one, (q_lat, q_pe, ckv_out, kpe_out, cache_len)).astype(jnp.bfloat16)
    o_heads = jnp.einsum('bhc,hvc->bhv', o_lat.astype(jnp.float32), w_uv.astype(jnp.float32)).astype(jnp.bfloat16)
    out = jnp.dot(o_heads.reshape(N_SEQS, N_HEADS * V_DIM), w_out, preferred_element_type=jnp.float32).astype(jnp.bfloat16)
    kv_new = jnp.concatenate([c_kv, k_pe], axis=-1)
    return (out, ckv_out, kpe_out, kv_new)
```

```python
import functools

import jax
import jax.numpy as jnp
from jax import lax
from jax.experimental import pallas as pl
from jax.experimental.pallas import tpu as pltpu
from jax.sharding import PartitionSpec as P

EPS = 1e-6
ROPE_THETA = 10000.0
NEG_FILL = -1e30
MESH = pl.DeviceIdType.MESH
VMEM = pl.BlockSpec(memory_space=pltpu.VMEM)
SMEM = pl.BlockSpec(memory_space=pltpu.SMEM)
ANY = pl.BlockSpec(memory_space=pl.ANY)


def rms_norm(vector, norm_gain):
    mean_sq = jnp.mean(vector * vector, axis=-1, keepdims=True)
    return vector * lax.rsqrt(mean_sq + EPS) * norm_gain.astype(jnp.float32)


def rope_tables(cache_len, rope_dim):
    inv_freq = jnp.power(ROPE_THETA, -2.0 * jnp.arange(rope_dim // 2, dtype=jnp.float32) / rope_dim)
    rope_angle = cache_len.astype(jnp.float32)[:, None] * inv_freq[None, :]
    return jnp.cos(rope_angle), jnp.sin(rope_angle)


def rotate(vector, cos_t, sin_t):
    half_dim = vector.shape[-1] // 2
    first_half = vector[..., :half_dim]
    second_half = vector[..., half_dim:]
    return jnp.concatenate([first_half * cos_t - second_half * sin_t, second_half * cos_t + first_half * sin_t], axis=-1)


def project_token(hidden, cache_len, w_dq, q_gain, w_uq, w_dkv, kv_gain, w_uk):
    n_seqs = hidden.shape[0]
    n_heads, nope_dim, value_a7 = w_uk.shape
    qk_dim = w_uq.shape[1] // n_heads
    cq_raw = jnp.dot(hidden, w_dq, preferred_element_type=jnp.float32)
    c_q = rms_norm(cq_raw, q_gain).astype(jnp.bfloat16)
    q_full = jnp.dot(c_q, w_uq, preferred_element_type=jnp.float32).astype(jnp.bfloat16)
    q_full = q_full.reshape(n_seqs, n_heads, qk_dim)
    cos_t, sin_t = rope_tables(cache_len, qk_dim - nope_dim)
    q_pe = rotate(q_full[:, :, nope_dim:].astype(jnp.float32), cos_t[:, None, :], sin_t[:, None, :]).astype(jnp.bfloat16)
    q_lat = jnp.einsum('bhn,hnc->bhc', q_full[:, :, :nope_dim], w_uk, preferred_element_type=jnp.float32).astype(jnp.bfloat16)
    kv_raw = jnp.dot(hidden, w_dkv, preferred_element_type=jnp.float32)
    c_kv = rms_norm(kv_raw[:, :value_a7], kv_gain)
    k_pe = rotate(kv_raw[:, value_a7:], cos_t, sin_t)
    kv_new = jnp.concatenate([c_kv, k_pe], axis=-1).astype(jnp.bfloat16)
    return q_lat, q_pe, kv_new


def attend_kernel(cfg, len_ref, qlat_ref, qpe_ref, ckvn_ref, kpen_ref, ckv_hbm, kpe_hbm, cout_hbm, kout_hbm, o_hbm,
                  cbuf, kbuf, obuf, stats, isem, osem, psem):
    n_seqs, shard_len = ckv_hbm.shape[0], ckv_hbm.shape[1]
    n_heads = stats.shape[0]
    n_buf, lag, chunk = cfg["n_buf"], cfg["lag"], cfg["chunk"]
    base = lax.axis_index('sp') * shard_len

    def copies_in(b, slot):
        return (pltpu.make_async_copy(ckv_hbm.at[b], cbuf.at[slot], isem.at[slot, 0]),
                pltpu.make_async_copy(kpe_hbm.at[b], kbuf.at[slot], isem.at[slot, 1]))

    def copies_out(b, slot):
        return (pltpu.make_async_copy(cbuf.at[slot], cout_hbm.at[b], osem.at[slot, 0]),
                pltpu.make_async_copy(kbuf.at[slot], kout_hbm.at[b], osem.at[slot, 1]))

    def copy_terms(b, side):
        return pltpu.make_async_copy(obuf.at[side], o_hbm.at[:, b], psem.at[side])

    for i in range(n_buf - lag):
        for c in copies_in(i, i):
            c.start()
    stats[...] = jnp.zeros_like(stats)

    def step(b, carry):
        slot = lax.rem(b, n_buf)

        @pl.when(b >= lag)
        def _():
            for c in copies_out(b - lag, lax.rem(b - lag + n_buf, n_buf)):
                c.wait()

        ahead = b - lag + n_buf

        @pl.when(ahead < n_seqs)
        def _():
            for c in copies_in(ahead, lax.rem(ahead, n_buf)):
                c.start()

        for c in copies_in(b, slot):
            c.wait()
        last = len_ref[b] - base

        @pl.when((last >= 0) & (last < shard_len))
        def _():
            r0 = pl.multiple_of((last // 16) * 16, 16)
            rows = cbuf[slot, pl.ds(r0, 16), :].astype(jnp.float32)
            row = lax.broadcasted_iota(jnp.int32, rows.shape, 0)
            cbuf[slot, pl.ds(r0, 16), :] = jnp.where(row == last - r0, ckvn_ref[b].astype(jnp.float32), rows).astype(cbuf.dtype)
            c0 = pl.multiple_of((last // 128) * 128, 128)
            cols = kbuf[slot, :, pl.ds(c0, 128)].astype(jnp.float32)
            lane = lax.broadcasted_iota(jnp.int32, cols.shape, 1)
            fresh = jnp.sum(jnp.where(lane == b, kpen_ref[...].astype(jnp.float32), 0.0), axis=1, keepdims=True)
            kbuf[slot, :, pl.ds(c0, 128)] = jnp.where(lane == last - c0, fresh, cols).astype(kbuf.dtype)

        q_lat, q_pe = qlat_ref[b], qpe_ref[b]
        scores = []
        for t in range(0, shard_len, chunk):
            s = lax.dot_general(q_lat, cbuf[slot, t:t + chunk, :], (((1,), (1,)), ((), ())), preferred_element_type=jnp.float32)
            s = s + jnp.dot(q_pe, kbuf[slot, :, t:t + chunk], preferred_element_type=jnp.float32)
            pos = lax.broadcasted_iota(jnp.int32, (1, chunk), 1) + t
            scores.append(jnp.where(pos <= last, s * cfg["scale"], NEG_FILL))
        peak = functools.reduce(jnp.maximum, [jnp.max(s, axis=1, keepdims=True) for s in scores])
        denom = jnp.zeros_like(peak)
        lat_sum = None
        for k, t in enumerate(range(0, shard_len, chunk)):
            w = jnp.exp(scores[k] - peak)
            denom = denom + jnp.sum(w, axis=1, keepdims=True)
            term = jnp.dot(w.astype(jnp.bfloat16), cbuf[slot, t:t + chunk, :], preferred_element_type=jnp.float32)
            lat_sum = term if lat_sum is None else lat_sum + term
        for c in copies_out(b, slot):
            c.start()
        side = lax.rem(b, 2)

        @pl.when(b >= 2)
        def _():
            copy_terms(b - 2, side).wait()

        obuf[side] = lat_sum.reshape(obuf.shape[1:])
        lane = lax.broadcasted_iota(jnp.int32, stats.shape, 1)
        stats[...] = jnp.where(lane == b, peak, jnp.where(lane == b + 64, denom, stats[...]))
        copy_terms(b, side).start()
        return carry

    lax.fori_loop(0, n_seqs, step, 0)
    for i in range(n_seqs - 2, n_seqs):
        copy_terms(i, i % 2).wait()
    obuf[0, :, :, 0:128] = stats[...].reshape(obuf.shape[1], obuf.shape[2], 128)
    copy_terms(n_seqs, 0).start()
    for i in range(n_seqs - lag, n_seqs):
        for c in copies_out(i, i % n_buf):
            c.wait()
    copy_terms(n_seqs, 0).wait()


def attend(q_lat, q_pe, kv_new, cache_len, ckv_blk, kpe_blk_t, n_dev):
    n_seqs, shard_len, lat_dim = ckv_blk.shape
    rope_dim = kpe_blk_t.shape[1]
    n_heads = q_lat.shape[1]
    cfg = dict(n_buf=8, lag=3, chunk=512, scale=(128 + rope_dim) ** -0.5)
    ckv_new = kv_new[:, :lat_dim].reshape(n_seqs, 1, lat_dim)
    kpe_new_t = jnp.pad(kv_new[:, lat_dim:].T, ((0, 0), (0, 128 - n_seqs)))
    terms_shape = (n_dev, n_seqs + 1, n_heads // n_dev, lat_dim)
    return pl.pallas_call(
        functools.partial(attend_kernel, cfg),
        out_shape=(
            jax.ShapeDtypeStruct(ckv_blk.shape, ckv_blk.dtype),
            jax.ShapeDtypeStruct(kpe_blk_t.shape, kpe_blk_t.dtype),
            jax.ShapeDtypeStruct(terms_shape, jnp.float32),
        ),
        in_specs=[SMEM, VMEM, VMEM, VMEM, VMEM, ANY, ANY],
        out_specs=(ANY, ANY, ANY),
        scratch_shapes=[
            pltpu.VMEM((cfg["n_buf"], shard_len, lat_dim), ckv_blk.dtype),
            pltpu.VMEM((cfg["n_buf"], rope_dim, shard_len), kpe_blk_t.dtype),
            pltpu.VMEM((2, n_dev, n_heads // n_dev, lat_dim), jnp.float32),
            pltpu.VMEM((n_heads, 128), jnp.float32),
            pltpu.SemaphoreType.DMA((cfg["n_buf"], 2)),
            pltpu.SemaphoreType.DMA((cfg["n_buf"], 2)),
            pltpu.SemaphoreType.DMA((2,)),
        ],
        compiler_params=pltpu.CompilerParams(vmem_limit_bytes=56 * 1024 * 1024),
        name="attend",
    )(cache_len, q_lat, q_pe, ckv_new, kpe_new_t, ckv_blk, kpe_blk_t)


def finish_kernel(terms, w_uv, w_out, out_ref, orecv, uv, wo, merged, oheads, psend, precv, isend, irecv, fin, agr, agp,
                  lsem, o_ss, o_rs, p_ss, p_rs, i_ss, i_rs, a_ss, a_rs, f_ss, f_rs):
    n_seqs, width = fin.shape
    heads = uv.shape[0]
    depth = wo.shape[0]
    me = lax.axis_index('sp')
    y, x, c = me // 4, (me // 2) % 2, me % 2

    def device(q, jc):
        return ((y + q // 2) % 2) * 4 + ((x + q % 2) % 2) * 2 + (c + jc) % 2

    def send(src, dst, ss, rs, dev):
        return pltpu.make_async_remote_copy(src_ref=src, dst_ref=dst, send_sem=ss, recv_sem=rs, device_id={'sp': dev}, device_id_type=MESH)

    load_uv = pltpu.make_async_copy(w_uv.at[pl.ds(me * heads, heads)], uv, lsem.at[0])
    load_wo = pltpu.make_async_copy(w_out.at[pl.ds(me * depth, depth)], wo, lsem.at[1])
    load_own = pltpu.make_async_copy(terms.at[me], orecv.at[0], lsem.at[2])
    load_own.start()
    load_uv.start()
    load_wo.start()

    others = [(q, jc) for q in (3, 1, 2, 0) for jc in (0, 1) if (q, jc) != (0, 0)]
    barrier = pltpu.get_barrier_semaphore()
    for q, jc in others:
        pl.semaphore_signal(barrier, inc=1, device_id={'sp': device(q, jc)}, device_id_type=MESH)
    pl.semaphore_wait(barrier, len(others))

    o_sends = []
    for q, jc in others:
        j = q * 2 + jc
        o_sends.append(send(terms.at[device(q, jc)], orecv.at[j], o_ss.at[j], o_rs.at[j], device(q, jc)))
        o_sends[-1].start()
    load_own.wait()
    for s in o_sends:
        s.wait_recv()
    stats = [orecv[j, n_seqs, :, 0:128] for j in range(8)]
    peak = functools.reduce(jnp.maximum, stats)
    factors = [jnp.exp(s - peak) for s in stats]
    denoms = [pltpu.roll(s, 64, 1) for s in stats]
    total = functools.reduce(jnp.add, [f * d for f, d in zip(factors, denoms)])
    factors = [f / total for f in factors]
    for b in range(n_seqs):
        acc = None
        for j in range(8):
            t = factors[j][:, b:b + 1] * orecv[j, b]
            acc = t if acc is None else acc + t
        for k in range(merged.shape[0]):
            merged[k, b * heads:(b + 1) * heads, :] = acc[:, k * 128:(k + 1) * 128]
    load_uv.wait()
    for h in range(heads):
        o_lat = jnp.concatenate([merged[k, pl.ds(h, n_seqs, stride=heads), :] for k in range(merged.shape[0])], axis=1).astype(jnp.bfloat16)
        o_h = lax.dot_general(o_lat, uv[h], (((1,), (1,)), ((), ())), preferred_element_type=jnp.float32)
        oheads[:, h * o_h.shape[1]:(h + 1) * o_h.shape[1]] = o_h.astype(jnp.bfloat16)
    load_wo.wait()

    def partial_out(dev):
        cols = pl.ds(pl.multiple_of(dev * width, 128), width)
        return jnp.dot(oheads[...], wo[:, cols], preferred_element_type=jnp.float32)

    waiting = []
    p_sends, i_sends = {}, []
    for q in (3, 1, 2, 0):
        psend[q] = partial_out(device(q, 1))
        p_sends[q] = send(psend.at[q], precv.at[q], p_ss.at[q], p_rs.at[q], device(0, 1))
        for w in waiting:
            w.start()
        waiting = [p_sends[q]]
    mine = None
    for q in (3, 1, 2, 0):
        part = partial_out(device(q, 0))
        for w in waiting:
            w.start()
        waiting = []
        p_sends[q].wait_recv()
        if q:
            isend[q - 1] = part + precv[q]
            i_sends.append(send(isend.at[q - 1], irecv.at[q - 1], i_ss.at[q - 1], i_rs.at[q - 1], device(q, 0)))
            waiting = [i_sends[-1]]
        else:
            mine = part + precv[0]
    for s in i_sends:
        s.wait_recv()
    result = mine + irecv[0] + irecv[1] + irecv[2]
    fin[...] = result
    out_ref[:, pl.ds(pl.multiple_of(me * width, 128), width)] = result.astype(out_ref.dtype)

    a_sends = {q: send(fin, agr.at[q - 1], a_ss.at[q - 1], a_rs.at[q - 1], device(q, 0)) for q in (3, 1, 2)}
    f_sends = {0: send(fin, agp.at[0], f_ss.at[0], f_rs.at[0], device(0, 1))}
    for q in (3, 1, 2):
        a_sends[q].start()
    f_sends[0].start()
    for q in (1, 2, 3):
        f_sends[q] = send(agr.at[q - 1], agp.at[q], f_ss.at[q], f_rs.at[q], device(0, 1))
        a_sends[q].wait_recv()
        f_sends[q].start()
        out_ref[:, pl.ds(pl.multiple_of(device(q, 0) * width, 128), width)] = agr[q - 1].astype(out_ref.dtype)
    for q in range(4):
        f_sends[q].wait_recv()
        out_ref[:, pl.ds(pl.multiple_of(device(q, 1) * width, 128), width)] = agp[q].astype(out_ref.dtype)
    for s in o_sends + list(p_sends.values()) + i_sends + list(a_sends.values()) + list(f_sends.values()):
        s.wait_send()


def finish(terms, w_uv, w_out):
    n_dev, rows, heads, lat_dim = terms.shape
    n_seqs = rows - 1
    d_model = w_out.shape[1]
    depth = w_out.shape[0] // n_dev
    width = d_model // n_dev
    f32 = jnp.float32
    return pl.pallas_call(
        finish_kernel,
        out_shape=jax.ShapeDtypeStruct((n_seqs, d_model), jnp.bfloat16),
        in_specs=[ANY, ANY, ANY],
        out_specs=VMEM,
        scratch_shapes=[
            pltpu.VMEM((n_dev, rows, heads, lat_dim), f32),
            pltpu.VMEM((heads,) + w_uv.shape[1:], w_uv.dtype),
            pltpu.VMEM((depth, d_model), w_out.dtype),
            pltpu.VMEM((lat_dim // 128, n_seqs * heads, 128), f32),
            pltpu.VMEM((n_seqs, depth), jnp.bfloat16),
            pltpu.VMEM((4, n_seqs, width), f32),
            pltpu.VMEM((4, n_seqs, width), f32),
            pltpu.VMEM((3, n_seqs, width), f32),
            pltpu.VMEM((3, n_seqs, width), f32),
            pltpu.VMEM((n_seqs, width), f32),
            pltpu.VMEM((3, n_seqs, width), f32),
            pltpu.VMEM((4, n_seqs, width), f32),
            pltpu.SemaphoreType.DMA((3,)),
            pltpu.SemaphoreType.DMA((8,)),
            pltpu.SemaphoreType.DMA((8,)),
            pltpu.SemaphoreType.DMA((4,)),
            pltpu.SemaphoreType.DMA((4,)),
            pltpu.SemaphoreType.DMA((3,)),
            pltpu.SemaphoreType.DMA((3,)),
            pltpu.SemaphoreType.DMA((3,)),
            pltpu.SemaphoreType.DMA((3,)),
            pltpu.SemaphoreType.DMA((4,)),
            pltpu.SemaphoreType.DMA((4,)),
        ],
        compiler_params=pltpu.CompilerParams(collective_id=0, has_side_effects=True, vmem_limit_bytes=56 * 1024 * 1024),
        name="finish",
    )(terms, w_uv, w_out)


def solution(mesh):
    n_dev = mesh.shape['sp']

    def local_step(hidden, ckv_blk, kpe_blk, cache_len, w_dq, q_gain, w_uq, w_dkv, kv_gain, w_uk, w_uv, w_out):
        q_lat, q_pe, kv_new = project_token(hidden, cache_len, w_dq, q_gain, w_uq, w_dkv, kv_gain, w_uk)
        ckv_out, kpe_out_t, terms = attend(q_lat, q_pe, kv_new, cache_len, ckv_blk, jnp.swapaxes(kpe_blk, 1, 2), n_dev)
        out = finish(terms, w_uv, w_out)
        return out, ckv_out, jnp.swapaxes(kpe_out_t, 1, 2), kv_new

    cache_spec = P('dp', 'sp', None)
    return jax.shard_map(local_step, mesh=mesh, in_specs=(P('dp', None), cache_spec, cache_spec, P('dp'), P(), P(), P(), P(), P(), P(), P(), P()), out_specs=(P('dp', None), cache_spec, cache_spec, P('dp', None)), check_vma=False)
```

```python
import functools

import jax
import jax.numpy as jnp
from jax import lax
from jax.experimental import pallas as pl
from jax.experimental.pallas import tpu as pltpu
from jax.sharding import PartitionSpec as P

EPS = 1e-6
ROPE_THETA = 10000.0
NEG_FILL = -1e30
MESH = pl.DeviceIdType.MESH
VMEM = pl.BlockSpec(memory_space=pltpu.VMEM)
SMEM = pl.BlockSpec(memory_space=pltpu.SMEM)
ANY = pl.BlockSpec(memory_space=pl.ANY)


def rope_tables(cache_len, rope_dim):
    inv_freq = jnp.power(ROPE_THETA, -2.0 * jnp.arange(rope_dim // 2, dtype=jnp.float32) / rope_dim)
    rope_angle = cache_len.astype(jnp.float32)[:, None] * inv_freq[None, :]
    return jnp.cos(rope_angle), jnp.sin(rope_angle)


def project_kernel(cfg, hidden, w_dq, w_dkv_t, w_uq, w_uk, q_gain, kv_gain, cos_t, sin_t, q_out, kvn_out, kv_new_out,
                   dq, dkv, uq, uk, halves, q_mine, q_theirs, turn, dq_sem, dkv_sem, uq_sem, uk_sem, h_ss, h_rs, q_ss, q_rs):
    n_seqs = hidden.shape[0]
    n_k, k_rows, dq_cols = dq.shape
    n_blk, _, blk = uq.shape
    dkv_cols = dkv.shape[0]
    n_kt = cfg["n_kt"]
    k_tile = dkv.shape[1] // n_kt
    lat_dim = cfg["lat_dim"]
    nope_dim = uk.shape[1]
    heads = uk.shape[0]
    half_heads = heads // 2
    group = cfg["group"]
    me = lax.axis_index('sp')
    c = me % 2
    partner = me - c + (1 - c)
    f32 = jnp.float32

    def load_dq(k):
        return pltpu.make_async_copy(w_dq.at[pl.ds(k * k_rows, k_rows), pl.ds(pl.multiple_of(c * dq_cols, 128), dq_cols)], dq.at[k], dq_sem.at[k])

    def load_dkv(k):
        return pltpu.make_async_copy(w_dkv_t.at[pl.ds(pl.multiple_of(c * (lat_dim // 2), 16), dkv_cols), pl.ds(k * k_tile, k_tile)], dkv.at[:, pl.ds(k * k_tile, k_tile)], dkv_sem.at[k])

    def load_uq(k):
        return pltpu.make_async_copy(w_uq.at[:, pl.ds(pl.multiple_of((c * n_blk + k) * blk, 128), blk)], uq.at[k], uq_sem.at[k])

    def load_uk(k):
        first = (c * half_heads + k * group) % heads
        return pltpu.make_async_copy(w_uk.at[pl.ds(first, group)], uk.at[pl.ds(k * group, group)], uk_sem.at[k])

    n_grp = heads // group
    per_kt = n_k // n_kt
    for k in range(n_k):
        load_dq(k).start()
        if k % per_kt == 0:
            load_dkv(k // per_kt).start()
    per_grp = n_blk // (n_grp // 2)
    for g in range(n_grp // 2):
        for k in range(per_grp):
            load_uq(g * per_grp + k).start()
        load_uk(g).start()
    for g in range(n_grp // 2, n_grp):
        load_uk(g).start()

    barrier = pltpu.get_barrier_semaphore()
    pl.semaphore_signal(barrier, inc=1, device_id={'sp': partner}, device_id_type=MESH)
    pl.semaphore_wait(barrier, 1)

    acc_q = jnp.zeros((n_seqs, dq_cols), f32)
    acc_kv = jnp.zeros((n_seqs, dkv_cols), f32)
    for k in range(n_k):
        load_dq(k).wait()
        acc_q = acc_q + jnp.dot(hidden[:, k * k_rows:(k + 1) * k_rows], dq[k], preferred_element_type=f32)
        if k % per_kt == per_kt - 1:
            t = k // per_kt
            load_dkv(t).wait()
            cols = slice(t * k_tile, (t + 1) * k_tile)
            acc_kv = acc_kv + lax.dot_general(hidden[:, cols], dkv[:, cols], (((1,), (1,)), ((), ())), preferred_element_type=f32)
    halves[c, :, dq_cols + lat_dim // 2:] = jnp.zeros((n_seqs, 128), f32)
    halves[c, :, :dq_cols] = acc_q
    halves[c, :, dq_cols:dq_cols + dkv_cols] = acc_kv
    swap = pltpu.make_async_remote_copy(src_ref=halves.at[c], dst_ref=halves.at[c], send_sem=h_ss, recv_sem=h_rs, device_id={'sp': partner}, device_id_type=MESH)
    swap.start()
    swap.wait_recv()

    lo, hi = halves[0], halves[1]
    raw_q = [lo[:, :dq_cols], hi[:, :dq_cols]]
    mean_sq = sum(jnp.sum(r * r, axis=1, keepdims=True) for r in raw_q) / (2 * dq_cols)
    inv = lax.rsqrt(mean_sq + EPS)
    c_q = jnp.concatenate([r * inv * q_gain[:, i * dq_cols:(i + 1) * dq_cols].astype(f32) for i, r in enumerate(raw_q)], axis=1).astype(jnp.bfloat16)

    lane = lax.broadcasted_iota(jnp.int32, (n_seqs, 128), 1)

    def rotate_pair(pair):
        other = jnp.where(lane % 64 < 32, pltpu.roll(pair, 96, 1), pltpu.roll(pair, 32, 1))
        return pair * cos_t[...] + other * sin_t[...]

    def emit(q_blk, k, at):
        for p in range(blk // 384):
            t0, t1, t2 = (q_blk[:, p * 384 + i * 128:p * 384 + (i + 1) * 128] for i in range(3))
            odd = jnp.where(lane < 64, pltpu.roll(t1, 64, 1), pltpu.roll(t2, 64, 1))
            pe = rotate_pair(jnp.where(lane < 64, t1, t2))
            for i, (nope, rope) in enumerate(((t0, pe), (odd, pltpu.roll(pe, 64, 1)))):
                h = k * (blk // 192) + p * 2 + i
                lat = jnp.dot(nope.astype(jnp.bfloat16), uk[at + h], preferred_element_type=f32)
                row = (h % group) * n_seqs
                for j in range(lat_dim // 128):
                    turn[j, row:row + n_seqs, :] = lat[:, j * 128:(j + 1) * 128]
                turn[lat_dim // 128, row:row + n_seqs, :] = rope

    def flush(first):
        rows = pl.ds(pl.multiple_of(first, group), group)
        for b in range(n_seqs):
            for j in range(lat_dim // 128 + 1):
                q_out[b, rows, j * 128:(j + 1) * 128] = turn[j, pl.ds(b, group, stride=n_seqs), :].astype(q_out.dtype)

    sends = []
    for k in range(n_blk):
        load_uq(k).wait()
        q_blk = jnp.dot(c_q, uq[k], preferred_element_type=f32).astype(jnp.bfloat16).astype(f32)
        q_mine[k] = q_blk
        sends.append(pltpu.make_async_remote_copy(src_ref=q_mine.at[k], dst_ref=q_theirs.at[k], send_sem=q_ss.at[k], recv_sem=q_rs.at[k], device_id={'sp': partner}, device_id_type=MESH))
        if k % per_grp == 0:
            load_uk(k // per_grp).wait()
        emit(q_blk, k, 0)
        sends[k].start()
        if k % per_grp == per_grp - 1:
            flush(c * half_heads + (k // per_grp) * group)

    raw_kv = [lo[:, dq_cols:dq_cols + lat_dim // 2], hi[:, dq_cols:dq_cols + lat_dim // 2]]
    mean_sq = sum(jnp.sum(r * r, axis=1, keepdims=True) for r in raw_kv) / lat_dim
    inv = lax.rsqrt(mean_sq + EPS)
    c_kv = jnp.concatenate([r * inv * kv_gain[:, i * (lat_dim // 2):(i + 1) * (lat_dim // 2)].astype(f32) for i, r in enumerate(raw_kv)], axis=1).astype(jnp.bfloat16)
    k_pe = rotate_pair(hi[:, dq_cols + lat_dim // 2:]).astype(jnp.bfloat16)
    kvn_out[:, :lat_dim] = c_kv.astype(f32)
    kvn_out[:, lat_dim:] = k_pe.astype(f32)
    kv_new_out[:, :lat_dim] = c_kv
    kv_new_out[:, lat_dim:] = k_pe[:, :64]

    for k in range(n_blk):
        sends[k].wait_recv()
        if k % per_grp == 0:
            load_uk(n_grp // 2 + k // per_grp).wait()
        emit(q_theirs[k], k, half_heads)
        if k % per_grp == per_grp - 1:
            flush((1 - c) * half_heads + (k // per_grp) * group)
    swap.wait_send()
    for s in sends:
        s.wait_send()


def project(hidden, cache_len, w_dq, q_gain, w_uq, w_dkv, kv_gain, w_uk):
    n_seqs, d_model = hidden.shape
    heads, nope_dim, lat_dim = w_uk.shape
    q_rank = w_dq.shape[1]
    rope_dim = w_dkv.shape[1] - lat_dim
    cos_t, sin_t = rope_tables(cache_len, rope_dim)
    cos_t = jnp.concatenate([cos_t] * 4, axis=1)
    sin_t = jnp.concatenate([-sin_t, sin_t] * 2, axis=1)
    cfg = dict(n_kt=4, lat_dim=lat_dim, group=16)
    n_k, n_blk = 8, 8
    dq_cols, dkv_cols = q_rank // 2, lat_dim // 2 + rope_dim
    blk = w_uq.shape[1] // 2 // n_blk
    f32, bf16 = jnp.float32, jnp.bfloat16
    dma = pltpu.SemaphoreType.DMA
    return pl.pallas_call(
        functools.partial(project_kernel, cfg),
        out_shape=(
            jax.ShapeDtypeStruct((n_seqs, heads, lat_dim + 128), bf16),
            jax.ShapeDtypeStruct((n_seqs, lat_dim + 128), f32),
            jax.ShapeDtypeStruct((n_seqs, lat_dim + rope_dim), bf16),
        ),
        in_specs=[VMEM, ANY, ANY, ANY, ANY, VMEM, VMEM, VMEM, VMEM],
        out_specs=(VMEM, VMEM, VMEM),
        scratch_shapes=[
            pltpu.VMEM((n_k, d_model // n_k, dq_cols), bf16),
            pltpu.VMEM((dkv_cols, d_model), bf16),
            pltpu.VMEM((n_blk, q_rank, blk), bf16),
            pltpu.VMEM((heads, nope_dim, lat_dim), bf16),
            pltpu.VMEM((2, n_seqs, dq_cols + lat_dim // 2 + 128), f32),
            pltpu.VMEM((n_blk, n_seqs, blk), f32),
            pltpu.VMEM((n_blk, n_seqs, blk), f32),
            pltpu.VMEM((lat_dim // 128 + 1, cfg["group"] * n_seqs, 128), f32),
            dma((n_k,)), dma((cfg["n_kt"],)), dma((n_blk,)), dma((heads // cfg["group"],)),
            dma, dma, dma((n_blk,)), dma((n_blk,)),
        ],
        compiler_params=pltpu.CompilerParams(collective_id=1, has_side_effects=True, vmem_limit_bytes=56 * 1024 * 1024),
        name="project",
    )(hidden, w_dq, w_dkv.T, w_uq, w_uk, q_gain.reshape(1, -1), kv_gain.reshape(1, -1), cos_t, sin_t)


def attend_kernel(cfg, len_ref, q_ref, kvn_ref, ckv_hbm, kpe_hbm, cout_hbm, kout_hbm, o_hbm,
                  cbuf, kbuf, obuf, peaks, denoms, isem, osem, psem):
    n_seqs, shard_len = ckv_hbm.shape[0], ckv_hbm.shape[1]
    lat_dim = ckv_hbm.shape[2]
    rope_dim = kpe_hbm.shape[1]
    per = o_hbm.shape[2] - 1
    n_buf, lag, chunk = cfg["n_buf"], cfg["lag"], cfg["chunk"]
    base = lax.axis_index('sp') * shard_len

    def copies_in(b, slot):
        return (pltpu.make_async_copy(ckv_hbm.at[b], cbuf.at[slot], isem.at[slot, 0]),
                pltpu.make_async_copy(kpe_hbm.at[b], kbuf.at[slot], isem.at[slot, 1]))

    def copies_out(b, slot):
        return (pltpu.make_async_copy(cbuf.at[slot], cout_hbm.at[b], osem.at[slot, 0]),
                pltpu.make_async_copy(kbuf.at[slot], kout_hbm.at[b], osem.at[slot, 1]))

    def copy_terms(b, side):
        return pltpu.make_async_copy(obuf.at[side], o_hbm.at[:, b // per, b % per], psem.at[side])

    def copy_stats(part):
        return pltpu.make_async_copy(obuf.at[0], o_hbm.at[:, part, per], psem.at[part])

    for i in range(n_buf - lag):
        for c in copies_in(i, i):
            c.start()
    peaks[...] = jnp.zeros_like(peaks)
    denoms[...] = jnp.zeros_like(denoms)

    def step(b, carry):
        slot = lax.rem(b, n_buf)

        @pl.when(b >= lag)
        def _():
            for c in copies_out(b - lag, lax.rem(b - lag + n_buf, n_buf)):
                c.wait()

        ahead = b - lag + n_buf

        @pl.when(ahead < n_seqs)
        def _():
            for c in copies_in(ahead, lax.rem(ahead, n_buf)):
                c.start()

        for c in copies_in(b, slot):
            c.wait()
        last = len_ref[b] - base

        @pl.when((last >= 0) & (last < shard_len))
        def _():
            picked = lax.broadcasted_iota(jnp.int32, kvn_ref.shape, 0) == b
            fresh_row = jnp.sum(jnp.where(picked, kvn_ref[...], 0.0), axis=0, keepdims=True)
            r0 = pl.multiple_of((last // 16) * 16, 16)
            rows = cbuf[slot, pl.ds(r0, 16), :].astype(jnp.float32)
            row = lax.broadcasted_iota(jnp.int32, rows.shape, 0)
            cbuf[slot, pl.ds(r0, 16), :] = jnp.where(row == last - r0, fresh_row[:, :lat_dim], rows).astype(cbuf.dtype)
            c0 = pl.multiple_of((last // 128) * 128, 128)
            cols = kbuf[slot, :, pl.ds(c0, 128)].astype(jnp.float32)
            lane = lax.broadcasted_iota(jnp.int32, cols.shape, 1)
            diag = lane == lax.broadcasted_iota(jnp.int32, cols.shape, 0)
            fresh = jnp.sum(jnp.where(diag, fresh_row[:, lat_dim:], 0.0), axis=1, keepdims=True)
            kbuf[slot, :, pl.ds(c0, 128)] = jnp.where(lane == last - c0, fresh, cols).astype(kbuf.dtype)

        q_lat, q_pe = q_ref[b, :, :lat_dim], q_ref[b, :, lat_dim:lat_dim + rope_dim]
        scores = []
        for t in range(0, shard_len, chunk):
            s = lax.dot_general(q_lat, cbuf[slot, t:t + chunk, :], (((1,), (1,)), ((), ())), preferred_element_type=jnp.float32)
            s = s + jnp.dot(q_pe, kbuf[slot, :, t:t + chunk], preferred_element_type=jnp.float32)
            pos = lax.broadcasted_iota(jnp.int32, (1, chunk), 1) + t
            scores.append(jnp.where(pos <= last, s * cfg["scale"], NEG_FILL))
        peak = functools.reduce(jnp.maximum, [jnp.max(s, axis=1, keepdims=True) for s in scores])
        denom = jnp.zeros_like(peak)
        lat_sum = None
        for k, t in enumerate(range(0, shard_len, chunk)):
            w = jnp.exp(scores[k] - peak)
            denom = denom + jnp.sum(w, axis=1, keepdims=True)
            term = jnp.dot(w.astype(jnp.bfloat16), cbuf[slot, t:t + chunk, :], preferred_element_type=jnp.float32)
            lat_sum = term if lat_sum is None else lat_sum + term
        for c in copies_out(b, slot):
            c.start()
        side = lax.rem(b, 2)

        @pl.when(b >= 2)
        def _():
            copy_terms(b - 2, side).wait()

        obuf[side] = lat_sum.reshape(obuf.shape[1:])
        lane = lax.broadcasted_iota(jnp.int32, peaks.shape, 1)
        peaks[...] = jnp.where(lane == b, peak, peaks[...])
        denoms[...] = jnp.where(lane == b, denom, denoms[...])
        copy_terms(b, side).start()
        return carry

    lax.fori_loop(0, n_seqs, step, 0)
    for i in range(n_seqs - 2, n_seqs):
        copy_terms(i, i % 2).wait()
    obuf[0, :, :, 0:128] = peaks[...].reshape(obuf.shape[1], obuf.shape[2], 128)
    obuf[0, :, :, 128:256] = denoms[...].reshape(obuf.shape[1], obuf.shape[2], 128)
    for i in range(n_seqs - lag, n_seqs):
        for c in copies_out(i, i % n_buf):
            c.wait()
    for part in range(2):
        copy_stats(part).start()
    for part in range(2):
        copy_stats(part).wait()


def attend(q, kvn, cache_len, ckv_blk, kpe_blk_t, n_dev, qk_dim):
    n_seqs, shard_len, lat_dim = ckv_blk.shape
    rope_dim = kpe_blk_t.shape[1]
    n_heads = q.shape[1]
    cfg = dict(n_buf=8, lag=3, chunk=512, scale=qk_dim ** -0.5)
    terms_shape = (n_dev, 2, n_seqs // 2 + 1, n_heads // n_dev, lat_dim)
    return pl.pallas_call(
        functools.partial(attend_kernel, cfg),
        out_shape=(
            jax.ShapeDtypeStruct(ckv_blk.shape, ckv_blk.dtype),
            jax.ShapeDtypeStruct(kpe_blk_t.shape, kpe_blk_t.dtype),
            jax.ShapeDtypeStruct(terms_shape, jnp.float32),
        ),
        in_specs=[SMEM, VMEM, VMEM, ANY, ANY],
        out_specs=(ANY, ANY, ANY),
        scratch_shapes=[
            pltpu.VMEM((cfg["n_buf"], shard_len, lat_dim), ckv_blk.dtype),
            pltpu.VMEM((cfg["n_buf"], rope_dim, shard_len), kpe_blk_t.dtype),
            pltpu.VMEM((2, n_dev, n_heads // n_dev, lat_dim), jnp.float32),
            pltpu.VMEM((n_heads, 128), jnp.float32),
            pltpu.VMEM((n_heads, 128), jnp.float32),
            pltpu.SemaphoreType.DMA((cfg["n_buf"], 2)),
            pltpu.SemaphoreType.DMA((cfg["n_buf"], 2)),
            pltpu.SemaphoreType.DMA((2,)),
        ],
        compiler_params=pltpu.CompilerParams(vmem_limit_bytes=56 * 1024 * 1024),
        name="attend",
    )(cache_len, q, kvn, ckv_blk, kpe_blk_t)


def finish_kernel(terms, w_uv, w_out, out_ref, own, pair, from_x, from_y, uv, wo, merged, oheads, psend, precv, isend, irecv, fin, agr, agp,
                  lsem, own_sem, d_ss, d_rs, x_ss, x_rs, y_ss, y_rs, p_ss, p_rs, i_ss, i_rs, a_ss, a_rs, f_ss, f_rs):
    n_seqs, width = fin.shape
    heads = uv.shape[0]
    depth = wo.shape[0]
    me = lax.axis_index('sp')
    y, x, c = me // 4, (me // 2) % 2, me % 2

    def device(q, jc):
        return ((y + q // 2) % 2) * 4 + ((x + q % 2) % 2) * 2 + (c + jc) % 2

    def send(src, dst, ss, rs, dev):
        return pltpu.make_async_remote_copy(src_ref=src, dst_ref=dst, send_sem=ss, recv_sem=rs, device_id={'sp': dev}, device_id_type=MESH)

    load_uv = pltpu.make_async_copy(w_uv.at[pl.ds(me * heads, heads)], uv, lsem.at[0])
    load_wo = pltpu.make_async_copy(w_out.at[pl.ds(me * depth, depth)], wo, lsem.at[1])
    order = ((3, 0), (3, 1), (1, 0), (2, 1), (2, 0), (1, 1), (0, 0), (0, 1))
    per = n_seqs // 2
    loads = {(q, h): pltpu.make_async_copy(terms.at[device(q, 0), h], own.at[q, h], own_sem.at[q, h]) for q, h in order}
    for k in order:
        loads[k].start()
    load_uv.start()
    load_wo.start()

    others = ((0, 1), (1, 0), (2, 0), (3, 0))
    barrier = pltpu.get_barrier_semaphore()
    for q, jc in others:
        pl.semaphore_signal(barrier, inc=1, device_id={'sp': device(q, jc)}, device_id_type=MESH)
    pl.semaphore_wait(barrier, len(others))

    d_sends = {(q, h): send(terms.at[device(q, 1), h], pair.at[q, h], d_ss.at[q, h], d_rs.at[q, h], device(0, 1)) for q, h in order}
    for k in order:
        d_sends[k].start()

    def merge(dst, src, h):
        old, new = dst[per, :, :128], src[per, :, :128]
        peak = jnp.maximum(old, new)
        f_old, f_new = jnp.exp(old - peak), jnp.exp(new - peak)
        dst[per, :, :128] = peak
        dst[per, :, 128:256] = f_old * dst[per, :, 128:256] + f_new * src[per, :, 128:256]
        for i in range(per):
            b = h * per + i
            dst[i] = f_old[:, b:b + 1] * dst[i] + f_new[:, b:b + 1] * src[i]

    def merge_pair(q, h):
        loads[q, h].wait()
        d_sends[q, h].wait_recv()
        merge(own.at[q, h], pair.at[q, h], h)

    x_dev, y_dev = device(1, 0), device(2, 0)
    x_sends = [send(own.at[k], from_x.at[i], x_ss.at[i], x_rs.at[i], x_dev) for i, k in enumerate(((3, 0), (1, 0), (1, 1)))]
    y_sends = [send(own.at[k], from_y.at[i], y_ss.at[i], y_rs.at[i], y_dev) for i, k in enumerate(((3, 1), (2, 1), (2, 0)))]
    merge_pair(3, 0)
    merge_pair(3, 1)
    x_sends[0].start()
    merge_pair(1, 0)
    y_sends[0].start()
    merge_pair(2, 1)
    x_sends[1].start()
    merge_pair(2, 0)
    y_sends[1].start()
    merge_pair(1, 1)
    merge_pair(0, 0)
    merge_pair(0, 1)
    x_sends[0].wait_recv()
    merge(own.at[2, 0], from_x.at[0], 0)
    y_sends[0].wait_recv()
    merge(own.at[1, 1], from_y.at[0], 1)
    y_sends[2].start()
    x_sends[2].start()
    x_sends[1].wait_recv()
    merge(own.at[0, 0], from_x.at[1], 0)
    y_sends[1].wait_recv()
    merge(own.at[0, 1], from_y.at[1], 1)
    y_sends[2].wait_recv()
    merge(own.at[0, 0], from_y.at[2], 0)
    x_sends[2].wait_recv()
    merge(own.at[0, 1], from_x.at[2], 1)
    for h in range(2):
        inv = 1.0 / own[0, h, per, :, 128:256]
        for i in range(per):
            b = h * per + i
            acc = inv[:, b:b + 1] * own[0, h, i]
            for k in range(merged.shape[0]):
                merged[k, b * heads:(b + 1) * heads, :] = acc[:, k * 128:(k + 1) * 128]
    load_uv.wait()
    for h in range(heads):
        o_lat = jnp.concatenate([merged[k, pl.ds(h, n_seqs, stride=heads), :] for k in range(merged.shape[0])], axis=1).astype(jnp.bfloat16)
        o_h = lax.dot_general(o_lat, uv[h], (((1,), (1,)), ((), ())), preferred_element_type=jnp.float32)
        oheads[:, h * o_h.shape[1]:(h + 1) * o_h.shape[1]] = o_h.astype(jnp.bfloat16)
    load_wo.wait()

    def partial_out(dev):
        cols = pl.ds(pl.multiple_of(dev * width, 128), width)
        return jnp.dot(oheads[...], wo[:, cols], preferred_element_type=jnp.float32)

    waiting = []
    p_sends, i_sends = {}, []
    for q in (3, 1, 2, 0):
        psend[q] = partial_out(device(q, 1))
        p_sends[q] = send(psend.at[q], precv.at[q], p_ss.at[q], p_rs.at[q], device(0, 1))
        for w in waiting:
            w.start()
        waiting = [p_sends[q]]
    mine = None
    for q in (3, 1, 2, 0):
        part = partial_out(device(q, 0))
        for w in waiting:
            w.start()
        waiting = []
        p_sends[q].wait_recv()
        if q:
            isend[q - 1] = part + precv[q]
            i_sends.append(send(isend.at[q - 1], irecv.at[q - 1], i_ss.at[q - 1], i_rs.at[q - 1], device(q, 0)))
            waiting = [i_sends[-1]]
        else:
            mine = part + precv[0]
    for s in i_sends:
        s.wait_recv()
    result = mine + irecv[0] + irecv[1] + irecv[2]
    fin[...] = result
    out_ref[:, pl.ds(pl.multiple_of(me * width, 128), width)] = result.astype(out_ref.dtype)

    a_sends = {q: send(fin, agr.at[q - 1], a_ss.at[q - 1], a_rs.at[q - 1], device(q, 0)) for q in (3, 1, 2)}
    f_sends = {0: send(fin, agp.at[0], f_ss.at[0], f_rs.at[0], device(0, 1))}
    for q in (3, 1, 2):
        a_sends[q].start()
    f_sends[0].start()
    for q in (1, 2, 3):
        f_sends[q] = send(agr.at[q - 1], agp.at[q], f_ss.at[q], f_rs.at[q], device(0, 1))
        a_sends[q].wait_recv()
        f_sends[q].start()
        out_ref[:, pl.ds(pl.multiple_of(device(q, 0) * width, 128), width)] = agr[q - 1].astype(out_ref.dtype)
    for q in range(4):
        f_sends[q].wait_recv()
        out_ref[:, pl.ds(pl.multiple_of(device(q, 1) * width, 128), width)] = agp[q].astype(out_ref.dtype)
    for s in list(d_sends.values()) + x_sends + y_sends + list(p_sends.values()) + i_sends + list(a_sends.values()) + list(f_sends.values()):
        s.wait_send()


def finish(terms, w_uv, w_out):
    n_dev, _, rows, heads, lat_dim = terms.shape
    n_seqs = 2 * (rows - 1)
    d_model = w_out.shape[1]
    depth = w_out.shape[0] // n_dev
    width = d_model // n_dev
    f32 = jnp.float32
    return pl.pallas_call(
        finish_kernel,
        out_shape=jax.ShapeDtypeStruct((n_seqs, d_model), jnp.bfloat16),
        in_specs=[ANY, ANY, ANY],
        out_specs=VMEM,
        scratch_shapes=[
            pltpu.VMEM((4, 2, rows, heads, lat_dim), f32),
            pltpu.VMEM((4, 2, rows, heads, lat_dim), f32),
            pltpu.VMEM((3, rows, heads, lat_dim), f32),
            pltpu.VMEM((3, rows, heads, lat_dim), f32),
            pltpu.VMEM((heads,) + w_uv.shape[1:], w_uv.dtype),
            pltpu.VMEM((depth, d_model), w_out.dtype),
            pltpu.VMEM((lat_dim // 128, n_seqs * heads, 128), f32),
            pltpu.VMEM((n_seqs, depth), jnp.bfloat16),
            pltpu.VMEM((4, n_seqs, width), f32),
            pltpu.VMEM((4, n_seqs, width), f32),
            pltpu.VMEM((3, n_seqs, width), f32),
            pltpu.VMEM((3, n_seqs, width), f32),
            pltpu.VMEM((n_seqs, width), f32),
            pltpu.VMEM((3, n_seqs, width), f32),
            pltpu.VMEM((4, n_seqs, width), f32),
            pltpu.SemaphoreType.DMA((2,)),
            pltpu.SemaphoreType.DMA((4, 2)),
            pltpu.SemaphoreType.DMA((4, 2)),
            pltpu.SemaphoreType.DMA((4, 2)),
            pltpu.SemaphoreType.DMA((3,)),
            pltpu.SemaphoreType.DMA((3,)),
            pltpu.SemaphoreType.DMA((3,)),
            pltpu.SemaphoreType.DMA((3,)),
            pltpu.SemaphoreType.DMA((4,)),
            pltpu.SemaphoreType.DMA((4,)),
            pltpu.SemaphoreType.DMA((3,)),
            pltpu.SemaphoreType.DMA((3,)),
            pltpu.SemaphoreType.DMA((3,)),
            pltpu.SemaphoreType.DMA((3,)),
            pltpu.SemaphoreType.DMA((4,)),
            pltpu.SemaphoreType.DMA((4,)),
        ],
        compiler_params=pltpu.CompilerParams(collective_id=0, has_side_effects=True, vmem_limit_bytes=56 * 1024 * 1024),
        name="finish",
    )(terms, w_uv, w_out)


def solution(mesh):
    n_dev = mesh.shape['sp']

    def local_step(hidden, ckv_blk, kpe_blk, cache_len, w_dq, q_gain, w_uq, w_dkv, kv_gain, w_uk, w_uv, w_out):
        q, kvn, kv_new = project(hidden, cache_len, w_dq, q_gain, w_uq, w_dkv, kv_gain, w_uk)
        qk_dim = w_uk.shape[1] + kpe_blk.shape[2]
        ckv_out, kpe_out_t, terms = attend(q, kvn, cache_len, ckv_blk, jnp.swapaxes(kpe_blk, 1, 2), n_dev, qk_dim)
        out = finish(terms, w_uv, w_out)
        return out, ckv_out, jnp.swapaxes(kpe_out_t, 1, 2), kv_new

    cache_spec = P('dp', 'sp', None)
    return jax.shard_map(local_step, mesh=mesh, in_specs=(P('dp', None), cache_spec, cache_spec, P('dp'), P(), P(), P(), P(), P(), P(), P(), P()), out_specs=(P('dp', None), cache_spec, cache_spec, P('dp', None)), check_vma=False)
```

```python
import functools

import jax
import jax.numpy as jnp
import numpy as np
from jax import lax
from jax.experimental import pallas as pl
from jax.experimental.pallas import tpu as pltpu
from jax.sharding import PartitionSpec as P

EPS = 1e-6
ROPE_THETA = 10000.0
NEG_FILL = -1e30
MESH = pl.DeviceIdType.MESH
VMEM = pl.BlockSpec(memory_space=pltpu.VMEM)
SMEM = pl.BlockSpec(memory_space=pltpu.SMEM)
ANY = pl.BlockSpec(memory_space=pl.ANY)


def project_kernel(cfg, len_ref, hidden, w_dq, w_dkv_t, w_uq, w_uk, q_gain_ref, kv_gain_ref, freq, q_out, kvn_out,
                   dq, dkv, uq, uk, halves, q_mine, q_theirs, turn, dq_sem, dkv_sem, uq_sem, uk_sem, h_ss, h_rs, q_ss, q_rs):
    n_seqs = hidden.shape[0]
    n_k, k_rows, dq_cols = dq.shape
    n_blk, _, blk = uq.shape
    dkv_cols = dkv.shape[0]
    n_kt = cfg["n_kt"]
    k_tile = dkv.shape[1] // n_kt
    lat_dim = cfg["lat_dim"]
    nope_dim = uk.shape[1]
    heads = uk.shape[0]
    half_heads = heads // 2
    group, pitch = cfg["group"], cfg["pitch"]
    me = lax.axis_index('sp')
    c = me % 2
    partner = me - c + (1 - c)
    f32 = jnp.float32

    def load_dq(k):
        return pltpu.make_async_copy(w_dq.at[pl.ds(k * k_rows, k_rows), pl.ds(pl.multiple_of(c * dq_cols, 128), dq_cols)], dq.at[k], dq_sem.at[k])

    def load_dkv(k):
        return pltpu.make_async_copy(w_dkv_t.at[pl.ds(pl.multiple_of(c * (lat_dim // 2), 16), dkv_cols), pl.ds(k * k_tile, k_tile)], dkv.at[:, pl.ds(k * k_tile, k_tile)], dkv_sem.at[k])

    def load_uq(k):
        return pltpu.make_async_copy(w_uq.at[:, pl.ds(pl.multiple_of((c * n_blk + k) * blk, 128), blk)], uq.at[k], uq_sem.at[k])

    def load_uk(k):
        first = (c * half_heads + k * group) % heads
        return pltpu.make_async_copy(w_uk.at[pl.ds(first, group)], uk.at[pl.ds(k * group, group)], uk_sem.at[k])

    n_grp = heads // group
    per_kt = n_k // n_kt
    per_grp = n_blk // (n_grp // 2)
    loads = []
    for k in range(n_k):
        loads.append(load_dq(k))
        if k % per_kt == 0:
            loads.append(load_dkv(k // per_kt))
    for k in range(n_blk):
        loads.append(load_uq(k))
        if k % per_grp == 0:
            loads.append(load_uk(k // per_grp))
        if k >= cfg["behind"] and (k - cfg["behind"]) % per_grp == 0:
            loads.append(load_uk(n_grp // 2 + (k - cfg["behind"]) // per_grp))
    in_flight = cfg["in_flight"]
    for load in loads[:in_flight]:
        load.start()
    queue = loads[in_flight:]

    def wait_load(load):
        load.wait()
        if queue:
            queue.pop(0).start()

    barrier = pltpu.get_barrier_semaphore()
    pl.semaphore_signal(barrier, inc=1, device_id={'sp': partner}, device_id_type=MESH)
    pl.semaphore_wait(barrier, 1)

    lane = lax.broadcasted_iota(jnp.int32, (n_seqs, 128), 1)
    row = lax.broadcasted_iota(jnp.int32, (n_seqs, 128), 0)
    position = jnp.zeros((n_seqs, 128), f32)
    for b in range(n_seqs):
        position = jnp.where(row == b, len_ref[b].astype(f32), position)
    angle = position * freq[...]
    cos_t = jnp.cos(angle)
    sin_t = jnp.where(lane % 64 < 32, -jnp.sin(angle), jnp.sin(angle))
    q_gain = q_gain_ref[...].astype(f32).reshape(1, -1)
    kv_gain = kv_gain_ref[...].astype(f32).reshape(1, -1)

    acc_q = jnp.zeros((n_seqs, dq_cols), f32)
    acc_kv = jnp.zeros((n_seqs, dkv_cols), f32)
    for k in range(n_k):
        wait_load(load_dq(k))
        acc_q = acc_q + jnp.dot(hidden[:, k * k_rows:(k + 1) * k_rows], dq[k], preferred_element_type=f32)
        if k % per_kt == per_kt - 1:
            t = k // per_kt
            wait_load(load_dkv(t))
            cols = slice(t * k_tile, (t + 1) * k_tile)
            acc_kv = acc_kv + lax.dot_general(hidden[:, cols], dkv[:, cols], (((1,), (1,)), ((), ())), preferred_element_type=f32)
    halves[c, :, dq_cols + lat_dim // 2:] = jnp.zeros((n_seqs, 128), f32)
    halves[c, :, :dq_cols] = acc_q
    halves[c, :, dq_cols:dq_cols + dkv_cols] = acc_kv
    swap = pltpu.make_async_remote_copy(src_ref=halves.at[c], dst_ref=halves.at[c], send_sem=h_ss, recv_sem=h_rs, device_id={'sp': partner}, device_id_type=MESH)
    swap.start()
    swap.wait_recv()

    lo, hi = halves[0], halves[1]
    raw_q = [lo[:, :dq_cols], hi[:, :dq_cols]]
    mean_sq = sum(jnp.sum(r * r, axis=1, keepdims=True) for r in raw_q) / (2 * dq_cols)
    inv = lax.rsqrt(mean_sq + EPS)
    c_q = jnp.concatenate([r * inv * q_gain[:, i * dq_cols:(i + 1) * dq_cols] for i, r in enumerate(raw_q)], axis=1).astype(jnp.bfloat16)

    def rotate_pair(pair):
        other = jnp.where(lane % 64 < 32, pltpu.roll(pair, 96, 1), pltpu.roll(pair, 32, 1))
        return pair * cos_t + other * sin_t

    def emit(q_blk, k, side):
        for p in range(blk // 384):
            t0, t1, t2 = (q_blk[:, p * 384 + i * 128:p * 384 + (i + 1) * 128] for i in range(3))
            odd = jnp.where(lane < 64, pltpu.roll(t1, 64, 1), pltpu.roll(t2, 64, 1))
            pe = rotate_pair(jnp.where(lane < 64, t1, t2))
            for i, (nope, rope) in enumerate(((t0, pe), (odd, pltpu.roll(pe, 64, 1)))):
                h = k * (blk // 192) + p * 2 + i
                lat = jnp.dot(nope.astype(jnp.bfloat16), uk[side * half_heads + h], preferred_element_type=f32)
                first = (h % group) * pitch
                for j in range(lat_dim // 128):
                    turn[side, j, first:first + n_seqs, :] = lat[:, j * 128:(j + 1) * 128]
                turn[side, lat_dim // 128, first:first + n_seqs, :] = rope

    def flush(first, side):
        rows = pl.ds(pl.multiple_of(first, group), group)
        for b in range(n_seqs):
            for j in range(lat_dim // 128 + 1):
                q_out[b, rows, j * 128:(j + 1) * 128] = turn[side, j, pl.ds(b, group, stride=pitch), :].astype(q_out.dtype)

    sends = []

    def own_block(k):
        wait_load(load_uq(k))
        q_blk = jnp.dot(c_q, uq[k], preferred_element_type=f32).astype(jnp.bfloat16).astype(f32)
        q_mine[k] = q_blk
        sends.append(pltpu.make_async_remote_copy(src_ref=q_mine.at[k], dst_ref=q_theirs.at[k], send_sem=q_ss.at[k], recv_sem=q_rs.at[k], device_id={'sp': partner}, device_id_type=MESH))
        if k % per_grp == 0:
            wait_load(load_uk(k // per_grp))
        emit(q_blk, k, 0)
        sends[k].start()
        if k % per_grp == per_grp - 1:
            flush(c * half_heads + (k // per_grp) * group, 0)

    def their_block(k):
        sends[k].wait_recv()
        if k % per_grp == 0:
            wait_load(load_uk(n_grp // 2 + k // per_grp))
        emit(q_theirs[k], k, 1)
        if k % per_grp == per_grp - 1:
            flush((1 - c) * half_heads + (k // per_grp) * group, 1)

    behind = cfg["behind"]
    for k in range(n_blk):
        own_block(k)
        if k >= behind:
            their_block(k - behind)
    raw_kv = [lo[:, dq_cols:dq_cols + lat_dim // 2], hi[:, dq_cols:dq_cols + lat_dim // 2]]
    mean_sq = sum(jnp.sum(r * r, axis=1, keepdims=True) for r in raw_kv) / lat_dim
    inv = lax.rsqrt(mean_sq + EPS)
    c_kv = jnp.concatenate([r * inv * kv_gain[:, i * (lat_dim // 2):(i + 1) * (lat_dim // 2)] for i, r in enumerate(raw_kv)], axis=1).astype(jnp.bfloat16)
    k_pe = rotate_pair(hi[:, dq_cols + lat_dim // 2:]).astype(jnp.bfloat16)
    kvn_out[:, :lat_dim] = c_kv.astype(f32)
    kvn_out[:, lat_dim:] = k_pe.astype(f32)

    for k in range(n_blk - behind, n_blk):
        their_block(k)
    swap.wait_send()
    for s in sends:
        s.wait_send()


def project(hidden, cache_len, w_dq, q_gain, w_uq, w_dkv, kv_gain, w_uk):
    n_seqs, d_model = hidden.shape
    heads, nope_dim, lat_dim = w_uk.shape
    q_rank = w_dq.shape[1]
    rope_dim = w_dkv.shape[1] - lat_dim
    freq = np.power(ROPE_THETA, -2.0 * np.arange(rope_dim // 2) / rope_dim).astype(np.float32)
    freq = jnp.asarray(np.tile(freq, 128 // freq.size).reshape(1, 128))
    cfg = dict(n_kt=4, lat_dim=lat_dim, group=16, pitch=n_seqs + 8, in_flight=4, behind=2)
    n_k, n_blk = 8, 8
    dq_cols, dkv_cols = q_rank // 2, lat_dim // 2 + rope_dim
    blk = w_uq.shape[1] // 2 // n_blk
    f32, bf16 = jnp.float32, jnp.bfloat16
    dma = pltpu.SemaphoreType.DMA
    return pl.pallas_call(
        functools.partial(project_kernel, cfg),
        out_shape=(
            jax.ShapeDtypeStruct((n_seqs, heads, lat_dim + 128), bf16),
            jax.ShapeDtypeStruct((n_seqs, lat_dim + 128), f32),
        ),
        in_specs=[SMEM, VMEM, ANY, ANY, ANY, ANY, VMEM, VMEM, VMEM],
        out_specs=(VMEM, VMEM),
        scratch_shapes=[
            pltpu.VMEM((n_k, d_model // n_k, dq_cols), bf16),
            pltpu.VMEM((dkv_cols, d_model), bf16),
            pltpu.VMEM((n_blk, q_rank, blk), bf16),
            pltpu.VMEM((heads, nope_dim, lat_dim), bf16),
            pltpu.VMEM((2, n_seqs, dq_cols + lat_dim // 2 + 128), f32),
            pltpu.VMEM((n_blk, n_seqs, blk), f32),
            pltpu.VMEM((n_blk, n_seqs, blk), f32),
            pltpu.VMEM((2, lat_dim // 128 + 1, cfg["group"] * cfg["pitch"], 128), f32),
            dma((n_k,)), dma((cfg["n_kt"],)), dma((n_blk,)), dma((heads // cfg["group"],)),
            dma, dma, dma((n_blk,)), dma((n_blk,)),
        ],
        compiler_params=pltpu.CompilerParams(collective_id=1, has_side_effects=True, vmem_limit_bytes=56 * 1024 * 1024),
        name="project",
    )(cache_len, hidden, w_dq, w_dkv.T, w_uq, w_uk, q_gain, kv_gain, freq)


def attend_kernel(cfg, len_ref, q_ref, kvn_ref, ckv_hbm, kpe_hbm, cout_hbm, kout_hbm, o_hbm, kv_new,
                  cbuf, kbuf, obuf, peaks, denoms, isem, osem, psem):
    n_seqs, shard_len = ckv_hbm.shape[0], ckv_hbm.shape[1]
    lat_dim = ckv_hbm.shape[2]
    rope_dim = kpe_hbm.shape[1]
    per = o_hbm.shape[2] - 1
    n_buf, lag, chunk = cfg["n_buf"], cfg["lag"], cfg["chunk"]
    base = lax.axis_index('sp') * shard_len

    def copies_in(b, slot):
        return (pltpu.make_async_copy(ckv_hbm.at[b], cbuf.at[slot], isem.at[slot, 0]),
                pltpu.make_async_copy(kpe_hbm.at[b], kbuf.at[slot], isem.at[slot, 1]))

    def copies_out(b, slot):
        return (pltpu.make_async_copy(cbuf.at[slot], cout_hbm.at[b], osem.at[slot, 0]),
                pltpu.make_async_copy(kbuf.at[slot], kout_hbm.at[b], osem.at[slot, 1]))

    def copy_terms(b, side):
        return pltpu.make_async_copy(obuf.at[side], o_hbm.at[:, b // per, b % per], psem.at[side])

    def copy_stats(part):
        return pltpu.make_async_copy(obuf.at[0], o_hbm.at[:, part, per], psem.at[part])

    for i in range(n_buf - lag):
        for c in copies_in(i, i):
            c.start()
    kv_new[...] = kvn_ref[:, :lat_dim + rope_dim].astype(kv_new.dtype)
    peaks[...] = jnp.zeros_like(peaks)
    denoms[...] = jnp.zeros_like(denoms)

    def step(b, carry):
        slot = lax.rem(b, n_buf)

        @pl.when(b >= lag)
        def _():
            for c in copies_out(b - lag, lax.rem(b - lag + n_buf, n_buf)):
                c.wait()

        ahead = b - lag + n_buf

        @pl.when(ahead < n_seqs)
        def _():
            for c in copies_in(ahead, lax.rem(ahead, n_buf)):
                c.start()

        for c in copies_in(b, slot):
            c.wait()
        last = len_ref[b] - base

        @pl.when((last >= 0) & (last < shard_len))
        def _():
            picked = lax.broadcasted_iota(jnp.int32, kvn_ref.shape, 0) == b
            fresh_row = jnp.sum(jnp.where(picked, kvn_ref[...], 0.0), axis=0, keepdims=True)
            r0 = pl.multiple_of((last // 16) * 16, 16)
            rows = cbuf[slot, pl.ds(r0, 16), :].astype(jnp.float32)
            row = lax.broadcasted_iota(jnp.int32, rows.shape, 0)
            cbuf[slot, pl.ds(r0, 16), :] = jnp.where(row == last - r0, fresh_row[:, :lat_dim], rows).astype(cbuf.dtype)
            c0 = pl.multiple_of((last // 128) * 128, 128)
            cols = kbuf[slot, :, pl.ds(c0, 128)].astype(jnp.float32)
            lane = lax.broadcasted_iota(jnp.int32, cols.shape, 1)
            diag = lane == lax.broadcasted_iota(jnp.int32, cols.shape, 0)
            fresh = jnp.sum(jnp.where(diag, fresh_row[:, lat_dim:], 0.0), axis=1, keepdims=True)
            kbuf[slot, :, pl.ds(c0, 128)] = jnp.where(lane == last - c0, fresh, cols).astype(kbuf.dtype)

        q_lat, q_pe = q_ref[b, :, :lat_dim], q_ref[b, :, lat_dim:lat_dim + rope_dim]
        scores = []
        for t in range(0, shard_len, chunk):
            s = lax.dot_general(q_lat, cbuf[slot, t:t + chunk, :], (((1,), (1,)), ((), ())), preferred_element_type=jnp.float32)
            s = s + jnp.dot(q_pe, kbuf[slot, :, t:t + chunk], preferred_element_type=jnp.float32)
            pos = lax.broadcasted_iota(jnp.int32, (1, chunk), 1) + t
            scores.append(jnp.where(pos <= last, s * cfg["scale"], NEG_FILL))
        peak = functools.reduce(jnp.maximum, [jnp.max(s, axis=1, keepdims=True) for s in scores])
        denom = jnp.zeros_like(peak)
        lat_sum = None
        for k, t in enumerate(range(0, shard_len, chunk)):
            w = jnp.exp(scores[k] - peak)
            denom = denom + jnp.sum(w, axis=1, keepdims=True)
            term = jnp.dot(w.astype(jnp.bfloat16), cbuf[slot, t:t + chunk, :], preferred_element_type=jnp.float32)
            lat_sum = term if lat_sum is None else lat_sum + term
        for c in copies_out(b, slot):
            c.start()
        side = lax.rem(b, 2)

        @pl.when(b >= 2)
        def _():
            copy_terms(b - 2, side).wait()

        obuf[side] = lat_sum.reshape(obuf.shape[1:])
        lane = lax.broadcasted_iota(jnp.int32, peaks.shape, 1)
        peaks[...] = jnp.where(lane == b, peak, peaks[...])
        denoms[...] = jnp.where(lane == b, denom, denoms[...])
        copy_terms(b, side).start()
        return carry

    lax.fori_loop(0, n_seqs, step, 0)
    for i in range(n_seqs - 2, n_seqs):
        copy_terms(i, i % 2).wait()
    obuf[0, :, :, 0:128] = peaks[...].reshape(obuf.shape[1], obuf.shape[2], 128)
    obuf[0, :, :, 128:256] = denoms[...].reshape(obuf.shape[1], obuf.shape[2], 128)
    for i in range(n_seqs - lag, n_seqs):
        for c in copies_out(i, i % n_buf):
            c.wait()
    for part in range(2):
        copy_stats(part).start()
    for part in range(2):
        copy_stats(part).wait()


def attend(q, kvn, cache_len, ckv_blk, kpe_blk_t, n_dev, qk_dim):
    n_seqs, shard_len, lat_dim = ckv_blk.shape
    rope_dim = kpe_blk_t.shape[1]
    n_heads = q.shape[1]
    cfg = dict(n_buf=8, lag=3, chunk=512, scale=qk_dim ** -0.5)
    terms_shape = (n_dev, 2, n_seqs // 2 + 1, n_heads // n_dev, lat_dim)
    return pl.pallas_call(
        functools.partial(attend_kernel, cfg),
        out_shape=(
            jax.ShapeDtypeStruct(ckv_blk.shape, ckv_blk.dtype),
            jax.ShapeDtypeStruct(kpe_blk_t.shape, kpe_blk_t.dtype),
            jax.ShapeDtypeStruct(terms_shape, jnp.float32),
            jax.ShapeDtypeStruct((n_seqs, lat_dim + rope_dim), ckv_blk.dtype),
        ),
        in_specs=[SMEM, VMEM, VMEM, ANY, ANY],
        out_specs=(ANY, ANY, ANY, VMEM),
        scratch_shapes=[
            pltpu.VMEM((cfg["n_buf"], shard_len, lat_dim), ckv_blk.dtype),
            pltpu.VMEM((cfg["n_buf"], rope_dim, shard_len), kpe_blk_t.dtype),
            pltpu.VMEM((2, n_dev, n_heads // n_dev, lat_dim), jnp.float32),
            pltpu.VMEM((n_heads, 128), jnp.float32),
            pltpu.VMEM((n_heads, 128), jnp.float32),
            pltpu.SemaphoreType.DMA((cfg["n_buf"], 2)),
            pltpu.SemaphoreType.DMA((cfg["n_buf"], 2)),
            pltpu.SemaphoreType.DMA((2,)),
        ],
        compiler_params=pltpu.CompilerParams(vmem_limit_bytes=56 * 1024 * 1024),
        name="attend",
    )(cache_len, q, kvn, ckv_blk, kpe_blk_t)


def finish_kernel(terms, w_uv, w_out, out_ref, own, pair, from_x, from_y, uv, wo, merged, oheads, psend, precv, isend, irecv, fin, agr, agp,
                  lsem, own_sem, d_ss, d_rs, x_ss, x_rs, y_ss, y_rs, p_ss, p_rs, i_ss, i_rs, a_ss, a_rs, f_ss, f_rs):
    n_seqs, width = fin.shape
    heads = uv.shape[0]
    depth = wo.shape[0]
    me = lax.axis_index('sp')
    y, x, c = me // 4, (me // 2) % 2, me % 2

    def device(q, jc):
        return ((y + q // 2) % 2) * 4 + ((x + q % 2) % 2) * 2 + (c + jc) % 2

    def send(src, dst, ss, rs, dev):
        return pltpu.make_async_remote_copy(src_ref=src, dst_ref=dst, send_sem=ss, recv_sem=rs, device_id={'sp': dev}, device_id_type=MESH)

    load_uv = pltpu.make_async_copy(w_uv.at[pl.ds(me * heads, heads)], uv, lsem.at[0])
    load_wo = pltpu.make_async_copy(w_out.at[pl.ds(me * depth, depth)], wo, lsem.at[1])
    order = ((3, 0), (3, 1), (1, 0), (2, 1), (2, 0), (1, 1), (0, 0), (0, 1))
    per = n_seqs // 2
    loads = {(q, h): pltpu.make_async_copy(terms.at[device(q, 0), h], own.at[q, h], own_sem.at[q, h]) for q, h in order}
    for k in order:
        loads[k].start()
    load_uv.start()

    others = ((0, 1), (1, 0), (2, 0), (3, 0))
    barrier = pltpu.get_barrier_semaphore()
    for q, jc in others:
        pl.semaphore_signal(barrier, inc=1, device_id={'sp': device(q, jc)}, device_id_type=MESH)
    pl.semaphore_wait(barrier, len(others))

    d_sends = {(q, h): send(terms.at[device(q, 1), h], pair.at[q, h], d_ss.at[q, h], d_rs.at[q, h], device(0, 1)) for q, h in order}
    for k in order:
        d_sends[k].start()

    def merge(dst, src, h):
        old, new = dst[per, :, :128], src[per, :, :128]
        peak = jnp.maximum(old, new)
        f_old, f_new = jnp.exp(old - peak), jnp.exp(new - peak)
        dst[per, :, :128] = peak
        dst[per, :, 128:256] = f_old * dst[per, :, 128:256] + f_new * src[per, :, 128:256]
        for i in range(per):
            b = h * per + i
            dst[i] = f_old[:, b:b + 1] * dst[i] + f_new[:, b:b + 1] * src[i]

    def merge_pair(q, h):
        loads[q, h].wait()
        d_sends[q, h].wait_recv()
        merge(own.at[q, h], pair.at[q, h], h)

    x_dev, y_dev = device(1, 0), device(2, 0)
    x_sends = [send(own.at[k], from_x.at[i], x_ss.at[i], x_rs.at[i], x_dev) for i, k in enumerate(((3, 0), (1, 0), (1, 1)))]
    y_sends = [send(own.at[k], from_y.at[i], y_ss.at[i], y_rs.at[i], y_dev) for i, k in enumerate(((3, 1), (2, 1), (2, 0)))]
    merge_pair(3, 0)
    merge_pair(3, 1)
    x_sends[0].start()
    merge_pair(1, 0)
    y_sends[0].start()
    merge_pair(2, 1)
    x_sends[1].start()
    merge_pair(2, 0)
    y_sends[1].start()
    merge_pair(1, 1)
    merge_pair(0, 0)
    merge_pair(0, 1)
    load_wo.start()
    x_sends[0].wait_recv()
    merge(own.at[2, 0], from_x.at[0], 0)
    y_sends[0].wait_recv()
    merge(own.at[1, 1], from_y.at[0], 1)
    y_sends[2].start()
    x_sends[2].start()
    x_sends[1].wait_recv()
    merge(own.at[0, 0], from_x.at[1], 0)
    y_sends[1].wait_recv()
    merge(own.at[0, 1], from_y.at[1], 1)
    y_sends[2].wait_recv()
    merge(own.at[0, 0], from_y.at[2], 0)
    x_sends[2].wait_recv()
    merge(own.at[0, 1], from_x.at[2], 1)
    for h in range(2):
        inv = 1.0 / own[0, h, per, :, 128:256]
        for i in range(per):
            b = h * per + i
            acc = inv[:, b:b + 1] * own[0, h, i]
            for k in range(merged.shape[0]):
                merged[k, b * heads:(b + 1) * heads, :] = acc[:, k * 128:(k + 1) * 128]
    load_uv.wait()
    for h in range(heads):
        o_lat = jnp.concatenate([merged[k, pl.ds(h, n_seqs, stride=heads), :] for k in range(merged.shape[0])], axis=1).astype(jnp.bfloat16)
        o_h = lax.dot_general(o_lat, uv[h], (((1,), (1,)), ((), ())), preferred_element_type=jnp.float32)
        oheads[:, h * o_h.shape[1]:(h + 1) * o_h.shape[1]] = o_h.astype(jnp.bfloat16)
    load_wo.wait()

    def columns(dev, part):
        at, size = parts[part]
        return pl.ds(pl.multiple_of(dev * width + at, 128), size)

    def partial_out(dev, part):
        return jnp.dot(oheads[...], wo[:, columns(dev, part)], preferred_element_type=jnp.float32)

    parts = ((0, width // 256 * 128), (width // 256 * 128, width - width // 256 * 128))
    far = (3, 1, 2)
    p_sends, i_sends, a_sends, f_sends = {}, {}, {}, {}

    def start(waiting):
        while waiting:
            waiting.pop().start()

    def put(ref, part, value):
        ref[:, parts[part][0]:sum(parts[part])] = value

    def get(ref, part):
        return ref[:, parts[part][0]:sum(parts[part])]

    def cut(ref, part):
        return ref.at[:, pl.ds(*parts[part])]

    mine = []
    waiting = []
    for part in range(2):
        for q in far + (0,):
            put(psend.at[q], part, partial_out(device(q, 1), part))
            start(waiting)
            p_sends[q, part] = send(cut(psend.at[q], part), cut(precv.at[q], part), p_ss.at[q, part], p_rs.at[q, part], device(0, 1))
            waiting.append(p_sends[q, part])
        for q in far + (0,):
            value = partial_out(device(q, 0), part)
            start(waiting)
            p_sends[q, part].wait_recv()
            value = value + get(precv.at[q], part)
            if q:
                put(isend.at[q - 1], part, value)
                i_sends[q, part] = send(cut(isend.at[q - 1], part), cut(irecv.at[q - 1], part), i_ss.at[q - 1, part], i_rs.at[q - 1, part], device(q, 0))
                waiting.append(i_sends[q, part])
            else:
                mine.append(value)
        start(waiting)
    for part in range(2):
        for q in far:
            i_sends[q, part].wait_recv()
        result = mine[part] + get(irecv.at[0], part) + get(irecv.at[1], part) + get(irecv.at[2], part)
        put(fin, part, result)
        out_ref[:, columns(me, part)] = result
        for q in far:
            a_sends[q, part] = send(cut(fin, part), cut(agr.at[q - 1], part), a_ss.at[q - 1, part], a_rs.at[q - 1, part], device(q, 0))
            a_sends[q, part].start()
        f_sends[0, part] = send(cut(fin, part), cut(agp.at[0], part), f_ss.at[0, part], f_rs.at[0, part], device(0, 1))
        f_sends[0, part].start()
    for part in range(2):
        for q in (1, 2, 3):
            a_sends[q, part].wait_recv()
            f_sends[q, part] = send(cut(agr.at[q - 1], part), cut(agp.at[q], part), f_ss.at[q, part], f_rs.at[q, part], device(0, 1))
            f_sends[q, part].start()
            out_ref[:, columns(device(q, 0), part)] = get(agr.at[q - 1], part)
    for part in range(2):
        for q in range(4):
            f_sends[q, part].wait_recv()
            out_ref[:, columns(device(q, 1), part)] = get(agp.at[q], part)
    for s in list(d_sends.values()) + x_sends + y_sends + list(p_sends.values()) + list(i_sends.values()) + list(a_sends.values()) + list(f_sends.values()):
        s.wait_send()


def finish(terms, w_uv, w_out):
    n_dev, _, rows, heads, lat_dim = terms.shape
    n_seqs = 2 * (rows - 1)
    d_model = w_out.shape[1]
    depth = w_out.shape[0] // n_dev
    width = d_model // n_dev
    f32 = jnp.float32
    return pl.pallas_call(
        finish_kernel,
        out_shape=jax.ShapeDtypeStruct((n_seqs, d_model), f32),
        in_specs=[ANY, ANY, ANY],
        out_specs=VMEM,
        scratch_shapes=[
            pltpu.VMEM((4, 2, rows, heads, lat_dim), f32),
            pltpu.VMEM((4, 2, rows, heads, lat_dim), f32),
            pltpu.VMEM((3, rows, heads, lat_dim), f32),
            pltpu.VMEM((3, rows, heads, lat_dim), f32),
            pltpu.VMEM((heads,) + w_uv.shape[1:], w_uv.dtype),
            pltpu.VMEM((depth, d_model), w_out.dtype),
            pltpu.VMEM((lat_dim // 128, n_seqs * heads, 128), f32),
            pltpu.VMEM((n_seqs, depth), jnp.bfloat16),
            pltpu.VMEM((4, n_seqs, width), f32),
            pltpu.VMEM((4, n_seqs, width), f32),
            pltpu.VMEM((3, n_seqs, width), f32),
            pltpu.VMEM((3, n_seqs, width), f32),
            pltpu.VMEM((n_seqs, width), f32),
            pltpu.VMEM((3, n_seqs, width), f32),
            pltpu.VMEM((4, n_seqs, width), f32),
            pltpu.SemaphoreType.DMA((2,)),
            pltpu.SemaphoreType.DMA((4, 2)),
            pltpu.SemaphoreType.DMA((4, 2)),
            pltpu.SemaphoreType.DMA((4, 2)),
            pltpu.SemaphoreType.DMA((3,)),
            pltpu.SemaphoreType.DMA((3,)),
            pltpu.SemaphoreType.DMA((3,)),
            pltpu.SemaphoreType.DMA((3,)),
            pltpu.SemaphoreType.DMA((4, 2)),
            pltpu.SemaphoreType.DMA((4, 2)),
            pltpu.SemaphoreType.DMA((3, 2)),
            pltpu.SemaphoreType.DMA((3, 2)),
            pltpu.SemaphoreType.DMA((3, 2)),
            pltpu.SemaphoreType.DMA((3, 2)),
            pltpu.SemaphoreType.DMA((4, 2)),
            pltpu.SemaphoreType.DMA((4, 2)),
        ],
        compiler_params=pltpu.CompilerParams(collective_id=0, has_side_effects=True, vmem_limit_bytes=56 * 1024 * 1024),
        name="finish",
    )(terms, w_uv, w_out)


def solution(mesh):
    n_dev = mesh.shape['sp']

    def local_step(hidden, ckv_blk, kpe_blk, cache_len, w_dq, q_gain, w_uq, w_dkv, kv_gain, w_uk, w_uv, w_out):
        q, kvn = project(hidden, cache_len, w_dq, q_gain, w_uq, w_dkv, kv_gain, w_uk)
        qk_dim = w_uk.shape[1] + kpe_blk.shape[2]
        ckv_out, kpe_out_t, terms, kv_new = attend(q, kvn, cache_len, ckv_blk, jnp.swapaxes(kpe_blk, 1, 2), n_dev, qk_dim)
        out = finish(terms, w_uv, w_out).astype(jnp.bfloat16)
        return out, ckv_out, jnp.swapaxes(kpe_out_t, 1, 2), kv_new

    cache_spec = P('dp', 'sp', None)
    return jax.shard_map(local_step, mesh=mesh, in_specs=(P('dp', None), cache_spec, cache_spec, P('dp'), P(), P(), P(), P(), P(), P(), P(), P()), out_specs=(P('dp', None), cache_spec, cache_spec, P('dp', None)), check_vma=False)
```

```python
import functools

import jax
import jax.numpy as jnp
import numpy as np
from jax import lax
from jax.experimental import pallas as pl
from jax.experimental.pallas import tpu as pltpu
from jax.sharding import PartitionSpec as P

EPS = 1e-6
ROPE_THETA = 10000.0
NEG_FILL = -1e30
MESH = pl.DeviceIdType.MESH
VMEM = pl.BlockSpec(memory_space=pltpu.VMEM)
SMEM = pl.BlockSpec(memory_space=pltpu.SMEM)
HBM = pl.BlockSpec(memory_space=pltpu.HBM)


def project_kernel(cfg, len_ref, hidden, w_dq, w_dkv_t, w_uq, w_uk, q_gain_ref, kv_gain_ref, freq, q_out, kvn_out,
                   dq, dkv, uq, uk, halves, q_mine, q_theirs, turn, dq_sem, dkv_sem, uq_sem, uk_sem, h_ss, h_rs, q_ss, q_rs):
    n_seqs = hidden.shape[0]
    n_k, k_rows, dq_cols = dq.shape
    n_blk, _, blk = uq.shape
    dkv_cols = dkv.shape[0]
    n_kt = cfg["n_kt"]
    k_tile = dkv.shape[1] // n_kt
    lat_dim = cfg["lat_dim"]
    nope_dim = uk.shape[1]
    heads = uk.shape[0]
    half_heads = heads // 2
    group, pitch = cfg["group"], cfg["pitch"]
    me = lax.axis_index('sp')
    c = me % 2
    partner = me - c + (1 - c)
    f32 = jnp.float32

    def load_dq(k):
        return pltpu.make_async_copy(w_dq.at[pl.ds(k * k_rows, k_rows), pl.ds(pl.multiple_of(c * dq_cols, 128), dq_cols)], dq.at[k], dq_sem.at[k])

    def load_dkv(k):
        return pltpu.make_async_copy(w_dkv_t.at[pl.ds(pl.multiple_of(c * (lat_dim // 2), 16), dkv_cols), pl.ds(k * k_tile, k_tile)], dkv.at[:, pl.ds(k * k_tile, k_tile)], dkv_sem.at[k])

    def load_uq(k):
        return pltpu.make_async_copy(w_uq.at[:, pl.ds(pl.multiple_of((c * n_blk + k) * blk, 128), blk)], uq.at[k], uq_sem.at[k])

    def load_uk(k):
        first = (c * half_heads + k * group) % heads
        return pltpu.make_async_copy(w_uk.at[pl.ds(first, group)], uk.at[pl.ds(k * group, group)], uk_sem.at[k])

    n_grp = heads // group
    per_kt = n_k // n_kt
    per_grp = n_blk // (n_grp // 2)
    loads = []
    for k in range(n_k):
        loads.append(load_dq(k))
        if k % per_kt == 0:
            loads.append(load_dkv(k // per_kt))
    for k in range(n_blk):
        loads.append(load_uq(k))
        if k % per_grp == 0:
            loads.append(load_uk(k // per_grp))
        if k >= cfg["behind"] and (k - cfg["behind"]) % per_grp == 0:
            loads.append(load_uk(n_grp // 2 + (k - cfg["behind"]) // per_grp))
    in_flight = cfg["in_flight"]
    for load in loads[:in_flight]:
        load.start()
    queue = loads[in_flight:]

    def wait_load(load):
        load.wait()
        if queue:
            queue.pop(0).start()

    barrier = pltpu.get_barrier_semaphore()
    pl.semaphore_signal(barrier, inc=1, device_id={'sp': partner}, device_id_type=MESH)
    pl.semaphore_wait(barrier, 1)

    lane = lax.broadcasted_iota(jnp.int32, (n_seqs, 128), 1)
    row = lax.broadcasted_iota(jnp.int32, (n_seqs, 128), 0)
    position = jnp.zeros((n_seqs, 128), f32)
    for b in range(n_seqs):
        position = jnp.where(row == b, len_ref[b].astype(f32), position)
    angle = position * freq[...]
    cos_t = jnp.cos(angle)
    sin_t = jnp.where(lane % 64 < 32, -jnp.sin(angle), jnp.sin(angle))
    q_gain = q_gain_ref[...].astype(f32).reshape(1, -1)
    kv_gain = kv_gain_ref[...].astype(f32).reshape(1, -1)

    acc_q = jnp.zeros((n_seqs, dq_cols), f32)
    acc_kv = jnp.zeros((n_seqs, dkv_cols), f32)
    for k in range(n_k):
        wait_load(load_dq(k))
        acc_q = acc_q + jnp.dot(hidden[:, k * k_rows:(k + 1) * k_rows], dq[k], preferred_element_type=f32)
        if k % per_kt == per_kt - 1:
            t = k // per_kt
            wait_load(load_dkv(t))
            cols = slice(t * k_tile, (t + 1) * k_tile)
            acc_kv = acc_kv + lax.dot_general(hidden[:, cols], dkv[:, cols], (((1,), (1,)), ((), ())), preferred_element_type=f32)
    halves[c, :, dq_cols + lat_dim // 2:] = jnp.zeros((n_seqs, 128), f32)
    halves[c, :, :dq_cols] = acc_q
    halves[c, :, dq_cols:dq_cols + dkv_cols] = acc_kv
    swap = pltpu.make_async_remote_copy(src_ref=halves.at[c], dst_ref=halves.at[c], send_sem=h_ss, recv_sem=h_rs, device_id={'sp': partner}, device_id_type=MESH)
    swap.start()
    swap.wait_recv()

    lo, hi = halves[0], halves[1]
    raw_q = [lo[:, :dq_cols], hi[:, :dq_cols]]
    mean_sq = sum(jnp.sum(r * r, axis=1, keepdims=True) for r in raw_q) / (2 * dq_cols)
    inv = lax.rsqrt(mean_sq + EPS)
    c_q = jnp.concatenate([r * inv * q_gain[:, i * dq_cols:(i + 1) * dq_cols] for i, r in enumerate(raw_q)], axis=1).astype(jnp.bfloat16)

    def rotate_pair(pair):
        other = jnp.where(lane % 64 < 32, pltpu.roll(pair, 96, 1), pltpu.roll(pair, 32, 1))
        return pair * cos_t + other * sin_t

    def emit(q_blk, k, side):
        for p in range(blk // 384):
            t0, t1, t2 = (q_blk[:, p * 384 + i * 128:p * 384 + (i + 1) * 128] for i in range(3))
            odd = jnp.where(lane < 64, pltpu.roll(t1, 64, 1), pltpu.roll(t2, 64, 1))
            pe = rotate_pair(jnp.where(lane < 64, t1, t2))
            for i, (nope, rope) in enumerate(((t0, pe), (odd, pltpu.roll(pe, 64, 1)))):
                h = k * (blk // 192) + p * 2 + i
                lat = jnp.dot(nope.astype(jnp.bfloat16), uk[side * half_heads + h], preferred_element_type=f32)
                first = (h % group) * pitch
                for j in range(lat_dim // 128):
                    turn[side, j, first:first + n_seqs, :] = lat[:, j * 128:(j + 1) * 128]
                turn[side, lat_dim // 128, first:first + n_seqs, :] = rope

    def flush(first, side):
        rows = pl.ds(pl.multiple_of(first, group), group)
        for b in range(n_seqs):
            for j in range(lat_dim // 128 + 1):
                q_out[b, rows, j * 128:(j + 1) * 128] = turn[side, j, pl.ds(b, group, stride=pitch), :].astype(q_out.dtype)

    sends = []

    def own_block(k):
        wait_load(load_uq(k))
        q_blk = jnp.dot(c_q, uq[k], preferred_element_type=f32).astype(jnp.bfloat16).astype(f32)
        q_mine[k] = q_blk
        sends.append(pltpu.make_async_remote_copy(src_ref=q_mine.at[k], dst_ref=q_theirs.at[k], send_sem=q_ss.at[k], recv_sem=q_rs.at[k], device_id={'sp': partner}, device_id_type=MESH))
        if k % per_grp == 0:
            wait_load(load_uk(k // per_grp))
        emit(q_blk, k, 0)
        sends[k].start()
        if k % per_grp == per_grp - 1:
            flush(c * half_heads + (k // per_grp) * group, 0)

    def their_block(k):
        sends[k].wait_recv()
        if k % per_grp == 0:
            wait_load(load_uk(n_grp // 2 + k // per_grp))
        emit(q_theirs[k], k, 1)
        if k % per_grp == per_grp - 1:
            flush((1 - c) * half_heads + (k // per_grp) * group, 1)

    behind = cfg["behind"]
    for k in range(n_blk):
        own_block(k)
        if k >= behind:
            their_block(k - behind)
    raw_kv = [lo[:, dq_cols:dq_cols + lat_dim // 2], hi[:, dq_cols:dq_cols + lat_dim // 2]]
    mean_sq = sum(jnp.sum(r * r, axis=1, keepdims=True) for r in raw_kv) / lat_dim
    inv = lax.rsqrt(mean_sq + EPS)
    c_kv = jnp.concatenate([r * inv * kv_gain[:, i * (lat_dim // 2):(i + 1) * (lat_dim // 2)] for i, r in enumerate(raw_kv)], axis=1).astype(jnp.bfloat16)
    k_pe = rotate_pair(hi[:, dq_cols + lat_dim // 2:]).astype(jnp.bfloat16)
    kvn_out[:, :lat_dim] = c_kv.astype(f32)
    kvn_out[:, lat_dim:] = k_pe.astype(f32)

    for k in range(n_blk - behind, n_blk):
        their_block(k)
    swap.wait_send()
    for s in sends:
        s.wait_send()


def project(hidden, cache_len, w_dq, q_gain, w_uq, w_dkv, kv_gain, w_uk):
    n_seqs, d_model = hidden.shape
    heads, nope_dim, lat_dim = w_uk.shape
    q_rank = w_dq.shape[1]
    rope_dim = w_dkv.shape[1] - lat_dim
    freq = np.power(ROPE_THETA, -2.0 * np.arange(rope_dim // 2) / rope_dim).astype(np.float32)
    freq = jnp.asarray(np.tile(freq, 128 // freq.size).reshape(1, 128))
    cfg = dict(n_kt=4, lat_dim=lat_dim, group=16, pitch=n_seqs + 8, in_flight=4, behind=2)
    n_k, n_blk = 8, 8
    dq_cols, dkv_cols = q_rank // 2, lat_dim // 2 + rope_dim
    blk = w_uq.shape[1] // 2 // n_blk
    f32, bf16 = jnp.float32, jnp.bfloat16
    dma = pltpu.SemaphoreType.DMA
    return pl.pallas_call(
        functools.partial(project_kernel, cfg),
        out_shape=(
            jax.ShapeDtypeStruct((n_seqs, heads, lat_dim + 128), bf16),
            jax.ShapeDtypeStruct((n_seqs, lat_dim + 128), f32),
        ),
        in_specs=[SMEM, VMEM, HBM, HBM, HBM, HBM, VMEM, VMEM, VMEM],
        out_specs=(VMEM, VMEM),
        scratch_shapes=[
            pltpu.VMEM((n_k, d_model // n_k, dq_cols), bf16),
            pltpu.VMEM((dkv_cols, d_model), bf16),
            pltpu.VMEM((n_blk, q_rank, blk), bf16),
            pltpu.VMEM((heads, nope_dim, lat_dim), bf16),
            pltpu.VMEM((2, n_seqs, dq_cols + lat_dim // 2 + 128), f32),
            pltpu.VMEM((n_blk, n_seqs, blk), f32),
            pltpu.VMEM((n_blk, n_seqs, blk), f32),
            pltpu.VMEM((2, lat_dim // 128 + 1, cfg["group"] * cfg["pitch"], 128), f32),
            dma((n_k,)), dma((cfg["n_kt"],)), dma((n_blk,)), dma((heads // cfg["group"],)),
            dma, dma, dma((n_blk,)), dma((n_blk,)),
        ],
        compiler_params=pltpu.CompilerParams(collective_id=1, has_side_effects=True, vmem_limit_bytes=48 * 1024 * 1024),
        name="project",
    )(cache_len, hidden, w_dq, w_dkv.T, w_uq, w_uk, q_gain, kv_gain, freq)


def attend_kernel(cfg, len_ref, q_ref, kvn_ref, ckv_hbm, kpe_hbm, cout_hbm, kout_hbm, terms, kv_new,
                  cbuf, kbuf, peaks, denoms, isem, osem):
    n_seqs, shard_len = ckv_hbm.shape[0], ckv_hbm.shape[1]
    lat_dim = ckv_hbm.shape[2]
    rope_dim = kpe_hbm.shape[1]
    per = terms.shape[2] - 1
    n_buf, lag, chunk = cfg["n_buf"], cfg["lag"], cfg["chunk"]
    base = lax.axis_index('sp') * shard_len

    def copies_in(b, slot):
        return (pltpu.make_async_copy(ckv_hbm.at[b], cbuf.at[slot], isem.at[slot, 0]),
                pltpu.make_async_copy(kpe_hbm.at[b], kbuf.at[slot], isem.at[slot, 1]))

    def copies_out(b, slot):
        return (pltpu.make_async_copy(cbuf.at[slot], cout_hbm.at[b], osem.at[slot, 0]),
                pltpu.make_async_copy(kbuf.at[slot], kout_hbm.at[b], osem.at[slot, 1]))

    for i in range(n_buf - lag):
        for c in copies_in(i, i):
            c.start()
    kv_new[...] = kvn_ref[:, :lat_dim + rope_dim].astype(kv_new.dtype)
    peaks[...] = jnp.zeros_like(peaks)
    denoms[...] = jnp.zeros_like(denoms)

    def step(b, carry):
        slot = lax.rem(b, n_buf)

        @pl.when(b >= lag)
        def _():
            for c in copies_out(b - lag, lax.rem(b - lag + n_buf, n_buf)):
                c.wait()

        ahead = b - lag + n_buf

        @pl.when(ahead < n_seqs)
        def _():
            for c in copies_in(ahead, lax.rem(ahead, n_buf)):
                c.start()

        for c in copies_in(b, slot):
            c.wait()
        last = len_ref[b] - base

        @pl.when((last >= 0) & (last < shard_len))
        def _():
            picked = lax.broadcasted_iota(jnp.int32, kvn_ref.shape, 0) == b
            fresh_row = jnp.sum(jnp.where(picked, kvn_ref[...], 0.0), axis=0, keepdims=True)
            r0 = pl.multiple_of((last // 16) * 16, 16)
            rows = cbuf[slot, pl.ds(r0, 16), :].astype(jnp.float32)
            row = lax.broadcasted_iota(jnp.int32, rows.shape, 0)
            cbuf[slot, pl.ds(r0, 16), :] = jnp.where(row == last - r0, fresh_row[:, :lat_dim], rows).astype(cbuf.dtype)
            c0 = pl.multiple_of((last // 128) * 128, 128)
            cols = kbuf[slot, :, pl.ds(c0, 128)].astype(jnp.float32)
            lane = lax.broadcasted_iota(jnp.int32, cols.shape, 1)
            diag = lane == lax.broadcasted_iota(jnp.int32, cols.shape, 0)
            fresh = jnp.sum(jnp.where(diag, fresh_row[:, lat_dim:], 0.0), axis=1, keepdims=True)
            kbuf[slot, :, pl.ds(c0, 128)] = jnp.where(lane == last - c0, fresh, cols).astype(kbuf.dtype)

        q_lat, q_pe = q_ref[b, :, :lat_dim], q_ref[b, :, lat_dim:lat_dim + rope_dim]
        scores = []
        for t in range(0, shard_len, chunk):
            s = lax.dot_general(q_lat, cbuf[slot, t:t + chunk, :], (((1,), (1,)), ((), ())), preferred_element_type=jnp.float32)
            s = s + jnp.dot(q_pe, kbuf[slot, :, t:t + chunk], preferred_element_type=jnp.float32)
            pos = lax.broadcasted_iota(jnp.int32, (1, chunk), 1) + t
            scores.append(jnp.where(pos <= last, s * cfg["scale"], NEG_FILL))
        peak = functools.reduce(jnp.maximum, [jnp.max(s, axis=1, keepdims=True) for s in scores])
        denom = jnp.zeros_like(peak)
        lat_sum = None
        for k, t in enumerate(range(0, shard_len, chunk)):
            w = jnp.exp(scores[k] - peak)
            denom = denom + jnp.sum(w, axis=1, keepdims=True)
            term = jnp.dot(w.astype(jnp.bfloat16), cbuf[slot, t:t + chunk, :], preferred_element_type=jnp.float32)
            lat_sum = term if lat_sum is None else lat_sum + term
        for c in copies_out(b, slot):
            c.start()
        terms[:, b // per, b % per] = lat_sum.reshape(terms.shape[0], *terms.shape[3:])
        lane = lax.broadcasted_iota(jnp.int32, peaks.shape, 1)
        peaks[...] = jnp.where(lane == b, peak, peaks[...])
        denoms[...] = jnp.where(lane == b, denom, denoms[...])
        return carry

    lax.fori_loop(0, n_seqs, step, 0)
    for part in range(2):
        terms[:, part, per, :, :128] = peaks[...].reshape(terms.shape[0], terms.shape[3], 128)
        terms[:, part, per, :, 128:256] = denoms[...].reshape(terms.shape[0], terms.shape[3], 128)
    for i in range(n_seqs - lag, n_seqs):
        for c in copies_out(i, i % n_buf):
            c.wait()


def attend(q, kvn, cache_len, ckv_blk, kpe_blk_t, n_dev, qk_dim):
    n_seqs, shard_len, lat_dim = ckv_blk.shape
    rope_dim = kpe_blk_t.shape[1]
    n_heads = q.shape[1]
    cfg = dict(n_buf=8, lag=3, chunk=512, scale=qk_dim ** -0.5)
    terms_shape = (n_dev, 2, n_seqs // 2 + 1, n_heads // n_dev, lat_dim)
    return pl.pallas_call(
        functools.partial(attend_kernel, cfg),
        out_shape=(
            jax.ShapeDtypeStruct(ckv_blk.shape, ckv_blk.dtype),
            jax.ShapeDtypeStruct(kpe_blk_t.shape, kpe_blk_t.dtype),
            jax.ShapeDtypeStruct(terms_shape, jnp.float32),
            jax.ShapeDtypeStruct((n_seqs, lat_dim + rope_dim), ckv_blk.dtype),
        ),
        in_specs=[SMEM, VMEM, VMEM, HBM, HBM],
        out_specs=(HBM, HBM, VMEM, VMEM),
        scratch_shapes=[
            pltpu.VMEM((cfg["n_buf"], shard_len, lat_dim), ckv_blk.dtype),
            pltpu.VMEM((cfg["n_buf"], rope_dim, shard_len), kpe_blk_t.dtype),
            pltpu.VMEM((n_heads, 128), jnp.float32),
            pltpu.VMEM((n_heads, 128), jnp.float32),
            pltpu.SemaphoreType.DMA((cfg["n_buf"], 2)),
            pltpu.SemaphoreType.DMA((cfg["n_buf"], 2)),
        ],
        compiler_params=pltpu.CompilerParams(vmem_limit_bytes=44 * 1024 * 1024),
        name="attend",
    )(cache_len, q, kvn, ckv_blk, kpe_blk_t)


def finish_kernel(terms, w_uv, w_out, out_ref, own, pair, from_x, from_y, uv, wo, merged, oheads, psend, precv, isend, irecv, fin, agr, agp,
                  lsem, own_sem, d_ss, d_rs, x_ss, x_rs, y_ss, y_rs, p_ss, p_rs, i_ss, i_rs, a_ss, a_rs, f_ss, f_rs):
    n_seqs, width = fin.shape
    heads = uv.shape[0]
    depth = wo.shape[0]
    me = lax.axis_index('sp')
    y, x, c = me // 4, (me // 2) % 2, me % 2

    def device(q, jc):
        return ((y + q // 2) % 2) * 4 + ((x + q % 2) % 2) * 2 + (c + jc) % 2

    def send(src, dst, ss, rs, dev):
        return pltpu.make_async_remote_copy(src_ref=src, dst_ref=dst, send_sem=ss, recv_sem=rs, device_id={'sp': dev}, device_id_type=MESH)

    load_uv = pltpu.make_async_copy(w_uv.at[pl.ds(me * heads, heads)], uv, lsem.at[0])
    load_wo = pltpu.make_async_copy(w_out.at[pl.ds(me * depth, depth)], wo, lsem.at[1])
    order = ((3, 0), (3, 1), (1, 0), (2, 1), (2, 0), (1, 1), (0, 0), (0, 1))
    per = n_seqs // 2
    loads = {(q, h): pltpu.make_async_copy(terms.at[device(q, 0), h], own.at[q, h], own_sem.at[q, h]) for q, h in order}
    for k in order:
        loads[k].start()
    load_uv.start()

    others = ((0, 1), (1, 0), (2, 0), (3, 0))
    barrier = pltpu.get_barrier_semaphore()
    for q, jc in others:
        pl.semaphore_signal(barrier, inc=1, device_id={'sp': device(q, jc)}, device_id_type=MESH)
    pl.semaphore_wait(barrier, len(others))

    d_sends = {(q, h): send(terms.at[device(q, 1), h], pair.at[q, h], d_ss.at[q, h], d_rs.at[q, h], device(0, 1)) for q, h in order}
    for k in order:
        d_sends[k].start()

    def merge(dst, src, h):
        old, new = dst[per, :, :128], src[per, :, :128]
        peak = jnp.maximum(old, new)
        f_old, f_new = jnp.exp(old - peak), jnp.exp(new - peak)
        dst[per, :, :128] = peak
        dst[per, :, 128:256] = f_old * dst[per, :, 128:256] + f_new * src[per, :, 128:256]
        for i in range(per):
            b = h * per + i
            dst[i] = f_old[:, b:b + 1] * dst[i] + f_new[:, b:b + 1] * src[i]

    def merge_pair(q, h):
        loads[q, h].wait()
        d_sends[q, h].wait_recv()
        merge(own.at[q, h], pair.at[q, h], h)

    x_dev, y_dev = device(1, 0), device(2, 0)
    x_sends = [send(own.at[k], from_x.at[i], x_ss.at[i], x_rs.at[i], x_dev) for i, k in enumerate(((3, 0), (1, 0), (1, 1)))]
    y_sends = [send(own.at[k], from_y.at[i], y_ss.at[i], y_rs.at[i], y_dev) for i, k in enumerate(((3, 1), (2, 1), (2, 0)))]
    merge_pair(3, 0)
    merge_pair(3, 1)
    x_sends[0].start()
    merge_pair(1, 0)
    y_sends[0].start()
    merge_pair(2, 1)
    x_sends[1].start()
    merge_pair(2, 0)
    y_sends[1].start()
    merge_pair(1, 1)
    merge_pair(0, 0)
    merge_pair(0, 1)
    load_wo.start()
    x_sends[0].wait_recv()
    merge(own.at[2, 0], from_x.at[0], 0)
    y_sends[0].wait_recv()
    merge(own.at[1, 1], from_y.at[0], 1)
    y_sends[2].start()
    x_sends[2].start()
    x_sends[1].wait_recv()
    merge(own.at[0, 0], from_x.at[1], 0)
    y_sends[1].wait_recv()
    merge(own.at[0, 1], from_y.at[1], 1)
    y_sends[2].wait_recv()
    merge(own.at[0, 0], from_y.at[2], 0)
    x_sends[2].wait_recv()
    merge(own.at[0, 1], from_x.at[2], 1)
    for h in range(2):
        inv = 1.0 / own[0, h, per, :, 128:256]
        for i in range(per):
            b = h * per + i
            acc = inv[:, b:b + 1] * own[0, h, i]
            for k in range(merged.shape[0]):
                merged[k, b * heads:(b + 1) * heads, :] = acc[:, k * 128:(k + 1) * 128]
    load_uv.wait()
    for h in range(heads):
        o_lat = jnp.concatenate([merged[k, pl.ds(h, n_seqs, stride=heads), :] for k in range(merged.shape[0])], axis=1).astype(jnp.bfloat16)
        o_h = lax.dot_general(o_lat, uv[h], (((1,), (1,)), ((), ())), preferred_element_type=jnp.float32)
        oheads[:, h * o_h.shape[1]:(h + 1) * o_h.shape[1]] = o_h.astype(jnp.bfloat16)
    load_wo.wait()

    def columns(dev, part):
        at, size = parts[part]
        return pl.ds(pl.multiple_of(dev * width + at, 128), size)

    def partial_out(dev, part):
        return jnp.dot(oheads[...], wo[:, columns(dev, part)], preferred_element_type=jnp.float32)

    parts = ((0, width // 256 * 128), (width // 256 * 128, width - width // 256 * 128))
    far = (3, 1, 2)
    p_sends, i_sends, a_sends, f_sends = {}, {}, {}, {}

    def start(waiting):
        while waiting:
            waiting.pop().start()

    def put(ref, part, value):
        ref[:, parts[part][0]:sum(parts[part])] = value

    def get(ref, part):
        return ref[:, parts[part][0]:sum(parts[part])]

    def cut(ref, part):
        return ref.at[:, pl.ds(*parts[part])]

    mine = []
    waiting = []
    for part in range(2):
        for q in far + (0,):
            put(psend.at[q], part, partial_out(device(q, 1), part))
            start(waiting)
            p_sends[q, part] = send(cut(psend.at[q], part), cut(precv.at[q], part), p_ss.at[q, part], p_rs.at[q, part], device(0, 1))
            waiting.append(p_sends[q, part])
        for q in far + (0,):
            value = partial_out(device(q, 0), part)
            start(waiting)
            p_sends[q, part].wait_recv()
            value = value + get(precv.at[q], part)
            if q:
                put(isend.at[q - 1], part, value)
                i_sends[q, part] = send(cut(isend.at[q - 1], part), cut(irecv.at[q - 1], part), i_ss.at[q - 1, part], i_rs.at[q - 1, part], device(q, 0))
                waiting.append(i_sends[q, part])
            else:
                mine.append(value)
        start(waiting)
    for part in range(2):
        for q in far:
            i_sends[q, part].wait_recv()
        result = mine[part] + get(irecv.at[0], part) + get(irecv.at[1], part) + get(irecv.at[2], part)
        put(fin, part, result)
        out_ref[:, columns(me, part)] = result
        for q in far:
            a_sends[q, part] = send(cut(fin, part), cut(agr.at[q - 1], part), a_ss.at[q - 1, part], a_rs.at[q - 1, part], device(q, 0))
            a_sends[q, part].start()
        f_sends[0, part] = send(cut(fin, part), cut(agp.at[0], part), f_ss.at[0, part], f_rs.at[0, part], device(0, 1))
        f_sends[0, part].start()
    for part in range(2):
        for q in (1, 2, 3):
            a_sends[q, part].wait_recv()
            f_sends[q, part] = send(cut(agr.at[q - 1], part), cut(agp.at[q], part), f_ss.at[q, part], f_rs.at[q, part], device(0, 1))
            f_sends[q, part].start()
            out_ref[:, columns(device(q, 0), part)] = get(agr.at[q - 1], part)
    for part in range(2):
        for q in range(4):
            f_sends[q, part].wait_recv()
            out_ref[:, columns(device(q, 1), part)] = get(agp.at[q], part)
    for s in list(d_sends.values()) + x_sends + y_sends + list(p_sends.values()) + list(i_sends.values()) + list(a_sends.values()) + list(f_sends.values()):
        s.wait_send()


def finish(terms, w_uv, w_out):
    n_dev, _, rows, heads, lat_dim = terms.shape
    n_seqs = 2 * (rows - 1)
    d_model = w_out.shape[1]
    depth = w_out.shape[0] // n_dev
    width = d_model // n_dev
    f32 = jnp.float32
    return pl.pallas_call(
        finish_kernel,
        out_shape=jax.ShapeDtypeStruct((n_seqs, d_model), f32),
        in_specs=[VMEM, HBM, HBM],
        out_specs=VMEM,
        scratch_shapes=[
            pltpu.VMEM((4, 2, rows, heads, lat_dim), f32),
            pltpu.VMEM((4, 2, rows, heads, lat_dim), f32),
            pltpu.VMEM((3, rows, heads, lat_dim), f32),
            pltpu.VMEM((3, rows, heads, lat_dim), f32),
            pltpu.VMEM((heads,) + w_uv.shape[1:], w_uv.dtype),
            pltpu.VMEM((depth, d_model), w_out.dtype),
            pltpu.VMEM((lat_dim // 128, n_seqs * heads, 128), f32),
            pltpu.VMEM((n_seqs, depth), jnp.bfloat16),
            pltpu.VMEM((4, n_seqs, width), f32),
            pltpu.VMEM((4, n_seqs, width), f32),
            pltpu.VMEM((3, n_seqs, width), f32),
            pltpu.VMEM((3, n_seqs, width), f32),
            pltpu.VMEM((n_seqs, width), f32),
            pltpu.VMEM((3, n_seqs, width), f32),
            pltpu.VMEM((4, n_seqs, width), f32),
            pltpu.SemaphoreType.DMA((2,)),
            pltpu.SemaphoreType.DMA((4, 2)),
            pltpu.SemaphoreType.DMA((4, 2)),
            pltpu.SemaphoreType.DMA((4, 2)),
            pltpu.SemaphoreType.DMA((3,)),
            pltpu.SemaphoreType.DMA((3,)),
            pltpu.SemaphoreType.DMA((3,)),
            pltpu.SemaphoreType.DMA((3,)),
            pltpu.SemaphoreType.DMA((4, 2)),
            pltpu.SemaphoreType.DMA((4, 2)),
            pltpu.SemaphoreType.DMA((3, 2)),
            pltpu.SemaphoreType.DMA((3, 2)),
            pltpu.SemaphoreType.DMA((3, 2)),
            pltpu.SemaphoreType.DMA((3, 2)),
            pltpu.SemaphoreType.DMA((4, 2)),
            pltpu.SemaphoreType.DMA((4, 2)),
        ],
        compiler_params=pltpu.CompilerParams(collective_id=0, has_side_effects=True, vmem_limit_bytes=48 * 1024 * 1024),
        name="finish",
    )(terms, w_uv, w_out)


def solution(mesh):
    n_dev = mesh.shape['sp']

    def local_step(hidden, ckv_blk, kpe_blk, cache_len, w_dq, q_gain, w_uq, w_dkv, kv_gain, w_uk, w_uv, w_out):
        q, kvn = project(hidden, cache_len, w_dq, q_gain, w_uq, w_dkv, kv_gain, w_uk)
        qk_dim = w_uk.shape[1] + kpe_blk.shape[2]
        ckv_out, kpe_out_t, terms, kv_new = attend(q, kvn, cache_len, ckv_blk, jnp.swapaxes(kpe_blk, 1, 2), n_dev, qk_dim)
        out = finish(terms, w_uv, w_out).astype(jnp.bfloat16)
        return out, ckv_out, jnp.swapaxes(kpe_out_t, 1, 2), kv_new

    cache_spec = P('dp', 'sp', None)
    return jax.shard_map(local_step, mesh=mesh, in_specs=(P('dp', None), cache_spec, cache_spec, P('dp'), P(), P(), P(), P(), P(), P(), P(), P()), out_specs=(P('dp', None), cache_spec, cache_spec, P('dp', None)), check_vma=False)
```

```python
import functools

import jax
import jax.numpy as jnp
import numpy as np
from jax import lax
from jax.experimental import pallas as pl
from jax.experimental.pallas import tpu as pltpu
from jax.sharding import PartitionSpec as P

EPS = 1e-6
ROPE_THETA = 10000.0
NEG_FILL = -1e30
MESH = pl.DeviceIdType.MESH
VMEM = pl.BlockSpec(memory_space=pltpu.VMEM)
SMEM = pl.BlockSpec(memory_space=pltpu.SMEM)
HBM = pl.BlockSpec(memory_space=pltpu.HBM)


def project_kernel(cfg, small_ref, hidden, w_dq, w_dkv_t, w_uq, w_uk, q_out, kvn_out,
                   dq, dkv, uq, uk, halves, q_mine, q_theirs, turn, dq_sem, dkv_sem, uq_sem, uk_sem, h_ss, h_rs, q_ss, q_rs):
    n_seqs = hidden.shape[0]
    n_k, k_rows, dq_cols = dq.shape
    n_blk, _, blk = uq.shape
    dkv_cols = dkv.shape[0]
    n_kt = cfg["n_kt"]
    k_tile = dkv.shape[1] // n_kt
    lat_dim = cfg["lat_dim"]
    nope_dim = uk.shape[1]
    heads = uk.shape[0]
    half_heads = heads // 2
    group, pitch = cfg["group"], cfg["pitch"]
    me = lax.axis_index('sp')
    c = me % 2
    partner = me - c + (1 - c)
    f32 = jnp.float32

    def load_dq(k):
        return pltpu.make_async_copy(w_dq.at[pl.ds(k * k_rows, k_rows), pl.ds(pl.multiple_of(c * dq_cols, 128), dq_cols)], dq.at[k], dq_sem.at[k])

    def load_dkv(k):
        return pltpu.make_async_copy(w_dkv_t.at[pl.ds(pl.multiple_of(c * (lat_dim // 2), 16), dkv_cols), pl.ds(k * k_tile, k_tile)], dkv.at[:, pl.ds(k * k_tile, k_tile)], dkv_sem.at[k])

    def load_uq(k):
        return pltpu.make_async_copy(w_uq.at[:, pl.ds(pl.multiple_of((c * n_blk + k) * blk, 128), blk)], uq.at[k], uq_sem.at[k])

    def load_uk(k):
        first = (c * half_heads + k * group) % heads
        return pltpu.make_async_copy(w_uk.at[pl.ds(first, group)], uk.at[pl.ds(k * group, group)], uk_sem.at[k])

    n_grp = heads // group
    per_kt = n_k // n_kt
    per_grp = n_blk // (n_grp // 2)
    loads = []
    for k in range(n_k):
        loads.append(load_dq(k))
        if k % per_kt == 0:
            loads.append(load_dkv(k // per_kt))
    for k in range(n_blk):
        loads.append(load_uq(k))
        if k % per_grp == 0:
            loads.append(load_uk(k // per_grp))
        if k >= cfg["behind"] and (k - cfg["behind"]) % per_grp == 0:
            loads.append(load_uk(n_grp // 2 + (k - cfg["behind"]) // per_grp))
    in_flight = cfg["in_flight"]
    for load in loads[:in_flight]:
        load.start()
    queue = loads[in_flight:]

    def wait_load(load):
        load.wait()
        if queue:
            queue.pop(0).start()

    barrier = pltpu.get_barrier_semaphore()
    pl.semaphore_signal(barrier, inc=1, device_id={'sp': partner}, device_id_type=MESH)
    pl.semaphore_wait(barrier, 1)

    lane = lax.broadcasted_iota(jnp.int32, (n_seqs, 128), 1)
    row = lax.broadcasted_iota(jnp.int32, (n_seqs, 128), 0)
    small = small_ref[...].reshape(1, -1)
    q_gain, kv_gain, lengths = small[:, :2 * dq_cols], small[:, 2 * dq_cols:2 * dq_cols + lat_dim], small[:, 2 * dq_cols + lat_dim:]
    position = jnp.sum(jnp.where(lane == row, lengths, 0.0), axis=1, keepdims=True)
    freq = jnp.zeros((n_seqs, 128), f32)
    for i, value in enumerate(cfg["freqs"]):
        freq = jnp.where(lane % 32 == i, value, freq)
    angle = position * freq
    cos_t = jnp.cos(angle)
    sin_t = jnp.where(lane % 64 < 32, -jnp.sin(angle), jnp.sin(angle))

    acc_q = jnp.zeros((n_seqs, dq_cols), f32)
    acc_kv = jnp.zeros((n_seqs, dkv_cols), f32)
    for k in range(n_k):
        wait_load(load_dq(k))
        acc_q = acc_q + jnp.dot(hidden[:, k * k_rows:(k + 1) * k_rows], dq[k], preferred_element_type=f32)
        if k % per_kt == per_kt - 1:
            t = k // per_kt
            wait_load(load_dkv(t))
            cols = slice(t * k_tile, (t + 1) * k_tile)
            acc_kv = acc_kv + lax.dot_general(hidden[:, cols], dkv[:, cols], (((1,), (1,)), ((), ())), preferred_element_type=f32)
    halves[c, :, dq_cols + lat_dim // 2:] = jnp.zeros((n_seqs, 128), f32)
    halves[c, :, :dq_cols] = acc_q
    halves[c, :, dq_cols:dq_cols + dkv_cols] = acc_kv
    swap = pltpu.make_async_remote_copy(src_ref=halves.at[c], dst_ref=halves.at[c], send_sem=h_ss, recv_sem=h_rs, device_id={'sp': partner}, device_id_type=MESH)
    swap.start()
    swap.wait_recv()

    lo, hi = halves[0], halves[1]
    raw_q = [lo[:, :dq_cols], hi[:, :dq_cols]]
    mean_sq = sum(jnp.sum(r * r, axis=1, keepdims=True) for r in raw_q) / (2 * dq_cols)
    inv = lax.rsqrt(mean_sq + EPS)
    c_q = jnp.concatenate([r * inv * q_gain[:, i * dq_cols:(i + 1) * dq_cols] for i, r in enumerate(raw_q)], axis=1).astype(jnp.bfloat16)

    def rotate_pair(pair):
        other = jnp.where(lane % 64 < 32, pltpu.roll(pair, 96, 1), pltpu.roll(pair, 32, 1))
        return pair * cos_t + other * sin_t

    def emit(q_blk, k, side):
        for p in range(blk // 384):
            t0, t1, t2 = (q_blk[:, p * 384 + i * 128:p * 384 + (i + 1) * 128] for i in range(3))
            odd = jnp.where(lane < 64, pltpu.roll(t1, 64, 1), pltpu.roll(t2, 64, 1))
            pe = rotate_pair(jnp.where(lane < 64, t1, t2))
            for i, (nope, rope) in enumerate(((t0, pe), (odd, pltpu.roll(pe, 64, 1)))):
                h = k * (blk // 192) + p * 2 + i
                lat = jnp.dot(nope.astype(jnp.bfloat16), uk[side * half_heads + h], preferred_element_type=f32)
                first = (h % group) * pitch
                for j in range(lat_dim // 128):
                    turn[side, j, first:first + n_seqs, :] = lat[:, j * 128:(j + 1) * 128]
                turn[side, lat_dim // 128, first:first + n_seqs, :] = rope

    def flush(first, side):
        rows = pl.ds(pl.multiple_of(first, group), group)
        for b in range(n_seqs):
            for j in range(lat_dim // 128 + 1):
                q_out[b, rows, j * 128:(j + 1) * 128] = turn[side, j, pl.ds(b, group, stride=pitch), :].astype(q_out.dtype)

    sends = []

    def own_block(k):
        wait_load(load_uq(k))
        q_blk = jnp.dot(c_q, uq[k], preferred_element_type=f32).astype(jnp.bfloat16).astype(f32)
        q_mine[k] = q_blk
        sends.append(pltpu.make_async_remote_copy(src_ref=q_mine.at[k], dst_ref=q_theirs.at[k], send_sem=q_ss.at[k], recv_sem=q_rs.at[k], device_id={'sp': partner}, device_id_type=MESH))
        if k % per_grp == 0:
            wait_load(load_uk(k // per_grp))
        emit(q_blk, k, 0)
        sends[k].start()
        if k % per_grp == per_grp - 1:
            flush(c * half_heads + (k // per_grp) * group, 0)

    def their_block(k):
        sends[k].wait_recv()
        if k % per_grp == 0:
            wait_load(load_uk(n_grp // 2 + k // per_grp))
        emit(q_theirs[k], k, 1)
        if k % per_grp == per_grp - 1:
            flush((1 - c) * half_heads + (k // per_grp) * group, 1)

    behind = cfg["behind"]
    for k in range(n_blk):
        own_block(k)
        if k >= behind:
            their_block(k - behind)
    raw_kv = [lo[:, dq_cols:dq_cols + lat_dim // 2], hi[:, dq_cols:dq_cols + lat_dim // 2]]
    mean_sq = sum(jnp.sum(r * r, axis=1, keepdims=True) for r in raw_kv) / lat_dim
    inv = lax.rsqrt(mean_sq + EPS)
    c_kv = jnp.concatenate([r * inv * kv_gain[:, i * (lat_dim // 2):(i + 1) * (lat_dim // 2)] for i, r in enumerate(raw_kv)], axis=1).astype(jnp.bfloat16)
    k_pe = rotate_pair(hi[:, dq_cols + lat_dim // 2:]).astype(jnp.bfloat16)
    kvn_out[:, :lat_dim] = c_kv.astype(f32)
    kvn_out[:, lat_dim:] = k_pe.astype(f32)

    for k in range(n_blk - behind, n_blk):
        their_block(k)
    swap.wait_send()
    for s in sends:
        s.wait_send()


def project(hidden, cache_len, w_dq, q_gain, w_uq, w_dkv, kv_gain, w_uk):
    n_seqs, d_model = hidden.shape
    heads, nope_dim, lat_dim = w_uk.shape
    q_rank = w_dq.shape[1]
    rope_dim = w_dkv.shape[1] - lat_dim
    freqs = [float(f) for f in np.power(ROPE_THETA, -2.0 * np.arange(rope_dim // 2) / rope_dim).astype(np.float32)]
    cfg = dict(n_kt=4, lat_dim=lat_dim, group=16, pitch=n_seqs + 8, in_flight=4, behind=2, freqs=freqs)
    n_k, n_blk = 8, 8
    dq_cols, dkv_cols = q_rank // 2, lat_dim // 2 + rope_dim
    blk = w_uq.shape[1] // 2 // n_blk
    f32, bf16 = jnp.float32, jnp.bfloat16
    small = jnp.concatenate([q_gain.astype(f32), kv_gain.astype(f32), cache_len.astype(f32), jnp.zeros((128 - n_seqs,), f32)])
    dma = pltpu.SemaphoreType.DMA
    return pl.pallas_call(
        functools.partial(project_kernel, cfg),
        out_shape=(
            jax.ShapeDtypeStruct((n_seqs, heads, lat_dim + 128), bf16),
            jax.ShapeDtypeStruct((n_seqs, lat_dim + 128), f32),
        ),
        in_specs=[VMEM, VMEM, HBM, HBM, HBM, HBM],
        out_specs=(VMEM, VMEM),
        scratch_shapes=[
            pltpu.VMEM((n_k, d_model // n_k, dq_cols), bf16),
            pltpu.VMEM((dkv_cols, d_model), bf16),
            pltpu.VMEM((n_blk, q_rank, blk), bf16),
            pltpu.VMEM((heads, nope_dim, lat_dim), bf16),
            pltpu.VMEM((2, n_seqs, dq_cols + lat_dim // 2 + 128), f32),
            pltpu.VMEM((n_blk, n_seqs, blk), f32),
            pltpu.VMEM((n_blk, n_seqs, blk), f32),
            pltpu.VMEM((2, lat_dim // 128 + 1, cfg["group"] * cfg["pitch"], 128), f32),
            dma((n_k,)), dma((cfg["n_kt"],)), dma((n_blk,)), dma((heads // cfg["group"],)),
            dma, dma, dma((n_blk,)), dma((n_blk,)),
        ],
        compiler_params=pltpu.CompilerParams(collective_id=1, has_side_effects=True, vmem_limit_bytes=48 * 1024 * 1024),
        name="project",
    )(small, hidden, w_dq, w_dkv.T, w_uq, w_uk)


def attend_kernel(cfg, len_ref, q_ref, kvn_ref, ckv_hbm, kpe_hbm, cout_hbm, kout_hbm, terms, kv_new,
                  cbuf, kbuf, peaks, denoms, isem, osem):
    n_seqs, shard_len = ckv_hbm.shape[0], ckv_hbm.shape[1]
    lat_dim = ckv_hbm.shape[2]
    rope_dim = kpe_hbm.shape[1]
    per = terms.shape[2] - 1
    n_buf, lag, chunk = cfg["n_buf"], cfg["lag"], cfg["chunk"]
    base = lax.axis_index('sp') * shard_len

    def copies_in(b, slot):
        return (pltpu.make_async_copy(ckv_hbm.at[b], cbuf.at[slot], isem.at[slot, 0]),
                pltpu.make_async_copy(kpe_hbm.at[b], kbuf.at[slot], isem.at[slot, 1]))

    def copies_out(b, slot):
        return (pltpu.make_async_copy(cbuf.at[slot], cout_hbm.at[b], osem.at[slot, 0]),
                pltpu.make_async_copy(kbuf.at[slot], kout_hbm.at[b], osem.at[slot, 1]))

    for i in range(n_buf - lag):
        for c in copies_in(i, i):
            c.start()
    kv_new[...] = kvn_ref[:, :lat_dim + rope_dim].astype(kv_new.dtype)
    peaks[...] = jnp.zeros_like(peaks)
    denoms[...] = jnp.zeros_like(denoms)

    def step(b, carry):
        slot = lax.rem(b, n_buf)

        @pl.when(b >= lag)
        def _():
            for c in copies_out(b - lag, lax.rem(b - lag + n_buf, n_buf)):
                c.wait()

        ahead = b - lag + n_buf

        @pl.when(ahead < n_seqs)
        def _():
            for c in copies_in(ahead, lax.rem(ahead, n_buf)):
                c.start()

        for c in copies_in(b, slot):
            c.wait()
        last = len_ref[b] - base

        @pl.when((last >= 0) & (last < shard_len))
        def _():
            picked = lax.broadcasted_iota(jnp.int32, kvn_ref.shape, 0) == b
            fresh_row = jnp.sum(jnp.where(picked, kvn_ref[...], 0.0), axis=0, keepdims=True)
            r0 = pl.multiple_of((last // 16) * 16, 16)
            rows = cbuf[slot, pl.ds(r0, 16), :].astype(jnp.float32)
            row = lax.broadcasted_iota(jnp.int32, rows.shape, 0)
            cbuf[slot, pl.ds(r0, 16), :] = jnp.where(row == last - r0, fresh_row[:, :lat_dim], rows).astype(cbuf.dtype)
            c0 = pl.multiple_of((last // 128) * 128, 128)
            cols = kbuf[slot, :, pl.ds(c0, 128)].astype(jnp.float32)
            lane = lax.broadcasted_iota(jnp.int32, cols.shape, 1)
            diag = lane == lax.broadcasted_iota(jnp.int32, cols.shape, 0)
            fresh = jnp.sum(jnp.where(diag, fresh_row[:, lat_dim:], 0.0), axis=1, keepdims=True)
            kbuf[slot, :, pl.ds(c0, 128)] = jnp.where(lane == last - c0, fresh, cols).astype(kbuf.dtype)

        q_lat, q_pe = q_ref[b, :, :lat_dim], q_ref[b, :, lat_dim:lat_dim + rope_dim]
        scores = []
        for t in range(0, shard_len, chunk):
            s = lax.dot_general(q_lat, cbuf[slot, t:t + chunk, :], (((1,), (1,)), ((), ())), preferred_element_type=jnp.float32)
            s = s + jnp.dot(q_pe, kbuf[slot, :, t:t + chunk], preferred_element_type=jnp.float32)
            pos = lax.broadcasted_iota(jnp.int32, (1, chunk), 1) + t
            scores.append(jnp.where(pos <= last, s * cfg["scale"], NEG_FILL))
        peak = functools.reduce(jnp.maximum, [jnp.max(s, axis=1, keepdims=True) for s in scores])
        denom = jnp.zeros_like(peak)
        lat_sum = None
        for k, t in enumerate(range(0, shard_len, chunk)):
            w = jnp.exp(scores[k] - peak)
            denom = denom + jnp.sum(w, axis=1, keepdims=True)
            term = jnp.dot(w.astype(jnp.bfloat16), cbuf[slot, t:t + chunk, :], preferred_element_type=jnp.float32)
            lat_sum = term if lat_sum is None else lat_sum + term
        for c in copies_out(b, slot):
            c.start()
        terms[:, b // per, b % per] = lat_sum.reshape(terms.shape[0], *terms.shape[3:])
        lane = lax.broadcasted_iota(jnp.int32, peaks.shape, 1)
        peaks[...] = jnp.where(lane == b, peak, peaks[...])
        denoms[...] = jnp.where(lane == b, denom, denoms[...])
        return carry

    lax.fori_loop(0, n_seqs, step, 0)
    for part in range(2):
        terms[:, part, per, :, :128] = peaks[...].reshape(terms.shape[0], terms.shape[3], 128)
        terms[:, part, per, :, 128:256] = denoms[...].reshape(terms.shape[0], terms.shape[3], 128)
    for i in range(n_seqs - lag, n_seqs):
        for c in copies_out(i, i % n_buf):
            c.wait()


def attend(q, kvn, cache_len, ckv_blk, kpe_blk_t, n_dev, qk_dim):
    n_seqs, shard_len, lat_dim = ckv_blk.shape
    rope_dim = kpe_blk_t.shape[1]
    n_heads = q.shape[1]
    cfg = dict(n_buf=8, lag=3, chunk=512, scale=qk_dim ** -0.5)
    terms_shape = (n_dev, 2, n_seqs // 2 + 1, n_heads // n_dev, lat_dim)
    return pl.pallas_call(
        functools.partial(attend_kernel, cfg),
        out_shape=(
            jax.ShapeDtypeStruct(ckv_blk.shape, ckv_blk.dtype),
            jax.ShapeDtypeStruct(kpe_blk_t.shape, kpe_blk_t.dtype),
            jax.ShapeDtypeStruct(terms_shape, jnp.float32),
            jax.ShapeDtypeStruct((n_seqs, lat_dim + rope_dim), ckv_blk.dtype),
        ),
        in_specs=[SMEM, VMEM, VMEM, HBM, HBM],
        out_specs=(HBM, HBM, VMEM, VMEM),
        scratch_shapes=[
            pltpu.VMEM((cfg["n_buf"], shard_len, lat_dim), ckv_blk.dtype),
            pltpu.VMEM((cfg["n_buf"], rope_dim, shard_len), kpe_blk_t.dtype),
            pltpu.VMEM((n_heads, 128), jnp.float32),
            pltpu.VMEM((n_heads, 128), jnp.float32),
            pltpu.SemaphoreType.DMA((cfg["n_buf"], 2)),
            pltpu.SemaphoreType.DMA((cfg["n_buf"], 2)),
        ],
        compiler_params=pltpu.CompilerParams(vmem_limit_bytes=36 * 1024 * 1024),
        name="attend",
    )(cache_len, q, kvn, ckv_blk, kpe_blk_t)


def finish_kernel(terms, w_uv, w_out, out_ref, own, pair, from_x, from_y, uv, wo, merged, oheads, psend, precv, isend, irecv, fin, agr, agp,
                  lsem, own_sem, d_ss, d_rs, x_ss, x_rs, y_ss, y_rs, p_ss, p_rs, i_ss, i_rs, a_ss, a_rs, f_ss, f_rs):
    n_seqs, width = fin.shape
    heads = uv.shape[0]
    depth = wo.shape[0]
    me = lax.axis_index('sp')
    y, x, c = me // 4, (me // 2) % 2, me % 2

    def device(q, jc):
        return ((y + q // 2) % 2) * 4 + ((x + q % 2) % 2) * 2 + (c + jc) % 2

    def send(src, dst, ss, rs, dev):
        return pltpu.make_async_remote_copy(src_ref=src, dst_ref=dst, send_sem=ss, recv_sem=rs, device_id={'sp': dev}, device_id_type=MESH)

    load_uv = pltpu.make_async_copy(w_uv.at[pl.ds(me * heads, heads)], uv, lsem.at[0])
    load_wo = pltpu.make_async_copy(w_out.at[pl.ds(me * depth, depth)], wo, lsem.at[1])
    order = ((3, 0), (3, 1), (1, 0), (2, 1), (2, 0), (1, 1), (0, 0), (0, 1))
    per = n_seqs // 2
    loads = {(q, h): pltpu.make_async_copy(terms.at[device(q, 0), h], own.at[q, h], own_sem.at[q, h]) for q, h in order}
    for k in order:
        loads[k].start()
    load_uv.start()

    others = ((0, 1), (1, 0), (2, 0), (3, 0))
    barrier = pltpu.get_barrier_semaphore()
    for q, jc in others:
        pl.semaphore_signal(barrier, inc=1, device_id={'sp': device(q, jc)}, device_id_type=MESH)
    pl.semaphore_wait(barrier, len(others))

    d_sends = {(q, h): send(terms.at[device(q, 1), h], pair.at[q, h], d_ss.at[q, h], d_rs.at[q, h], device(0, 1)) for q, h in order}
    for k in order:
        d_sends[k].start()

    def merge(dst, src, h):
        old, new = dst[per, :, :128], src[per, :, :128]
        peak = jnp.maximum(old, new)
        f_old, f_new = jnp.exp(old - peak), jnp.exp(new - peak)
        dst[per, :, :128] = peak
        dst[per, :, 128:256] = f_old * dst[per, :, 128:256] + f_new * src[per, :, 128:256]
        for i in range(per):
            b = h * per + i
            dst[i] = f_old[:, b:b + 1] * dst[i] + f_new[:, b:b + 1] * src[i]

    def merge_pair(q, h):
        loads[q, h].wait()
        d_sends[q, h].wait_recv()
        merge(own.at[q, h], pair.at[q, h], h)

    x_dev, y_dev = device(1, 0), device(2, 0)
    x_sends = [send(own.at[k], from_x.at[i], x_ss.at[i], x_rs.at[i], x_dev) for i, k in enumerate(((3, 0), (1, 0), (1, 1)))]
    y_sends = [send(own.at[k], from_y.at[i], y_ss.at[i], y_rs.at[i], y_dev) for i, k in enumerate(((3, 1), (2, 1), (2, 0)))]
    merge_pair(3, 0)
    merge_pair(3, 1)
    x_sends[0].start()
    merge_pair(1, 0)
    y_sends[0].start()
    merge_pair(2, 1)
    x_sends[1].start()
    merge_pair(2, 0)
    y_sends[1].start()
    merge_pair(1, 1)
    merge_pair(0, 0)
    merge_pair(0, 1)
    load_wo.start()
    x_sends[0].wait_recv()
    merge(own.at[2, 0], from_x.at[0], 0)
    y_sends[0].wait_recv()
    merge(own.at[1, 1], from_y.at[0], 1)
    y_sends[2].start()
    x_sends[2].start()
    x_sends[1].wait_recv()
    merge(own.at[0, 0], from_x.at[1], 0)
    y_sends[1].wait_recv()
    merge(own.at[0, 1], from_y.at[1], 1)
    y_sends[2].wait_recv()
    merge(own.at[0, 0], from_y.at[2], 0)
    x_sends[2].wait_recv()
    merge(own.at[0, 1], from_x.at[2], 1)
    for h in range(2):
        inv = 1.0 / own[0, h, per, :, 128:256]
        for i in range(per):
            b = h * per + i
            acc = inv[:, b:b + 1] * own[0, h, i]
            for k in range(merged.shape[0]):
                merged[k, b * heads:(b + 1) * heads, :] = acc[:, k * 128:(k + 1) * 128]
    load_uv.wait()
    for h in range(heads):
        o_lat = jnp.concatenate([merged[k, pl.ds(h, n_seqs, stride=heads), :] for k in range(merged.shape[0])], axis=1).astype(jnp.bfloat16)
        o_h = lax.dot_general(o_lat, uv[h], (((1,), (1,)), ((), ())), preferred_element_type=jnp.float32)
        oheads[:, h * o_h.shape[1]:(h + 1) * o_h.shape[1]] = o_h.astype(jnp.bfloat16)
    load_wo.wait()

    def columns(dev, part):
        at, size = parts[part]
        return pl.ds(pl.multiple_of(dev * width + at, 128), size)

    def partial_out(dev, part):
        return jnp.dot(oheads[...], wo[:, columns(dev, part)], preferred_element_type=jnp.float32)

    parts = ((0, width // 256 * 128), (width // 256 * 128, width - width // 256 * 128))
    far = (3, 1, 2)
    p_sends, i_sends, a_sends, f_sends = {}, {}, {}, {}

    def start(waiting):
        while waiting:
            waiting.pop().start()

    def put(ref, part, value):
        ref[:, parts[part][0]:sum(parts[part])] = value

    def get(ref, part):
        return ref[:, parts[part][0]:sum(parts[part])]

    def cut(ref, part):
        return ref.at[:, pl.ds(*parts[part])]

    mine = []
    waiting = []
    for part in range(2):
        for q in far + (0,):
            put(psend.at[q], part, partial_out(device(q, 1), part))
            start(waiting)
            p_sends[q, part] = send(cut(psend.at[q], part), cut(precv.at[q], part), p_ss.at[q, part], p_rs.at[q, part], device(0, 1))
            waiting.append(p_sends[q, part])
        for q in far + (0,):
            value = partial_out(device(q, 0), part)
            start(waiting)
            p_sends[q, part].wait_recv()
            value = value + get(precv.at[q], part)
            if q:
                put(isend.at[q - 1], part, value)
                i_sends[q, part] = send(cut(isend.at[q - 1], part), cut(irecv.at[q - 1], part), i_ss.at[q - 1, part], i_rs.at[q - 1, part], device(q, 0))
                waiting.append(i_sends[q, part])
            else:
                mine.append(value)
        start(waiting)
    for part in range(2):
        for q in far:
            i_sends[q, part].wait_recv()
        result = mine[part] + get(irecv.at[0], part) + get(irecv.at[1], part) + get(irecv.at[2], part)
        put(fin, part, result)
        out_ref[:, columns(me, part)] = result
        for q in far:
            a_sends[q, part] = send(cut(fin, part), cut(agr.at[q - 1], part), a_ss.at[q - 1, part], a_rs.at[q - 1, part], device(q, 0))
            a_sends[q, part].start()
        f_sends[0, part] = send(cut(fin, part), cut(agp.at[0], part), f_ss.at[0, part], f_rs.at[0, part], device(0, 1))
        f_sends[0, part].start()
    for part in range(2):
        for q in (1, 2, 3):
            a_sends[q, part].wait_recv()
            f_sends[q, part] = send(cut(agr.at[q - 1], part), cut(agp.at[q], part), f_ss.at[q, part], f_rs.at[q, part], device(0, 1))
            f_sends[q, part].start()
            out_ref[:, columns(device(q, 0), part)] = get(agr.at[q - 1], part)
    for part in range(2):
        for q in range(4):
            f_sends[q, part].wait_recv()
            out_ref[:, columns(device(q, 1), part)] = get(agp.at[q], part)
    for s in list(d_sends.values()) + x_sends + y_sends + list(p_sends.values()) + list(i_sends.values()) + list(a_sends.values()) + list(f_sends.values()):
        s.wait_send()


def finish(terms, w_uv, w_out):
    n_dev, _, rows, heads, lat_dim = terms.shape
    n_seqs = 2 * (rows - 1)
    d_model = w_out.shape[1]
    depth = w_out.shape[0] // n_dev
    width = d_model // n_dev
    f32 = jnp.float32
    return pl.pallas_call(
        finish_kernel,
        out_shape=jax.ShapeDtypeStruct((n_seqs, d_model), f32),
        in_specs=[VMEM, HBM, HBM],
        out_specs=VMEM,
        scratch_shapes=[
            pltpu.VMEM((4, 2, rows, heads, lat_dim), f32),
            pltpu.VMEM((4, 2, rows, heads, lat_dim), f32),
            pltpu.VMEM((3, rows, heads, lat_dim), f32),
            pltpu.VMEM((3, rows, heads, lat_dim), f32),
            pltpu.VMEM((heads,) + w_uv.shape[1:], w_uv.dtype),
            pltpu.VMEM((depth, d_model), w_out.dtype),
            pltpu.VMEM((lat_dim // 128, n_seqs * heads, 128), f32),
            pltpu.VMEM((n_seqs, depth), jnp.bfloat16),
            pltpu.VMEM((4, n_seqs, width), f32),
            pltpu.VMEM((4, n_seqs, width), f32),
            pltpu.VMEM((3, n_seqs, width), f32),
            pltpu.VMEM((3, n_seqs, width), f32),
            pltpu.VMEM((n_seqs, width), f32),
            pltpu.VMEM((3, n_seqs, width), f32),
            pltpu.VMEM((4, n_seqs, width), f32),
            pltpu.SemaphoreType.DMA((2,)),
            pltpu.SemaphoreType.DMA((4, 2)),
            pltpu.SemaphoreType.DMA((4, 2)),
            pltpu.SemaphoreType.DMA((4, 2)),
            pltpu.SemaphoreType.DMA((3,)),
            pltpu.SemaphoreType.DMA((3,)),
            pltpu.SemaphoreType.DMA((3,)),
            pltpu.SemaphoreType.DMA((3,)),
            pltpu.SemaphoreType.DMA((4, 2)),
            pltpu.SemaphoreType.DMA((4, 2)),
            pltpu.SemaphoreType.DMA((3, 2)),
            pltpu.SemaphoreType.DMA((3, 2)),
            pltpu.SemaphoreType.DMA((3, 2)),
            pltpu.SemaphoreType.DMA((3, 2)),
            pltpu.SemaphoreType.DMA((4, 2)),
            pltpu.SemaphoreType.DMA((4, 2)),
        ],
        compiler_params=pltpu.CompilerParams(collective_id=0, has_side_effects=True, vmem_limit_bytes=48 * 1024 * 1024),
        name="finish",
    )(terms, w_uv, w_out)


def solution(mesh):
    n_dev = mesh.shape['sp']

    def local_step(hidden, ckv_blk, kpe_blk, cache_len, w_dq, q_gain, w_uq, w_dkv, kv_gain, w_uk, w_uv, w_out):
        q, kvn = project(hidden, cache_len, w_dq, q_gain, w_uq, w_dkv, kv_gain, w_uk)
        qk_dim = w_uk.shape[1] + kpe_blk.shape[2]
        ckv_out, kpe_out_t, terms, kv_new = attend(q, kvn, cache_len, ckv_blk, jnp.swapaxes(kpe_blk, 1, 2), n_dev, qk_dim)
        out = finish(terms, w_uv, w_out).astype(jnp.bfloat16)
        return out, ckv_out, jnp.swapaxes(kpe_out_t, 1, 2), kv_new

    cache_spec = P('dp', 'sp', None)
    return jax.shard_map(local_step, mesh=mesh, in_specs=(P('dp', None), cache_spec, cache_spec, P('dp'), P(), P(), P(), P(), P(), P(), P(), P()), out_specs=(P('dp', None), cache_spec, cache_spec, P('dp', None)), check_vma=False)
```

```python
import functools

import jax
import jax.numpy as jnp
import numpy as np
from jax import lax
from jax.experimental import pallas as pl
from jax.experimental.pallas import tpu as pltpu
from jax.sharding import PartitionSpec as P

EPS = 1e-6
ROPE_THETA = 10000.0
NEG_FILL = -1e30
MESH = pl.DeviceIdType.MESH
VMEM = pl.BlockSpec(memory_space=pltpu.VMEM)
SMEM = pl.BlockSpec(memory_space=pltpu.SMEM)
HBM = pl.BlockSpec(memory_space=pltpu.HBM)


def project_kernel(cfg, small_ref, hidden, w_dq, w_dkv_t, w_uq, w_uk, q_out, kvn_out,
                   dq, dkv, uq, uk, halves, q_mine, q_theirs, turn, dq_sem, dkv_sem, uq_sem, uk_sem, h_ss, h_rs, q_ss, q_rs):
    n_seqs = hidden.shape[0]
    n_k, k_rows, dq_cols = dq.shape
    n_blk, _, blk = uq.shape
    dkv_cols = dkv.shape[0]
    n_kt = cfg["n_kt"]
    k_tile = dkv.shape[1] // n_kt
    lat_dim = cfg["lat_dim"]
    nope_dim = uk.shape[1]
    heads = uk.shape[0]
    half_heads = heads // 2
    group, pitch = cfg["group"], cfg["pitch"]
    me = lax.axis_index('sp')
    c = me % 2
    partner = me - c + (1 - c)
    f32 = jnp.float32

    def load_dq(k):
        return pltpu.make_async_copy(w_dq.at[pl.ds(k * k_rows, k_rows), pl.ds(pl.multiple_of(c * dq_cols, 128), dq_cols)], dq.at[k], dq_sem.at[k])

    def load_dkv(k):
        return pltpu.make_async_copy(w_dkv_t.at[pl.ds(pl.multiple_of(c * (lat_dim // 2), 16), dkv_cols), pl.ds(k * k_tile, k_tile)], dkv.at[:, pl.ds(k * k_tile, k_tile)], dkv_sem.at[k])

    def load_uq(k):
        return pltpu.make_async_copy(w_uq.at[:, pl.ds(pl.multiple_of((c * n_blk + k) * blk, 128), blk)], uq.at[k], uq_sem.at[k])

    def load_uk(k):
        first = (c * half_heads + k * group) % heads
        return pltpu.make_async_copy(w_uk.at[pl.ds(first, group)], uk.at[pl.ds(k * group, group)], uk_sem.at[k])

    n_grp = heads // group
    per_kt = n_k // n_kt
    per_grp = n_blk // (n_grp // 2)
    loads = []
    for k in range(n_k):
        loads.append(load_dq(k))
        if k % per_kt == 0:
            loads.append(load_dkv(k // per_kt))
    for k in range(n_blk):
        loads.append(load_uq(k))
        if k % per_grp == 0:
            loads.append(load_uk(k // per_grp))
        if k >= cfg["behind"] and (k - cfg["behind"]) % per_grp == 0:
            loads.append(load_uk(n_grp // 2 + (k - cfg["behind"]) // per_grp))
    in_flight = cfg["in_flight"]
    for load in loads[:in_flight]:
        load.start()
    queue = loads[in_flight:]

    def wait_load(load):
        load.wait()
        if queue:
            queue.pop(0).start()

    barrier = pltpu.get_barrier_semaphore()
    pl.semaphore_signal(barrier, inc=1, device_id={'sp': partner}, device_id_type=MESH)
    pl.semaphore_wait(barrier, 1)

    lane = lax.broadcasted_iota(jnp.int32, (n_seqs, 128), 1)
    row = lax.broadcasted_iota(jnp.int32, (n_seqs, 128), 0)
    small = small_ref[...].reshape(1, -1)
    q_gain, kv_gain, lengths = small[:, :2 * dq_cols], small[:, 2 * dq_cols:2 * dq_cols + lat_dim], small[:, 2 * dq_cols + lat_dim:]
    position = jnp.sum(jnp.where(lane == row, lengths, 0.0), axis=1, keepdims=True)
    freq = jnp.zeros((n_seqs, 128), f32)
    for i, value in enumerate(cfg["freqs"]):
        freq = jnp.where(lane % 32 == i, value, freq)
    angle = position * freq
    cos_t = jnp.cos(angle)
    sin_t = jnp.where(lane % 64 < 32, -jnp.sin(angle), jnp.sin(angle))

    acc_q = jnp.zeros((n_seqs, dq_cols), f32)
    acc_kv = jnp.zeros((n_seqs, dkv_cols), f32)
    for k in range(n_k):
        wait_load(load_dq(k))
        acc_q = acc_q + jnp.dot(hidden[:, k * k_rows:(k + 1) * k_rows], dq[k], preferred_element_type=f32)
        if k % per_kt == per_kt - 1:
            t = k // per_kt
            wait_load(load_dkv(t))
            cols = slice(t * k_tile, (t + 1) * k_tile)
            acc_kv = acc_kv + lax.dot_general(hidden[:, cols], dkv[:, cols], (((1,), (1,)), ((), ())), preferred_element_type=f32)
    halves[c, :, dq_cols + lat_dim // 2:] = jnp.zeros((n_seqs, 128), f32)
    halves[c, :, :dq_cols] = acc_q
    halves[c, :, dq_cols:dq_cols + dkv_cols] = acc_kv
    swap = pltpu.make_async_remote_copy(src_ref=halves.at[c], dst_ref=halves.at[c], send_sem=h_ss, recv_sem=h_rs, device_id={'sp': partner}, device_id_type=MESH)
    swap.start()
    swap.wait_recv()

    lo, hi = halves[0], halves[1]
    raw_q = [lo[:, :dq_cols], hi[:, :dq_cols]]
    mean_sq = sum(jnp.sum(r * r, axis=1, keepdims=True) for r in raw_q) / (2 * dq_cols)
    inv = lax.rsqrt(mean_sq + EPS)
    c_q = jnp.concatenate([r * inv * q_gain[:, i * dq_cols:(i + 1) * dq_cols] for i, r in enumerate(raw_q)], axis=1).astype(jnp.bfloat16)

    def rotate_pair(pair):
        other = jnp.where(lane % 64 < 32, pltpu.roll(pair, 96, 1), pltpu.roll(pair, 32, 1))
        return pair * cos_t + other * sin_t

    def emit(q_blk, k, side):
        for p in range(blk // 384):
            t0, t1, t2 = (q_blk[:, p * 384 + i * 128:p * 384 + (i + 1) * 128] for i in range(3))
            odd = jnp.where(lane < 64, pltpu.roll(t1, 64, 1), pltpu.roll(t2, 64, 1))
            pe = rotate_pair(jnp.where(lane < 64, t1, t2))
            for i, (nope, rope) in enumerate(((t0, pe), (odd, pltpu.roll(pe, 64, 1)))):
                h = k * (blk // 192) + p * 2 + i
                lat = jnp.dot(nope.astype(jnp.bfloat16), uk[side * half_heads + h], preferred_element_type=f32)
                first = (h % group) * pitch
                for j in range(lat_dim // 128):
                    turn[side, j, first:first + n_seqs, :] = lat[:, j * 128:(j + 1) * 128]
                turn[side, lat_dim // 128, first:first + n_seqs, :] = rope

    def flush(first, side):
        rows = pl.ds(pl.multiple_of(first, group), group)
        for b in range(n_seqs):
            for j in range(lat_dim // 128 + 1):
                q_out[b, rows, j * 128:(j + 1) * 128] = turn[side, j, pl.ds(b, group, stride=pitch), :].astype(q_out.dtype)

    sends = []

    def own_block(k):
        wait_load(load_uq(k))
        q_blk = jnp.dot(c_q, uq[k], preferred_element_type=f32).astype(jnp.bfloat16).astype(f32)
        q_mine[k] = q_blk
        sends.append(pltpu.make_async_remote_copy(src_ref=q_mine.at[k], dst_ref=q_theirs.at[k], send_sem=q_ss.at[k], recv_sem=q_rs.at[k], device_id={'sp': partner}, device_id_type=MESH))
        if k % per_grp == 0:
            wait_load(load_uk(k // per_grp))
        emit(q_blk, k, 0)
        sends[k].start()
        if k % per_grp == per_grp - 1:
            flush(c * half_heads + (k // per_grp) * group, 0)

    def their_block(k):
        sends[k].wait_recv()
        if k % per_grp == 0:
            wait_load(load_uk(n_grp // 2 + k // per_grp))
        emit(q_theirs[k], k, 1)
        if k % per_grp == per_grp - 1:
            flush((1 - c) * half_heads + (k // per_grp) * group, 1)

    behind = cfg["behind"]
    for k in range(n_blk):
        own_block(k)
        if k >= behind:
            their_block(k - behind)
    raw_kv = [lo[:, dq_cols:dq_cols + lat_dim // 2], hi[:, dq_cols:dq_cols + lat_dim // 2]]
    mean_sq = sum(jnp.sum(r * r, axis=1, keepdims=True) for r in raw_kv) / lat_dim
    inv = lax.rsqrt(mean_sq + EPS)
    c_kv = jnp.concatenate([r * inv * kv_gain[:, i * (lat_dim // 2):(i + 1) * (lat_dim // 2)] for i, r in enumerate(raw_kv)], axis=1).astype(jnp.bfloat16)
    k_pe = rotate_pair(hi[:, dq_cols + lat_dim // 2:]).astype(jnp.bfloat16)
    kvn_out[:, :lat_dim] = c_kv.astype(f32)
    kvn_out[:, lat_dim:] = k_pe.astype(f32)

    for k in range(n_blk - behind, n_blk):
        their_block(k)
    swap.wait_send()
    for s in sends:
        s.wait_send()


def project(hidden, cache_len, w_dq, q_gain, w_uq, w_dkv, kv_gain, w_uk):
    n_seqs, d_model = hidden.shape
    heads, nope_dim, lat_dim = w_uk.shape
    q_rank = w_dq.shape[1]
    rope_dim = w_dkv.shape[1] - lat_dim
    freqs = [float(f) for f in np.power(ROPE_THETA, -2.0 * np.arange(rope_dim // 2) / rope_dim).astype(np.float32)]
    cfg = dict(n_kt=4, lat_dim=lat_dim, group=16, pitch=n_seqs + 8, in_flight=4, behind=2, freqs=freqs)
    n_k, n_blk = 8, 8
    dq_cols, dkv_cols = q_rank // 2, lat_dim // 2 + rope_dim
    blk = w_uq.shape[1] // 2 // n_blk
    f32, bf16 = jnp.float32, jnp.bfloat16
    small = jnp.concatenate([q_gain.astype(f32), kv_gain.astype(f32), cache_len.astype(f32), jnp.zeros((128 - n_seqs,), f32)])
    dma = pltpu.SemaphoreType.DMA
    return pl.pallas_call(
        functools.partial(project_kernel, cfg),
        out_shape=(
            jax.ShapeDtypeStruct((n_seqs, heads, lat_dim + 128), bf16),
            jax.ShapeDtypeStruct((n_seqs, lat_dim + 128), f32),
        ),
        in_specs=[VMEM, VMEM, HBM, HBM, HBM, HBM],
        out_specs=(VMEM, VMEM),
        scratch_shapes=[
            pltpu.VMEM((n_k, d_model // n_k, dq_cols), bf16),
            pltpu.VMEM((dkv_cols, d_model), bf16),
            pltpu.VMEM((n_blk, q_rank, blk), bf16),
            pltpu.VMEM((heads, nope_dim, lat_dim), bf16),
            pltpu.VMEM((2, n_seqs, dq_cols + lat_dim // 2 + 128), f32),
            pltpu.VMEM((n_blk, n_seqs, blk), f32),
            pltpu.VMEM((n_blk, n_seqs, blk), f32),
            pltpu.VMEM((2, lat_dim // 128 + 1, cfg["group"] * cfg["pitch"], 128), f32),
            dma((n_k,)), dma((cfg["n_kt"],)), dma((n_blk,)), dma((heads // cfg["group"],)),
            dma, dma, dma((n_blk,)), dma((n_blk,)),
        ],
        compiler_params=pltpu.CompilerParams(collective_id=1, has_side_effects=True, vmem_limit_bytes=48 * 1024 * 1024),
        name="project",
    )(small, hidden, w_dq, w_dkv.T, w_uq, w_uk)


def device(me, q, jc):
    y, x, c = me // 4, (me // 2) % 2, me % 2
    return ((y + q // 2) % 2) * 4 + ((x + q % 2) % 2) * 2 + (c + jc) % 2


def attend_kernel(cfg, len_ref, q_ref, kvn_ref, ckv_hbm, kpe_hbm, *refs):
    first, count, spread = cfg["first"], cfg["count"], cfg["spread"]
    if not spread:
        refs = refs[2:]
    cout_hbm, kout_hbm, *terms = refs[:-7 if spread else -6]
    if spread:
        kv_new = terms.pop()
    cbuf, kbuf, peaks, denoms, isem, osem, *lat = refs[-7 if spread else -6:]
    n_seqs, shard_len = count, ckv_hbm.shape[1]
    lat_dim = ckv_hbm.shape[2]
    rope_dim = kpe_hbm.shape[1]
    per = count // 2
    me = lax.axis_index('sp')
    n_buf, lag, chunk = cfg["n_buf"], cfg["lag"], cfg["chunk"]
    base = lax.axis_index('sp') * shard_len

    def copies_in(b, slot):
        return (pltpu.make_async_copy(ckv_hbm.at[first + b], cbuf.at[slot], isem.at[slot, 0]),
                pltpu.make_async_copy(kpe_hbm.at[first + b], kbuf.at[slot], isem.at[slot, 1]))

    def copies_out(b, slot):
        return (pltpu.make_async_copy(cbuf.at[slot], cout_hbm.at[first + b], osem.at[slot, 0]),
                pltpu.make_async_copy(kbuf.at[slot], kout_hbm.at[first + b], osem.at[slot, 1]))

    for i in range(n_buf - lag):
        for c in copies_in(i, i):
            c.start()
    if spread:
        kv_new[...] = kvn_ref[:, :lat_dim + rope_dim].astype(kv_new.dtype)
    peaks[...] = jnp.zeros_like(peaks)
    denoms[...] = jnp.zeros_like(denoms)

    def step(b, carry):
        slot = lax.rem(b, n_buf)

        @pl.when(b >= lag)
        def _():
            for c in copies_out(b - lag, lax.rem(b - lag + n_buf, n_buf)):
                c.wait()

        ahead = b - lag + n_buf

        @pl.when(ahead < n_seqs)
        def _():
            for c in copies_in(ahead, lax.rem(ahead, n_buf)):
                c.start()

        for c in copies_in(b, slot):
            c.wait()
        last = len_ref[first + b] - base

        @pl.when((last >= 0) & (last < shard_len))
        def _():
            picked = lax.broadcasted_iota(jnp.int32, kvn_ref.shape, 0) == first + b
            fresh_row = jnp.sum(jnp.where(picked, kvn_ref[...], 0.0), axis=0, keepdims=True)
            r0 = pl.multiple_of((last // 16) * 16, 16)
            rows = cbuf[slot, pl.ds(r0, 16), :].astype(jnp.float32)
            row = lax.broadcasted_iota(jnp.int32, rows.shape, 0)
            cbuf[slot, pl.ds(r0, 16), :] = jnp.where(row == last - r0, fresh_row[:, :lat_dim], rows).astype(cbuf.dtype)
            c0 = pl.multiple_of((last // 128) * 128, 128)
            cols = kbuf[slot, :, pl.ds(c0, 128)].astype(jnp.float32)
            lane = lax.broadcasted_iota(jnp.int32, cols.shape, 1)
            diag = lane == lax.broadcasted_iota(jnp.int32, cols.shape, 0)
            fresh = jnp.sum(jnp.where(diag, fresh_row[:, lat_dim:], 0.0), axis=1, keepdims=True)
            kbuf[slot, :, pl.ds(c0, 128)] = jnp.where(lane == last - c0, fresh, cols).astype(kbuf.dtype)

        q_lat, q_pe = q_ref[first + b, :, :lat_dim], q_ref[first + b, :, lat_dim:lat_dim + rope_dim]
        scores = []
        for t in range(0, shard_len, chunk):
            s = lax.dot_general(q_lat, cbuf[slot, t:t + chunk, :], (((1,), (1,)), ((), ())), preferred_element_type=jnp.float32)
            s = s + jnp.dot(q_pe, kbuf[slot, :, t:t + chunk], preferred_element_type=jnp.float32)
            pos = lax.broadcasted_iota(jnp.int32, (1, chunk), 1) + t
            scores.append(jnp.where(pos <= last, s * cfg["scale"], NEG_FILL))
        peak = functools.reduce(jnp.maximum, [jnp.max(s, axis=1, keepdims=True) for s in scores])
        denom = jnp.zeros_like(peak)
        lat_sum = None
        for k, t in enumerate(range(0, shard_len, chunk)):
            w = jnp.exp(scores[k] - peak)
            denom = denom + jnp.sum(w, axis=1, keepdims=True)
            term = jnp.dot(w.astype(jnp.bfloat16), cbuf[slot, t:t + chunk, :], preferred_element_type=jnp.float32)
            lat_sum = term if lat_sum is None else lat_sum + term
        for c in copies_out(b, slot):
            c.start()
        if spread:
            lat[0][...] = lat_sum
            for j, term in enumerate(terms):
                term[b] = lat[0][pl.ds(pl.multiple_of(device(me, j // 2, j % 2) * term.shape[1], 8), term.shape[1]), :]
        else:
            terms[0][:, b // per, b % per] = lat_sum.reshape(terms[0].shape[0], *terms[0].shape[3:])
        lane = lax.broadcasted_iota(jnp.int32, peaks.shape, 1)
        peaks[...] = jnp.where(lane == b, peak, peaks[...])
        denoms[...] = jnp.where(lane == b, denom, denoms[...])
        return carry

    lax.fori_loop(0, n_seqs, step, 0)
    if spread:
        for j, term in enumerate(terms):
            rows = pl.ds(pl.multiple_of(device(me, j // 2, j % 2) * term.shape[1], 8), term.shape[1])
            term[count, :, :128] = peaks[rows, :]
            term[count, :, 128:256] = denoms[rows, :]
    else:
        for part in range(2):
            terms[0][:, part, per, :, :128] = peaks[...].reshape(terms[0].shape[0], terms[0].shape[3], 128)
            terms[0][:, part, per, :, 128:256] = denoms[...].reshape(terms[0].shape[0], terms[0].shape[3], 128)
    for i in range(n_seqs - lag, n_seqs):
        for c in copies_out(i, i % n_buf):
            c.wait()


def attend(q, kvn, cache_len, ckv_blk, kpe_blk_t, n_dev, qk_dim, first, count, done=None):
    n_seqs, shard_len, lat_dim = ckv_blk.shape
    rope_dim = kpe_blk_t.shape[1]
    n_heads = q.shape[1]
    heads = n_heads // n_dev
    spread = done is None
    cfg = dict(n_buf=8, lag=3, chunk=512, scale=qk_dim ** -0.5, first=first, count=count, spread=spread)
    f32 = jnp.float32
    if spread:
        extra = [jax.ShapeDtypeStruct((count + 1, heads, lat_dim), f32)] * n_dev + [jax.ShapeDtypeStruct((n_seqs, lat_dim + rope_dim), ckv_blk.dtype)]
    else:
        extra = [jax.ShapeDtypeStruct((n_dev, 2, count // 2 + 1, heads, lat_dim), f32)]
    return pl.pallas_call(
        functools.partial(attend_kernel, cfg),
        out_shape=[jax.ShapeDtypeStruct(ckv_blk.shape, ckv_blk.dtype), jax.ShapeDtypeStruct(kpe_blk_t.shape, kpe_blk_t.dtype)] + extra,
        in_specs=[SMEM, VMEM, VMEM, HBM, HBM] + ([] if spread else [HBM, HBM]),
        out_specs=[HBM, HBM] + [VMEM] * len(extra),
        input_output_aliases={} if spread else {5: 0, 6: 1},
        scratch_shapes=[
            pltpu.VMEM((cfg["n_buf"], shard_len, lat_dim), ckv_blk.dtype),
            pltpu.VMEM((cfg["n_buf"], rope_dim, shard_len), kpe_blk_t.dtype),
            pltpu.VMEM((n_heads, 128), f32),
            pltpu.VMEM((n_heads, 128), f32),
            pltpu.SemaphoreType.DMA((cfg["n_buf"], 2)),
            pltpu.SemaphoreType.DMA((cfg["n_buf"], 2)),
        ] + ([pltpu.VMEM((n_heads, lat_dim), f32)] if spread else []),
        compiler_params=pltpu.CompilerParams(vmem_limit_bytes=36 * 1024 * 1024),
        cost_estimate=pl.CostEstimate(flops=count * 2 * n_heads * shard_len * (2 * lat_dim + rope_dim), bytes_accessed=count * 4 * shard_len * (lat_dim + rope_dim), transcendentals=count * n_heads * shard_len),
        name="attend",
    )(cache_len, q, kvn, ckv_blk, kpe_blk_t, *(done or ()))


def finish_kernel(terms, *refs):
    early_hbm, (w_uv, w_out, out_ref, own, pair, from_x, from_y, early, early_sem, uv, wo, merged, oheads, psend, precv, isend, irecv, fin, agr, agp,
                  lsem, d_ss, d_rs, x_ss, x_rs, y_ss, y_rs, p_ss, p_rs, i_ss, i_rs, a_ss, a_rs, f_ss, f_rs) = refs[:8], refs[8:]
    n_seqs, width = fin.shape
    heads = uv.shape[0]
    depth = wo.shape[0]
    me = lax.axis_index('sp')

    def peer(q, jc):
        return device(me, q, jc)

    def send(src, dst, ss, rs, dev):
        return pltpu.make_async_remote_copy(src_ref=src, dst_ref=dst, send_sem=ss, recv_sem=rs, device_id={'sp': dev}, device_id_type=MESH)

    load_uv = pltpu.make_async_copy(w_uv.at[pl.ds(me * heads, heads)], uv, lsem.at[0])
    load_wo = pltpu.make_async_copy(w_out.at[pl.ds(me * depth, depth)], wo, lsem.at[1])
    order = ((3, 0), (3, 1), (1, 0), (2, 1), (2, 0), (1, 1), (0, 0), (0, 1))
    late = terms.shape[1] * (terms.shape[2] - 1)
    first = n_seqs - late
    per = late // 2
    early_loads = [pltpu.make_async_copy(e, early.at[j], early_sem.at[j]) for j, e in enumerate(early_hbm)]
    load_uv.start()

    others = ((0, 1), (1, 0), (2, 0), (3, 0))
    barrier = pltpu.get_barrier_semaphore()
    for q, jc in others:
        pl.semaphore_signal(barrier, inc=1, device_id={'sp': peer(q, jc)}, device_id_type=MESH)
    pl.semaphore_wait(barrier, len(others))

    d_sends = {(q, h): send(terms.at[peer(q, 1), h], pair.at[q, h], d_ss.at[q, h], d_rs.at[q, h], peer(0, 1)) for q, h in order}
    for k in order:
        d_sends[k].start()

    def merge(dst, src, h, old_src=None):
        base = dst if old_src is None else old_src
        old, new = base[per, :, :128], src[per, :, :128]
        peak = jnp.maximum(old, new)
        f_old, f_new = jnp.exp(old - peak), jnp.exp(new - peak)
        dst[per, :, :128] = peak
        dst[per, :, 128:256] = f_old * base[per, :, 128:256] + f_new * src[per, :, 128:256]
        for i in range(per):
            b = h * per + i
            dst[i] = f_old[:, b:b + 1] * base[i] + f_new[:, b:b + 1] * src[i]

    def merge_pair(q, h):
        d_sends[q, h].wait_recv()
        merge(own.at[q, h], pair.at[q, h], h, terms.at[peer(q, 0), h])

    x_dev, y_dev = peer(1, 0), peer(2, 0)
    x_sends = [send(own.at[k], from_x.at[i], x_ss.at[i], x_rs.at[i], x_dev) for i, k in enumerate(((3, 0), (1, 0), (1, 1)))]
    y_sends = [send(own.at[k], from_y.at[i], y_ss.at[i], y_rs.at[i], y_dev) for i, k in enumerate(((3, 1), (2, 1), (2, 0)))]
    merge_pair(3, 0)
    merge_pair(3, 1)
    x_sends[0].start()
    merge_pair(1, 0)
    y_sends[0].start()
    merge_pair(2, 1)
    x_sends[1].start()
    merge_pair(2, 0)
    y_sends[1].start()
    merge_pair(1, 1)
    merge_pair(0, 0)
    merge_pair(0, 1)
    for load in early_loads:
        load.start()
    load_wo.start()
    for load in early_loads:
        load.wait()
    stats = [early[j, first, :, :128] for j in range(8)]
    top = functools.reduce(jnp.maximum, stats)
    factors = [jnp.exp(st - top) for st in stats]
    total = functools.reduce(jnp.add, [f * early[j, first, :, 128:256] for j, f in enumerate(factors)])
    factors = [f / total for f in factors]
    for b in range(first):
        acc = functools.reduce(jnp.add, [f[:, b:b + 1] * early[j, b] for j, f in enumerate(factors)])
        for k in range(merged.shape[0]):
            merged[k, b * heads:(b + 1) * heads, :] = acc[:, k * 128:(k + 1) * 128]
    x_sends[0].wait_recv()
    merge(own.at[2, 0], from_x.at[0], 0)
    y_sends[0].wait_recv()
    merge(own.at[1, 1], from_y.at[0], 1)
    y_sends[2].start()
    x_sends[2].start()
    x_sends[1].wait_recv()
    merge(own.at[0, 0], from_x.at[1], 0)
    y_sends[1].wait_recv()
    merge(own.at[0, 1], from_y.at[1], 1)
    y_sends[2].wait_recv()
    merge(own.at[0, 0], from_y.at[2], 0)
    x_sends[2].wait_recv()
    merge(own.at[0, 1], from_x.at[2], 1)
    for h in range(2):
        inv = 1.0 / own[0, h, per, :, 128:256]
        for i in range(per):
            b = h * per + i
            acc = inv[:, b:b + 1] * own[0, h, i]
            for k in range(merged.shape[0]):
                merged[k, (first + b) * heads:(first + b + 1) * heads, :] = acc[:, k * 128:(k + 1) * 128]
    load_uv.wait()
    for h in range(heads):
        o_lat = jnp.concatenate([merged[k, pl.ds(h, n_seqs, stride=heads), :] for k in range(merged.shape[0])], axis=1).astype(jnp.bfloat16)
        o_h = lax.dot_general(o_lat, uv[h], (((1,), (1,)), ((), ())), preferred_element_type=jnp.float32)
        oheads[:, h * o_h.shape[1]:(h + 1) * o_h.shape[1]] = o_h.astype(jnp.bfloat16)
    load_wo.wait()

    def columns(dev, part):
        at, size = parts[part]
        return pl.ds(pl.multiple_of(dev * width + at, 128), size)

    def partial_out(dev, part):
        return jnp.dot(oheads[...], wo[:, columns(dev, part)], preferred_element_type=jnp.float32)

    parts = ((0, width // 256 * 128), (width // 256 * 128, width - width // 256 * 128))
    far = (3, 1, 2)
    p_sends, i_sends, a_sends, f_sends = {}, {}, {}, {}

    def start(waiting):
        while waiting:
            waiting.pop().start()

    def put(ref, part, value):
        ref[:, parts[part][0]:sum(parts[part])] = value

    def get(ref, part):
        return ref[:, parts[part][0]:sum(parts[part])]

    def cut(ref, part):
        return ref.at[:, pl.ds(*parts[part])]

    mine = []
    waiting = []
    for part in range(2):
        for q in far + (0,):
            put(psend.at[q], part, partial_out(peer(q, 1), part))
            start(waiting)
            p_sends[q, part] = send(cut(psend.at[q], part), cut(precv.at[q], part), p_ss.at[q, part], p_rs.at[q, part], peer(0, 1))
            waiting.append(p_sends[q, part])
        for q in far + (0,):
            value = partial_out(peer(q, 0), part)
            start(waiting)
            p_sends[q, part].wait_recv()
            value = value + get(precv.at[q], part)
            if q:
                put(isend.at[q - 1], part, value)
                i_sends[q, part] = send(cut(isend.at[q - 1], part), cut(irecv.at[q - 1], part), i_ss.at[q - 1, part], i_rs.at[q - 1, part], peer(q, 0))
                waiting.append(i_sends[q, part])
            else:
                mine.append(value)
        start(waiting)
    for part in range(2):
        for q in far:
            i_sends[q, part].wait_recv()
        result = mine[part] + get(irecv.at[0], part) + get(irecv.at[1], part) + get(irecv.at[2], part)
        put(fin, part, result)
        out_ref[:, columns(me, part)] = result
        for q in far:
            a_sends[q, part] = send(cut(fin, part), cut(agr.at[q - 1], part), a_ss.at[q - 1, part], a_rs.at[q - 1, part], peer(q, 0))
            a_sends[q, part].start()
        f_sends[0, part] = send(cut(fin, part), cut(agp.at[0], part), f_ss.at[0, part], f_rs.at[0, part], peer(0, 1))
        f_sends[0, part].start()
    for part in range(2):
        for q in (1, 2, 3):
            a_sends[q, part].wait_recv()
            f_sends[q, part] = send(cut(agr.at[q - 1], part), cut(agp.at[q], part), f_ss.at[q, part], f_rs.at[q, part], peer(0, 1))
            f_sends[q, part].start()
            out_ref[:, columns(peer(q, 0), part)] = get(agr.at[q - 1], part)
    for part in range(2):
        for q in range(4):
            f_sends[q, part].wait_recv()
            out_ref[:, columns(peer(q, 1), part)] = get(agp.at[q], part)
    for s in list(d_sends.values()) + x_sends + y_sends + list(p_sends.values()) + list(i_sends.values()) + list(a_sends.values()) + list(f_sends.values()):
        s.wait_send()


def finish(terms, early, w_uv, w_out):
    n_dev, _, rows, heads, lat_dim = terms.shape
    n_seqs = 2 * (rows - 1) + early[0].shape[0] - 1
    d_model = w_out.shape[1]
    depth = w_out.shape[0] // n_dev
    width = d_model // n_dev
    f32 = jnp.float32
    return pl.pallas_call(
        finish_kernel,
        out_shape=jax.ShapeDtypeStruct((n_seqs, d_model), f32),
        in_specs=[VMEM] + [HBM] * (n_dev + 2),
        out_specs=VMEM,
        scratch_shapes=[
            pltpu.VMEM((4, 2, rows, heads, lat_dim), f32),
            pltpu.VMEM((4, 2, rows, heads, lat_dim), f32),
            pltpu.VMEM((3, rows, heads, lat_dim), f32),
            pltpu.VMEM((3, rows, heads, lat_dim), f32),
            pltpu.VMEM((n_dev,) + early[0].shape, f32),
            pltpu.SemaphoreType.DMA((n_dev,)),
            pltpu.VMEM((heads,) + w_uv.shape[1:], w_uv.dtype),
            pltpu.VMEM((depth, d_model), w_out.dtype),
            pltpu.VMEM((lat_dim // 128, n_seqs * heads, 128), f32),
            pltpu.VMEM((n_seqs, depth), jnp.bfloat16),
            pltpu.VMEM((4, n_seqs, width), f32),
            pltpu.VMEM((4, n_seqs, width), f32),
            pltpu.VMEM((3, n_seqs, width), f32),
            pltpu.VMEM((3, n_seqs, width), f32),
            pltpu.VMEM((n_seqs, width), f32),
            pltpu.VMEM((3, n_seqs, width), f32),
            pltpu.VMEM((4, n_seqs, width), f32),
            pltpu.SemaphoreType.DMA((2,)),
            pltpu.SemaphoreType.DMA((4, 2)),
            pltpu.SemaphoreType.DMA((4, 2)),
            pltpu.SemaphoreType.DMA((3,)),
            pltpu.SemaphoreType.DMA((3,)),
            pltpu.SemaphoreType.DMA((3,)),
            pltpu.SemaphoreType.DMA((3,)),
            pltpu.SemaphoreType.DMA((4, 2)),
            pltpu.SemaphoreType.DMA((4, 2)),
            pltpu.SemaphoreType.DMA((3, 2)),
            pltpu.SemaphoreType.DMA((3, 2)),
            pltpu.SemaphoreType.DMA((3, 2)),
            pltpu.SemaphoreType.DMA((3, 2)),
            pltpu.SemaphoreType.DMA((4, 2)),
            pltpu.SemaphoreType.DMA((4, 2)),
        ],
        compiler_params=pltpu.CompilerParams(collective_id=0, has_side_effects=True, vmem_limit_bytes=48 * 1024 * 1024),
        name="finish",
    )(terms, *early, w_uv, w_out)


def solution(mesh):
    n_dev = mesh.shape['sp']

    def local_step(hidden, ckv_blk, kpe_blk, cache_len, w_dq, q_gain, w_uq, w_dkv, kv_gain, w_uk, w_uv, w_out):
        q, kvn = project(hidden, cache_len, w_dq, q_gain, w_uq, w_dkv, kv_gain, w_uk)
        qk_dim = w_uk.shape[1] + kpe_blk.shape[2]
        kpe_blk_t = jnp.swapaxes(kpe_blk, 1, 2)
        n_early = ckv_blk.shape[0] // 2
        ckv_out, kpe_out_t, *early, kv_new = attend(q, kvn, cache_len, ckv_blk, kpe_blk_t, n_dev, qk_dim, 0, n_early)
        moved = early[:1] + [lax.ppermute(early[j], 'sp', [(s, device(s, j // 2, j % 2)) for s in range(n_dev)]) for j in range(1, n_dev)]
        ckv_out, kpe_out_t, terms = attend(q, kvn, cache_len, ckv_blk, kpe_blk_t, n_dev, qk_dim, n_early, ckv_blk.shape[0] - n_early, (ckv_out, kpe_out_t))
        out = finish(terms, moved, w_uv, w_out).astype(jnp.bfloat16)
        return out, ckv_out, jnp.swapaxes(kpe_out_t, 1, 2), kv_new

    cache_spec = P('dp', 'sp', None)
    return jax.shard_map(local_step, mesh=mesh, in_specs=(P('dp', None), cache_spec, cache_spec, P('dp'), P(), P(), P(), P(), P(), P(), P(), P()), out_specs=(P('dp', None), cache_spec, cache_spec, P('dp', None)), check_vma=False)
```

```python
import functools

import jax
import jax.numpy as jnp
import numpy as np
from jax import lax
from jax.experimental import pallas as pl
from jax.experimental.pallas import tpu as pltpu
from jax.sharding import PartitionSpec as P

EPS = 1e-6
ROPE_THETA = 10000.0
NEG_FILL = -1e30
MESH = pl.DeviceIdType.MESH
VMEM = pl.BlockSpec(memory_space=pltpu.VMEM)
SMEM = pl.BlockSpec(memory_space=pltpu.SMEM)
HBM = pl.BlockSpec(memory_space=pltpu.HBM)


def project_kernel(cfg, small_ref, hidden, w_dq, w_dkv_t, w_uq, w_uk, q_out, kvn_out,
                   dq, dkv, uq, uk, halves, q_mine, q_theirs, turn, dq_sem, dkv_sem, uq_sem, uk_sem, h_ss, h_rs, q_ss, q_rs):
    n_seqs = hidden.shape[0]
    n_k, k_rows, dq_cols = dq.shape
    n_blk, _, blk = uq.shape
    dkv_cols = dkv.shape[0]
    n_kt = cfg["n_kt"]
    k_tile = dkv.shape[1] // n_kt
    lat_dim = cfg["lat_dim"]
    nope_dim = uk.shape[1]
    heads = uk.shape[0]
    half_heads = heads // 2
    group, pitch = cfg["group"], cfg["pitch"]
    me = lax.axis_index('sp')
    c = me % 2
    partner = me - c + (1 - c)
    f32 = jnp.float32

    def load_dq(k):
        return pltpu.make_async_copy(w_dq.at[pl.ds(k * k_rows, k_rows), pl.ds(pl.multiple_of(c * dq_cols, 128), dq_cols)], dq.at[k], dq_sem.at[k])

    def load_dkv(k):
        return pltpu.make_async_copy(w_dkv_t.at[pl.ds(pl.multiple_of(c * (lat_dim // 2), 16), dkv_cols), pl.ds(k * k_tile, k_tile)], dkv.at[:, pl.ds(k * k_tile, k_tile)], dkv_sem.at[k])

    def load_uq(k):
        return pltpu.make_async_copy(w_uq.at[:, pl.ds(pl.multiple_of((c * n_blk + k) * blk, 128), blk)], uq.at[k], uq_sem.at[k])

    def load_uk(k):
        first = (c * half_heads + k * group) % heads
        return pltpu.make_async_copy(w_uk.at[pl.ds(first, group)], uk.at[pl.ds(k * group, group)], uk_sem.at[k])

    n_grp = heads // group
    per_kt = n_k // n_kt
    per_grp = n_blk // (n_grp // 2)
    loads = []
    for k in range(n_k):
        loads.append(load_dq(k))
        if k % per_kt == 0:
            loads.append(load_dkv(k // per_kt))
    for k in range(n_blk):
        loads.append(load_uq(k))
        if k % per_grp == 0:
            loads.append(load_uk(k // per_grp))
        if k >= cfg["behind"] and (k - cfg["behind"]) % per_grp == 0:
            loads.append(load_uk(n_grp // 2 + (k - cfg["behind"]) // per_grp))
    in_flight = cfg["in_flight"]
    for load in loads[:in_flight]:
        load.start()
    queue = loads[in_flight:]

    def wait_load(load):
        load.wait()
        if queue:
            queue.pop(0).start()

    barrier = pltpu.get_barrier_semaphore()
    pl.semaphore_signal(barrier, inc=1, device_id={'sp': partner}, device_id_type=MESH)
    pl.semaphore_wait(barrier, 1)

    lane = lax.broadcasted_iota(jnp.int32, (n_seqs, 128), 1)
    row = lax.broadcasted_iota(jnp.int32, (n_seqs, 128), 0)
    small = small_ref[...].reshape(1, -1)
    q_gain, kv_gain, lengths = small[:, :2 * dq_cols], small[:, 2 * dq_cols:2 * dq_cols + lat_dim], small[:, 2 * dq_cols + lat_dim:]
    position = jnp.sum(jnp.where(lane == row, lengths, 0.0), axis=1, keepdims=True)
    freq = jnp.zeros((n_seqs, 128), f32)
    for i, value in enumerate(cfg["freqs"]):
        freq = jnp.where(lane % 32 == i, value, freq)
    angle = position * freq
    cos_t = jnp.cos(angle)
    sin_t = jnp.where(lane % 64 < 32, -jnp.sin(angle), jnp.sin(angle))

    acc_q = jnp.zeros((n_seqs, dq_cols), f32)
    acc_kv = jnp.zeros((n_seqs, dkv_cols), f32)
    for k in range(n_k):
        wait_load(load_dq(k))
        acc_q = acc_q + jnp.dot(hidden[:, k * k_rows:(k + 1) * k_rows], dq[k], preferred_element_type=f32)
        if k % per_kt == per_kt - 1:
            t = k // per_kt
            wait_load(load_dkv(t))
            cols = slice(t * k_tile, (t + 1) * k_tile)
            acc_kv = acc_kv + lax.dot_general(hidden[:, cols], dkv[:, cols], (((1,), (1,)), ((), ())), preferred_element_type=f32)
    halves[c, :, dq_cols + lat_dim // 2:] = jnp.zeros((n_seqs, 128), f32)
    halves[c, :, :dq_cols] = acc_q
    halves[c, :, dq_cols:dq_cols + dkv_cols] = acc_kv
    swap = pltpu.make_async_remote_copy(src_ref=halves.at[c], dst_ref=halves.at[c], send_sem=h_ss, recv_sem=h_rs, device_id={'sp': partner}, device_id_type=MESH)
    swap.start()
    swap.wait_recv()

    lo, hi = halves[0], halves[1]
    raw_q = [lo[:, :dq_cols], hi[:, :dq_cols]]
    mean_sq = sum(jnp.sum(r * r, axis=1, keepdims=True) for r in raw_q) / (2 * dq_cols)
    inv = lax.rsqrt(mean_sq + EPS)
    c_q = jnp.concatenate([r * inv * q_gain[:, i * dq_cols:(i + 1) * dq_cols] for i, r in enumerate(raw_q)], axis=1).astype(jnp.bfloat16)

    def rotate_pair(pair):
        other = jnp.where(lane % 64 < 32, pltpu.roll(pair, 96, 1), pltpu.roll(pair, 32, 1))
        return pair * cos_t + other * sin_t

    def emit(q_blk, k, side):
        for p in range(blk // 384):
            t0, t1, t2 = (q_blk[:, p * 384 + i * 128:p * 384 + (i + 1) * 128] for i in range(3))
            odd = jnp.where(lane < 64, pltpu.roll(t1, 64, 1), pltpu.roll(t2, 64, 1))
            pe = rotate_pair(jnp.where(lane < 64, t1, t2))
            for i, (nope, rope) in enumerate(((t0, pe), (odd, pltpu.roll(pe, 64, 1)))):
                h = k * (blk // 192) + p * 2 + i
                lat = jnp.dot(nope.astype(jnp.bfloat16), uk[side * half_heads + h], preferred_element_type=f32)
                first = (h % group) * pitch
                for j in range(lat_dim // 128):
                    turn[side, j, first:first + n_seqs, :] = lat[:, j * 128:(j + 1) * 128]
                turn[side, lat_dim // 128, first:first + n_seqs, :] = rope

    def flush(first, side):
        rows = pl.ds(pl.multiple_of(first, group), group)
        for b in range(n_seqs):
            for j in range(lat_dim // 128 + 1):
                q_out[b, rows, j * 128:(j + 1) * 128] = turn[side, j, pl.ds(b, group, stride=pitch), :].astype(q_out.dtype)

    sends = []

    def own_block(k):
        wait_load(load_uq(k))
        q_blk = jnp.dot(c_q, uq[k], preferred_element_type=f32).astype(jnp.bfloat16).astype(f32)
        q_mine[k] = q_blk
        sends.append(pltpu.make_async_remote_copy(src_ref=q_mine.at[k], dst_ref=q_theirs.at[k], send_sem=q_ss.at[k], recv_sem=q_rs.at[k], device_id={'sp': partner}, device_id_type=MESH))
        if k % per_grp == 0:
            wait_load(load_uk(k // per_grp))
        emit(q_blk, k, 0)
        sends[k].start()
        if k % per_grp == per_grp - 1:
            flush(c * half_heads + (k // per_grp) * group, 0)

    def their_block(k):
        sends[k].wait_recv()
        if k % per_grp == 0:
            wait_load(load_uk(n_grp // 2 + k // per_grp))
        emit(q_theirs[k], k, 1)
        if k % per_grp == per_grp - 1:
            flush((1 - c) * half_heads + (k // per_grp) * group, 1)

    behind = cfg["behind"]
    for k in range(n_blk):
        own_block(k)
        if k >= behind:
            their_block(k - behind)
    raw_kv = [lo[:, dq_cols:dq_cols + lat_dim // 2], hi[:, dq_cols:dq_cols + lat_dim // 2]]
    mean_sq = sum(jnp.sum(r * r, axis=1, keepdims=True) for r in raw_kv) / lat_dim
    inv = lax.rsqrt(mean_sq + EPS)
    c_kv = jnp.concatenate([r * inv * kv_gain[:, i * (lat_dim // 2):(i + 1) * (lat_dim // 2)] for i, r in enumerate(raw_kv)], axis=1).astype(jnp.bfloat16)
    k_pe = rotate_pair(hi[:, dq_cols + lat_dim // 2:]).astype(jnp.bfloat16)
    kvn_out[:, :lat_dim] = c_kv.astype(f32)
    kvn_out[:, lat_dim:] = k_pe.astype(f32)

    for k in range(n_blk - behind, n_blk):
        their_block(k)
    swap.wait_send()
    for s in sends:
        s.wait_send()


def project(hidden, cache_len, w_dq, q_gain, w_uq, w_dkv, kv_gain, w_uk):
    n_seqs, d_model = hidden.shape
    heads, nope_dim, lat_dim = w_uk.shape
    q_rank = w_dq.shape[1]
    rope_dim = w_dkv.shape[1] - lat_dim
    freqs = [float(f) for f in np.power(ROPE_THETA, -2.0 * np.arange(rope_dim // 2) / rope_dim).astype(np.float32)]
    cfg = dict(n_kt=4, lat_dim=lat_dim, group=16, pitch=n_seqs + 8, in_flight=4, behind=2, freqs=freqs)
    n_k, n_blk = 8, 8
    dq_cols, dkv_cols = q_rank // 2, lat_dim // 2 + rope_dim
    blk = w_uq.shape[1] // 2 // n_blk
    f32, bf16 = jnp.float32, jnp.bfloat16
    at, small = 0, 0.0
    n_small = q_rank + lat_dim + 128
    for piece in (q_gain, kv_gain, cache_len):
        small = small + jnp.pad(piece, (at, n_small - at - piece.size)).astype(f32)
        at += piece.size
    dma = pltpu.SemaphoreType.DMA
    return pl.pallas_call(
        functools.partial(project_kernel, cfg),
        out_shape=(
            jax.ShapeDtypeStruct((n_seqs, heads, lat_dim + 128), bf16),
            jax.ShapeDtypeStruct((n_seqs, lat_dim + 128), f32),
        ),
        in_specs=[VMEM, VMEM, HBM, HBM, HBM, HBM],
        out_specs=(VMEM, VMEM),
        scratch_shapes=[
            pltpu.VMEM((n_k, d_model // n_k, dq_cols), bf16),
            pltpu.VMEM((dkv_cols, d_model), bf16),
            pltpu.VMEM((n_blk, q_rank, blk), bf16),
            pltpu.VMEM((heads, nope_dim, lat_dim), bf16),
            pltpu.VMEM((2, n_seqs, dq_cols + lat_dim // 2 + 128), f32),
            pltpu.VMEM((n_blk, n_seqs, blk), f32),
            pltpu.VMEM((n_blk, n_seqs, blk), f32),
            pltpu.VMEM((2, lat_dim // 128 + 1, cfg["group"] * cfg["pitch"], 128), f32),
            dma((n_k,)), dma((cfg["n_kt"],)), dma((n_blk,)), dma((heads // cfg["group"],)),
            dma, dma, dma((n_blk,)), dma((n_blk,)),
        ],
        compiler_params=pltpu.CompilerParams(collective_id=1, has_side_effects=True, vmem_limit_bytes=48 * 1024 * 1024),
        name="project",
    )(small, hidden, w_dq, w_dkv.T, w_uq, w_uk)


def attend_kernel(cfg, len_ref, q_ref, kvn_ref, ckv_hbm, kpe_hbm, cout_hbm, kout_hbm, terms, kv_new,
                  cbuf, kbuf, peaks, denoms, isem, osem):
    n_seqs, shard_len = ckv_hbm.shape[0], ckv_hbm.shape[1]
    lat_dim = ckv_hbm.shape[2]
    rope_dim = kpe_hbm.shape[1]
    per = terms.shape[2] - 1
    n_buf, lag, chunk = cfg["n_buf"], cfg["lag"], cfg["chunk"]
    base = lax.axis_index('sp') * shard_len

    def copies_in(b, slot):
        return (pltpu.make_async_copy(ckv_hbm.at[b], cbuf.at[slot], isem.at[slot, 0]),
                pltpu.make_async_copy(kpe_hbm.at[b], kbuf.at[slot], isem.at[slot, 1]))

    def copies_out(b, slot):
        return (pltpu.make_async_copy(cbuf.at[slot], cout_hbm.at[b], osem.at[slot, 0]),
                pltpu.make_async_copy(kbuf.at[slot], kout_hbm.at[b], osem.at[slot, 1]))

    for i in range(n_buf - lag):
        for c in copies_in(i, i):
            c.start()
    kv_new[...] = kvn_ref[:, :lat_dim + rope_dim].astype(kv_new.dtype)
    peaks[...] = jnp.zeros_like(peaks)
    denoms[...] = jnp.zeros_like(denoms)

    def step(b, carry):
        slot = lax.rem(b, n_buf)

        @pl.when(b >= lag)
        def _():
            for c in copies_out(b - lag, lax.rem(b - lag + n_buf, n_buf)):
                c.wait()

        ahead = b - lag + n_buf

        @pl.when(ahead < n_seqs)
        def _():
            for c in copies_in(ahead, lax.rem(ahead, n_buf)):
                c.start()

        for c in copies_in(b, slot):
            c.wait()
        last = len_ref[b] - base

        @pl.when((last >= 0) & (last < shard_len))
        def _():
            picked = lax.broadcasted_iota(jnp.int32, kvn_ref.shape, 0) == b
            fresh_row = jnp.sum(jnp.where(picked, kvn_ref[...], 0.0), axis=0, keepdims=True)
            r0 = pl.multiple_of((last // 16) * 16, 16)
            rows = cbuf[slot, pl.ds(r0, 16), :].astype(jnp.float32)
            row = lax.broadcasted_iota(jnp.int32, rows.shape, 0)
            cbuf[slot, pl.ds(r0, 16), :] = jnp.where(row == last - r0, fresh_row[:, :lat_dim], rows).astype(cbuf.dtype)
            c0 = pl.multiple_of((last // 128) * 128, 128)
            cols = kbuf[slot, :, pl.ds(c0, 128)].astype(jnp.float32)
            lane = lax.broadcasted_iota(jnp.int32, cols.shape, 1)
            diag = lane == lax.broadcasted_iota(jnp.int32, cols.shape, 0)
            fresh = jnp.sum(jnp.where(diag, fresh_row[:, lat_dim:], 0.0), axis=1, keepdims=True)
            kbuf[slot, :, pl.ds(c0, 128)] = jnp.where(lane == last - c0, fresh, cols).astype(kbuf.dtype)

        q_lat, q_pe = q_ref[b, :, :lat_dim], q_ref[b, :, lat_dim:lat_dim + rope_dim]
        scores = []
        for t in range(0, shard_len, chunk):
            s = lax.dot_general(q_lat, cbuf[slot, t:t + chunk, :], (((1,), (1,)), ((), ())), preferred_element_type=jnp.float32)
            s = s + jnp.dot(q_pe, kbuf[slot, :, t:t + chunk], preferred_element_type=jnp.float32)
            pos = lax.broadcasted_iota(jnp.int32, (1, chunk), 1) + t
            scores.append(jnp.where(pos <= last, s * cfg["scale"], NEG_FILL))
        peak = functools.reduce(jnp.maximum, [jnp.max(s, axis=1, keepdims=True) for s in scores])
        denom = jnp.zeros_like(peak)
        lat_sum = None
        for k, t in enumerate(range(0, shard_len, chunk)):
            w = jnp.exp(scores[k] - peak)
            denom = denom + jnp.sum(w, axis=1, keepdims=True)
            term = jnp.dot(w.astype(jnp.bfloat16), cbuf[slot, t:t + chunk, :], preferred_element_type=jnp.float32)
            lat_sum = term if lat_sum is None else lat_sum + term
        for c in copies_out(b, slot):
            c.start()
        terms[:, b // per, b % per] = lat_sum.reshape(terms.shape[0], *terms.shape[3:])
        lane = lax.broadcasted_iota(jnp.int32, peaks.shape, 1)
        peaks[...] = jnp.where(lane == b, peak, peaks[...])
        denoms[...] = jnp.where(lane == b, denom, denoms[...])
        return carry

    lax.fori_loop(0, n_seqs, step, 0)
    for part in range(2):
        terms[:, part, per, :, :128] = peaks[...].reshape(terms.shape[0], terms.shape[3], 128)
        terms[:, part, per, :, 128:256] = denoms[...].reshape(terms.shape[0], terms.shape[3], 128)
    for i in range(n_seqs - lag, n_seqs):
        for c in copies_out(i, i % n_buf):
            c.wait()


def attend(q, kvn, cache_len, ckv_blk, kpe_blk_t, n_dev, qk_dim):
    n_seqs, shard_len, lat_dim = ckv_blk.shape
    rope_dim = kpe_blk_t.shape[1]
    n_heads = q.shape[1]
    cfg = dict(n_buf=8, lag=3, chunk=512, scale=qk_dim ** -0.5)
    terms_shape = (n_dev, 2, n_seqs // 2 + 1, n_heads // n_dev, lat_dim)
    return pl.pallas_call(
        functools.partial(attend_kernel, cfg),
        out_shape=(
            jax.ShapeDtypeStruct(ckv_blk.shape, ckv_blk.dtype),
            jax.ShapeDtypeStruct(kpe_blk_t.shape, kpe_blk_t.dtype),
            jax.ShapeDtypeStruct(terms_shape, jnp.float32),
            jax.ShapeDtypeStruct((n_seqs, lat_dim + rope_dim), ckv_blk.dtype),
        ),
        in_specs=[SMEM, VMEM, VMEM, HBM, HBM],
        out_specs=(HBM, HBM, VMEM, VMEM),
        scratch_shapes=[
            pltpu.VMEM((cfg["n_buf"], shard_len, lat_dim), ckv_blk.dtype),
            pltpu.VMEM((cfg["n_buf"], rope_dim, shard_len), kpe_blk_t.dtype),
            pltpu.VMEM((n_heads, 128), jnp.float32),
            pltpu.VMEM((n_heads, 128), jnp.float32),
            pltpu.SemaphoreType.DMA((cfg["n_buf"], 2)),
            pltpu.SemaphoreType.DMA((cfg["n_buf"], 2)),
        ],
        compiler_params=pltpu.CompilerParams(vmem_limit_bytes=36 * 1024 * 1024),
        name="attend",
    )(cache_len, q, kvn, ckv_blk, kpe_blk_t)


def finish_kernel(terms, w_uv, w_out, out_ref, own, pair, from_x, from_y, uv, wo, merged, oheads, psend, precv, isend, irecv, fin, agr, agp,
                  lsem, d_ss, d_rs, x_ss, x_rs, y_ss, y_rs, p_ss, p_rs, i_ss, i_rs, a_ss, a_rs, f_ss, f_rs):
    n_seqs, width = fin.shape
    heads = uv.shape[0]
    depth = wo.shape[0]
    me = lax.axis_index('sp')
    y, x, c = me // 4, (me // 2) % 2, me % 2

    def device(q, jc):
        return ((y + q // 2) % 2) * 4 + ((x + q % 2) % 2) * 2 + (c + jc) % 2

    def send(src, dst, ss, rs, dev):
        return pltpu.make_async_remote_copy(src_ref=src, dst_ref=dst, send_sem=ss, recv_sem=rs, device_id={'sp': dev}, device_id_type=MESH)

    load_uv = pltpu.make_async_copy(w_uv.at[pl.ds(me * heads, heads)], uv, lsem.at[0])
    load_wo = pltpu.make_async_copy(w_out.at[pl.ds(me * depth, depth)], wo, lsem.at[1])
    order = ((3, 0), (3, 1), (1, 0), (2, 1), (2, 0), (1, 1), (0, 0), (0, 1))
    per = n_seqs // 2
    load_uv.start()

    others = ((0, 1), (1, 0), (2, 0), (3, 0))
    barrier = pltpu.get_barrier_semaphore()
    for q, jc in others:
        pl.semaphore_signal(barrier, inc=1, device_id={'sp': device(q, jc)}, device_id_type=MESH)
    pl.semaphore_wait(barrier, len(others))

    d_sends = {(q, h): send(terms.at[device(q, 1), h], pair.at[q, h], d_ss.at[q, h], d_rs.at[q, h], device(0, 1)) for q, h in order}
    for k in order:
        d_sends[k].start()

    def merge(dst, src, h, first=None):
        base = dst if first is None else first
        old, new = base[per, :, :128], src[per, :, :128]
        peak = jnp.maximum(old, new)
        f_old, f_new = jnp.exp(old - peak), jnp.exp(new - peak)
        dst[per, :, :128] = peak
        dst[per, :, 128:256] = f_old * base[per, :, 128:256] + f_new * src[per, :, 128:256]
        for i in range(per):
            b = h * per + i
            dst[i] = f_old[:, b:b + 1] * base[i] + f_new[:, b:b + 1] * src[i]

    def merge_pair(q, h):
        d_sends[q, h].wait_recv()
        merge(own.at[q, h], pair.at[q, h], h, terms.at[device(q, 0), h])

    x_dev, y_dev = device(1, 0), device(2, 0)
    x_sends = [send(own.at[k], from_x.at[i], x_ss.at[i], x_rs.at[i], x_dev) for i, k in enumerate(((3, 0), (1, 0), (1, 1)))]
    y_sends = [send(own.at[k], from_y.at[i], y_ss.at[i], y_rs.at[i], y_dev) for i, k in enumerate(((3, 1), (2, 1), (2, 0)))]
    merge_pair(3, 0)
    merge_pair(3, 1)
    x_sends[0].start()
    merge_pair(1, 0)
    y_sends[0].start()
    merge_pair(2, 1)
    x_sends[1].start()
    merge_pair(2, 0)
    y_sends[1].start()
    merge_pair(1, 1)
    merge_pair(0, 0)
    merge_pair(0, 1)
    load_wo.start()
    x_sends[0].wait_recv()
    merge(own.at[2, 0], from_x.at[0], 0)
    y_sends[0].wait_recv()
    merge(own.at[1, 1], from_y.at[0], 1)
    y_sends[2].start()
    x_sends[2].start()
    x_sends[1].wait_recv()
    merge(own.at[0, 0], from_x.at[1], 0)
    y_sends[1].wait_recv()
    merge(own.at[0, 1], from_y.at[1], 1)
    y_sends[2].wait_recv()
    merge(own.at[0, 0], from_y.at[2], 0)
    x_sends[2].wait_recv()
    merge(own.at[0, 1], from_x.at[2], 1)
    for h in range(2):
        inv = 1.0 / own[0, h, per, :, 128:256]
        for i in range(per):
            b = h * per + i
            acc = inv[:, b:b + 1] * own[0, h, i]
            for k in range(merged.shape[0]):
                merged[k, b * heads:(b + 1) * heads, :] = acc[:, k * 128:(k + 1) * 128]
    load_uv.wait()
    for h in range(heads):
        o_lat = jnp.concatenate([merged[k, pl.ds(h, n_seqs, stride=heads), :] for k in range(merged.shape[0])], axis=1).astype(jnp.bfloat16)
        o_h = lax.dot_general(o_lat, uv[h], (((1,), (1,)), ((), ())), preferred_element_type=jnp.float32)
        oheads[:, h * o_h.shape[1]:(h + 1) * o_h.shape[1]] = o_h.astype(jnp.bfloat16)
    load_wo.wait()

    def columns(dev, part):
        at, size = parts[part]
        return pl.ds(pl.multiple_of(dev * width + at, 128), size)

    def partial_out(dev, part):
        return jnp.dot(oheads[...], wo[:, columns(dev, part)], preferred_element_type=jnp.float32)

    parts = ((0, width // 256 * 128), (width // 256 * 128, width - width // 256 * 128))
    far = (3, 1, 2)
    p_sends, i_sends, a_sends, f_sends = {}, {}, {}, {}

    def start(waiting):
        while waiting:
            waiting.pop().start()

    def put(ref, part, value):
        ref[:, parts[part][0]:sum(parts[part])] = value

    def get(ref, part):
        return ref[:, parts[part][0]:sum(parts[part])]

    def cut(ref, part):
        return ref.at[:, pl.ds(*parts[part])]

    mine = []
    waiting = []
    for part in range(2):
        for q in far + (0,):
            put(psend.at[q], part, partial_out(device(q, 1), part))
            start(waiting)
            p_sends[q, part] = send(cut(psend.at[q], part), cut(precv.at[q], part), p_ss.at[q, part], p_rs.at[q, part], device(0, 1))
            waiting.append(p_sends[q, part])
        for q in far + (0,):
            value = partial_out(device(q, 0), part)
            start(waiting)
            p_sends[q, part].wait_recv()
            value = value + get(precv.at[q], part)
            if q:
                put(isend.at[q - 1], part, value)
                i_sends[q, part] = send(cut(isend.at[q - 1], part), cut(irecv.at[q - 1], part), i_ss.at[q - 1, part], i_rs.at[q - 1, part], device(q, 0))
                waiting.append(i_sends[q, part])
            else:
                mine.append(value)
        start(waiting)
    for part in range(2):
        for q in far:
            i_sends[q, part].wait_recv()
        result = mine[part] + get(irecv.at[0], part) + get(irecv.at[1], part) + get(irecv.at[2], part)
        put(fin, part, result)
        out_ref[:, columns(me, part)] = result
        for q in far:
            a_sends[q, part] = send(cut(fin, part), cut(agr.at[q - 1], part), a_ss.at[q - 1, part], a_rs.at[q - 1, part], device(q, 0))
            a_sends[q, part].start()
        f_sends[0, part] = send(cut(fin, part), cut(agp.at[0], part), f_ss.at[0, part], f_rs.at[0, part], device(0, 1))
        f_sends[0, part].start()
    for part in range(2):
        for q in (1, 2, 3):
            a_sends[q, part].wait_recv()
            f_sends[q, part] = send(cut(agr.at[q - 1], part), cut(agp.at[q], part), f_ss.at[q, part], f_rs.at[q, part], device(0, 1))
            f_sends[q, part].start()
            out_ref[:, columns(device(q, 0), part)] = get(agr.at[q - 1], part)
    for part in range(2):
        for q in range(4):
            f_sends[q, part].wait_recv()
            out_ref[:, columns(device(q, 1), part)] = get(agp.at[q], part)
    for s in list(d_sends.values()) + x_sends + y_sends + list(p_sends.values()) + list(i_sends.values()) + list(a_sends.values()) + list(f_sends.values()):
        s.wait_send()


def finish(terms, w_uv, w_out):
    n_dev, _, rows, heads, lat_dim = terms.shape
    n_seqs = 2 * (rows - 1)
    d_model = w_out.shape[1]
    depth = w_out.shape[0] // n_dev
    width = d_model // n_dev
    f32 = jnp.float32
    return pl.pallas_call(
        finish_kernel,
        out_shape=jax.ShapeDtypeStruct((n_seqs, d_model), f32),
        in_specs=[VMEM, HBM, HBM],
        out_specs=VMEM,
        scratch_shapes=[
            pltpu.VMEM((4, 2, rows, heads, lat_dim), f32),
            pltpu.VMEM((4, 2, rows, heads, lat_dim), f32),
            pltpu.VMEM((3, rows, heads, lat_dim), f32),
            pltpu.VMEM((3, rows, heads, lat_dim), f32),
            pltpu.VMEM((heads,) + w_uv.shape[1:], w_uv.dtype),
            pltpu.VMEM((depth, d_model), w_out.dtype),
            pltpu.VMEM((lat_dim // 128, n_seqs * heads, 128), f32),
            pltpu.VMEM((n_seqs, depth), jnp.bfloat16),
            pltpu.VMEM((4, n_seqs, width), f32),
            pltpu.VMEM((4, n_seqs, width), f32),
            pltpu.VMEM((3, n_seqs, width), f32),
            pltpu.VMEM((3, n_seqs, width), f32),
            pltpu.VMEM((n_seqs, width), f32),
            pltpu.VMEM((3, n_seqs, width), f32),
            pltpu.VMEM((4, n_seqs, width), f32),
            pltpu.SemaphoreType.DMA((2,)),
            pltpu.SemaphoreType.DMA((4, 2)),
            pltpu.SemaphoreType.DMA((4, 2)),
            pltpu.SemaphoreType.DMA((3,)),
            pltpu.SemaphoreType.DMA((3,)),
            pltpu.SemaphoreType.DMA((3,)),
            pltpu.SemaphoreType.DMA((3,)),
            pltpu.SemaphoreType.DMA((4, 2)),
            pltpu.SemaphoreType.DMA((4, 2)),
            pltpu.SemaphoreType.DMA((3, 2)),
            pltpu.SemaphoreType.DMA((3, 2)),
            pltpu.SemaphoreType.DMA((3, 2)),
            pltpu.SemaphoreType.DMA((3, 2)),
            pltpu.SemaphoreType.DMA((4, 2)),
            pltpu.SemaphoreType.DMA((4, 2)),
        ],
        compiler_params=pltpu.CompilerParams(collective_id=0, has_side_effects=True, vmem_limit_bytes=48 * 1024 * 1024),
        name="finish",
    )(terms, w_uv, w_out)


def solution(mesh):
    n_dev = mesh.shape['sp']

    def local_step(hidden, ckv_blk, kpe_blk, cache_len, w_dq, q_gain, w_uq, w_dkv, kv_gain, w_uk, w_uv, w_out):
        q, kvn = project(hidden, cache_len, w_dq, q_gain, w_uq, w_dkv, kv_gain, w_uk)
        qk_dim = w_uk.shape[1] + kpe_blk.shape[2]
        ckv_out, kpe_out_t, terms, kv_new = attend(q, kvn, cache_len, ckv_blk, jnp.swapaxes(kpe_blk, 1, 2), n_dev, qk_dim)
        out = finish(terms, w_uv, w_out).astype(jnp.bfloat16)
        return out, ckv_out, jnp.swapaxes(kpe_out_t, 1, 2), kv_new

    cache_spec = P('dp', 'sp', None)
    return jax.shard_map(local_step, mesh=mesh, in_specs=(P('dp', None), cache_spec, cache_spec, P('dp'), P(), P(), P(), P(), P(), P(), P(), P()), out_specs=(P('dp', None), cache_spec, cache_spec, P('dp', None)), check_vma=False)
```

```python
import functools

import jax
import jax.numpy as jnp
import numpy as np
from jax import lax
from jax.experimental import pallas as pl
from jax.experimental.pallas import tpu as pltpu
from jax.sharding import PartitionSpec as P

EPS = 1e-6
ROPE_THETA = 10000.0
NEG_FILL = -1e30
MESH = pl.DeviceIdType.MESH
VMEM = pl.BlockSpec(memory_space=pltpu.VMEM)
SMEM = pl.BlockSpec(memory_space=pltpu.SMEM)
HBM = pl.BlockSpec(memory_space=pltpu.HBM)


def project_kernel(cfg, small_ref, hidden, w_dq, w_dkv_t, w_uq, w_uk, q_out, kvn_out,
                   dq, dkv, uq, uk, halves, q_mine, q_theirs, turn, dq_sem, dkv_sem, uq_sem, uk_sem, h_ss, h_rs, q_ss, q_rs):
    n_seqs = hidden.shape[0]
    n_k, k_rows, dq_cols = dq.shape
    n_blk, _, blk = uq.shape
    dkv_cols = dkv.shape[0]
    n_kt = cfg["n_kt"]
    k_tile = dkv.shape[1] // n_kt
    lat_dim = cfg["lat_dim"]
    nope_dim = uk.shape[1]
    heads = uk.shape[0]
    half_heads = heads // 2
    group, pitch = cfg["group"], cfg["pitch"]
    me = lax.axis_index('sp')
    c = me % 2
    partner = me - c + (1 - c)
    f32 = jnp.float32

    def load_dq(k):
        return pltpu.make_async_copy(w_dq.at[pl.ds(k * k_rows, k_rows), pl.ds(pl.multiple_of(c * dq_cols, 128), dq_cols)], dq.at[k], dq_sem.at[k])

    def load_dkv(k):
        return pltpu.make_async_copy(w_dkv_t.at[pl.ds(pl.multiple_of(c * (lat_dim // 2), 16), dkv_cols), pl.ds(k * k_tile, k_tile)], dkv.at[:, pl.ds(k * k_tile, k_tile)], dkv_sem.at[k])

    def load_uq(k):
        return pltpu.make_async_copy(w_uq.at[:, pl.ds(pl.multiple_of((c * n_blk + k) * blk, 128), blk)], uq.at[k], uq_sem.at[k])

    def load_uk(k):
        first = (c * half_heads + k * group) % heads
        return pltpu.make_async_copy(w_uk.at[pl.ds(first, group)], uk.at[pl.ds(k * group, group)], uk_sem.at[k])

    n_grp = heads // group
    per_kt = n_k // n_kt
    per_grp = n_blk // (n_grp // 2)
    loads = []
    for k in range(n_k):
        loads.append(load_dq(k))
        if k % per_kt == 0:
            loads.append(load_dkv(k // per_kt))
    for k in range(n_blk):
        loads.append(load_uq(k))
        if k % per_grp == 0:
            loads.append(load_uk(k // per_grp))
        if k >= cfg["behind"] and (k - cfg["behind"]) % per_grp == 0:
            loads.append(load_uk(n_grp // 2 + (k - cfg["behind"]) // per_grp))
    in_flight = cfg["in_flight"]
    for load in loads[:in_flight]:
        load.start()
    queue = loads[in_flight:]

    def wait_load(load):
        load.wait()
        if queue:
            queue.pop(0).start()

    barrier = pltpu.get_barrier_semaphore()
    pl.semaphore_signal(barrier, inc=1, device_id={'sp': partner}, device_id_type=MESH)
    pl.semaphore_wait(barrier, 1)

    lane = lax.broadcasted_iota(jnp.int32, (n_seqs, 128), 1)
    row = lax.broadcasted_iota(jnp.int32, (n_seqs, 128), 0)
    small = small_ref[...].reshape(1, -1)
    q_gain, kv_gain, lengths = small[:, :2 * dq_cols], small[:, 2 * dq_cols:2 * dq_cols + lat_dim], small[:, 2 * dq_cols + lat_dim:]
    position = jnp.sum(jnp.where(lane == row, lengths, 0.0), axis=1, keepdims=True)
    freq = jnp.zeros((n_seqs, 128), f32)
    for i, value in enumerate(cfg["freqs"]):
        freq = jnp.where(lane % 32 == i, value, freq)
    angle = position * freq
    cos_t = jnp.cos(angle)
    sin_t = jnp.where(lane % 64 < 32, -jnp.sin(angle), jnp.sin(angle))

    acc_q = jnp.zeros((n_seqs, dq_cols), f32)
    acc_kv = jnp.zeros((n_seqs, dkv_cols), f32)
    for k in range(n_k):
        wait_load(load_dq(k))
        acc_q = acc_q + jnp.dot(hidden[:, k * k_rows:(k + 1) * k_rows], dq[k], preferred_element_type=f32)
        if k % per_kt == per_kt - 1:
            t = k // per_kt
            wait_load(load_dkv(t))
            cols = slice(t * k_tile, (t + 1) * k_tile)
            acc_kv = acc_kv + lax.dot_general(hidden[:, cols], dkv[:, cols], (((1,), (1,)), ((), ())), preferred_element_type=f32)
    halves[c, :, dq_cols + lat_dim // 2:] = jnp.zeros((n_seqs, 128), f32)
    halves[c, :, :dq_cols] = acc_q
    halves[c, :, dq_cols:dq_cols + dkv_cols] = acc_kv
    swap = pltpu.make_async_remote_copy(src_ref=halves.at[c], dst_ref=halves.at[c], send_sem=h_ss, recv_sem=h_rs, device_id={'sp': partner}, device_id_type=MESH)
    swap.start()
    swap.wait_recv()

    lo, hi = halves[0], halves[1]
    raw_q = [lo[:, :dq_cols], hi[:, :dq_cols]]
    mean_sq = sum(jnp.sum(r * r, axis=1, keepdims=True) for r in raw_q) / (2 * dq_cols)
    inv = lax.rsqrt(mean_sq + EPS)
    c_q = jnp.concatenate([r * inv * q_gain[:, i * dq_cols:(i + 1) * dq_cols] for i, r in enumerate(raw_q)], axis=1).astype(jnp.bfloat16)

    def rotate_pair(pair):
        other = jnp.where(lane % 64 < 32, pltpu.roll(pair, 96, 1), pltpu.roll(pair, 32, 1))
        return pair * cos_t + other * sin_t

    def emit(q_blk, k, side):
        for p in range(blk // 384):
            t0, t1, t2 = (q_blk[:, p * 384 + i * 128:p * 384 + (i + 1) * 128] for i in range(3))
            odd = jnp.where(lane < 64, pltpu.roll(t1, 64, 1), pltpu.roll(t2, 64, 1))
            pe = rotate_pair(jnp.where(lane < 64, t1, t2))
            for i, (nope, rope) in enumerate(((t0, pe), (odd, pltpu.roll(pe, 64, 1)))):
                h = k * (blk // 192) + p * 2 + i
                lat = jnp.dot(nope.astype(jnp.bfloat16), uk[side * half_heads + h], preferred_element_type=f32)
                first = (h % group) * pitch
                for j in range(lat_dim // 128):
                    turn[side, j, first:first + n_seqs, :] = lat[:, j * 128:(j + 1) * 128]
                turn[side, lat_dim // 128, first:first + n_seqs, :] = rope

    def flush(first, side):
        rows = pl.ds(pl.multiple_of(first, group), group)
        for b in range(n_seqs):
            for j in range(lat_dim // 128 + 1):
                q_out[b, rows, j * 128:(j + 1) * 128] = turn[side, j, pl.ds(b, group, stride=pitch), :].astype(q_out.dtype)

    sends = []

    def own_block(k):
        wait_load(load_uq(k))
        q_blk = jnp.dot(c_q, uq[k], preferred_element_type=f32).astype(jnp.bfloat16).astype(f32)
        q_mine[k] = q_blk
        sends.append(pltpu.make_async_remote_copy(src_ref=q_mine.at[k], dst_ref=q_theirs.at[k], send_sem=q_ss.at[k], recv_sem=q_rs.at[k], device_id={'sp': partner}, device_id_type=MESH))
        if k % per_grp == 0:
            wait_load(load_uk(k // per_grp))
        emit(q_blk, k, 0)
        sends[k].start()
        if k % per_grp == per_grp - 1:
            flush(c * half_heads + (k // per_grp) * group, 0)

    def their_block(k):
        sends[k].wait_recv()
        if k % per_grp == 0:
            wait_load(load_uk(n_grp // 2 + k // per_grp))
        emit(q_theirs[k], k, 1)
        if k % per_grp == per_grp - 1:
            flush((1 - c) * half_heads + (k // per_grp) * group, 1)

    behind = cfg["behind"]
    for k in range(n_blk):
        own_block(k)
        if k >= behind:
            their_block(k - behind)
    raw_kv = [lo[:, dq_cols:dq_cols + lat_dim // 2], hi[:, dq_cols:dq_cols + lat_dim // 2]]
    mean_sq = sum(jnp.sum(r * r, axis=1, keepdims=True) for r in raw_kv) / lat_dim
    inv = lax.rsqrt(mean_sq + EPS)
    c_kv = jnp.concatenate([r * inv * kv_gain[:, i * (lat_dim // 2):(i + 1) * (lat_dim // 2)] for i, r in enumerate(raw_kv)], axis=1).astype(jnp.bfloat16)
    k_pe = rotate_pair(hi[:, dq_cols + lat_dim // 2:]).astype(jnp.bfloat16)
    kvn_out[:, :lat_dim] = c_kv.astype(f32)
    kvn_out[:, lat_dim:] = k_pe.astype(f32)

    for k in range(n_blk - behind, n_blk):
        their_block(k)
    swap.wait_send()
    for s in sends:
        s.wait_send()


def project(hidden, cache_len, w_dq, q_gain, w_uq, w_dkv, kv_gain, w_uk):
    n_seqs, d_model = hidden.shape
    heads, nope_dim, lat_dim = w_uk.shape
    q_rank = w_dq.shape[1]
    rope_dim = w_dkv.shape[1] - lat_dim
    freqs = [float(f) for f in np.power(ROPE_THETA, -2.0 * np.arange(rope_dim // 2) / rope_dim).astype(np.float32)]
    cfg = dict(n_kt=4, lat_dim=lat_dim, group=16, pitch=n_seqs + 8, in_flight=6, behind=2, freqs=freqs)
    n_k, n_blk = 8, 8
    dq_cols, dkv_cols = q_rank // 2, lat_dim // 2 + rope_dim
    blk = w_uq.shape[1] // 2 // n_blk
    f32, bf16 = jnp.float32, jnp.bfloat16
    at, small = 0, 0.0
    n_small = q_rank + lat_dim + 128
    for piece in (q_gain, kv_gain, cache_len):
        small = small + jnp.pad(piece, (at, n_small - at - piece.size)).astype(f32)
        at += piece.size
    dma = pltpu.SemaphoreType.DMA
    return pl.pallas_call(
        functools.partial(project_kernel, cfg),
        out_shape=(
            jax.ShapeDtypeStruct((n_seqs, heads, lat_dim + 128), bf16),
            jax.ShapeDtypeStruct((n_seqs, lat_dim + 128), f32),
        ),
        in_specs=[VMEM, VMEM, HBM, HBM, HBM, HBM],
        out_specs=(VMEM, VMEM),
        scratch_shapes=[
            pltpu.VMEM((n_k, d_model // n_k, dq_cols), bf16),
            pltpu.VMEM((dkv_cols, d_model), bf16),
            pltpu.VMEM((n_blk, q_rank, blk), bf16),
            pltpu.VMEM((heads, nope_dim, lat_dim), bf16),
            pltpu.VMEM((2, n_seqs, dq_cols + lat_dim // 2 + 128), f32),
            pltpu.VMEM((n_blk, n_seqs, blk), f32),
            pltpu.VMEM((n_blk, n_seqs, blk), f32),
            pltpu.VMEM((2, lat_dim // 128 + 1, cfg["group"] * cfg["pitch"], 128), f32),
            dma((n_k,)), dma((cfg["n_kt"],)), dma((n_blk,)), dma((heads // cfg["group"],)),
            dma, dma, dma((n_blk,)), dma((n_blk,)),
        ],
        compiler_params=pltpu.CompilerParams(collective_id=1, has_side_effects=True, vmem_limit_bytes=48 * 1024 * 1024),
        name="project",
    )(small, hidden, w_dq, w_dkv.T, w_uq, w_uk)


def attend_kernel(cfg, len_ref, q_ref, kvn_ref, ckv_hbm, kpe_hbm, cout_hbm, kout_hbm, terms, kv_new,
                  cbuf, kbuf, peaks, denoms, isem, osem):
    n_seqs, shard_len = ckv_hbm.shape[0], ckv_hbm.shape[1]
    lat_dim = ckv_hbm.shape[2]
    rope_dim = kpe_hbm.shape[1]
    per = terms.shape[2] - 1
    n_buf, lag, chunk = cfg["n_buf"], cfg["lag"], cfg["chunk"]
    base = lax.axis_index('sp') * shard_len

    def copies_in(b, slot):
        return (pltpu.make_async_copy(ckv_hbm.at[b], cbuf.at[slot], isem.at[slot, 0]),
                pltpu.make_async_copy(kpe_hbm.at[b], kbuf.at[slot], isem.at[slot, 1]))

    def copies_out(b, slot):
        return (pltpu.make_async_copy(cbuf.at[slot], cout_hbm.at[b], osem.at[slot, 0]),
                pltpu.make_async_copy(kbuf.at[slot], kout_hbm.at[b], osem.at[slot, 1]))

    for i in range(n_buf - lag):
        for c in copies_in(i, i):
            c.start()
    kv_new[...] = kvn_ref[:, :lat_dim + rope_dim].astype(kv_new.dtype)
    peaks[...] = jnp.zeros_like(peaks)
    denoms[...] = jnp.zeros_like(denoms)

    def step(b, carry):
        slot = lax.rem(b, n_buf)

        @pl.when(b >= lag)
        def _():
            for c in copies_out(b - lag, lax.rem(b - lag + n_buf, n_buf)):
                c.wait()

        ahead = b - lag + n_buf

        @pl.when(ahead < n_seqs)
        def _():
            for c in copies_in(ahead, lax.rem(ahead, n_buf)):
                c.start()

        for c in copies_in(b, slot):
            c.wait()
        last = len_ref[b] - base

        @pl.when((last >= 0) & (last < shard_len))
        def _():
            picked = lax.broadcasted_iota(jnp.int32, kvn_ref.shape, 0) == b
            fresh_row = jnp.sum(jnp.where(picked, kvn_ref[...], 0.0), axis=0, keepdims=True)
            r0 = pl.multiple_of((last // 16) * 16, 16)
            rows = cbuf[slot, pl.ds(r0, 16), :].astype(jnp.float32)
            row = lax.broadcasted_iota(jnp.int32, rows.shape, 0)
            cbuf[slot, pl.ds(r0, 16), :] = jnp.where(row == last - r0, fresh_row[:, :lat_dim], rows).astype(cbuf.dtype)
            c0 = pl.multiple_of((last // 128) * 128, 128)
            cols = kbuf[slot, :, pl.ds(c0, 128)].astype(jnp.float32)
            lane = lax.broadcasted_iota(jnp.int32, cols.shape, 1)
            diag = lane == lax.broadcasted_iota(jnp.int32, cols.shape, 0)
            fresh = jnp.sum(jnp.where(diag, fresh_row[:, lat_dim:], 0.0), axis=1, keepdims=True)
            kbuf[slot, :, pl.ds(c0, 128)] = jnp.where(lane == last - c0, fresh, cols).astype(kbuf.dtype)

        q_lat, q_pe = q_ref[b, :, :lat_dim], q_ref[b, :, lat_dim:lat_dim + rope_dim]
        scores = []
        for t in range(0, shard_len, chunk):
            s = lax.dot_general(q_lat, cbuf[slot, t:t + chunk, :], (((1,), (1,)), ((), ())), preferred_element_type=jnp.float32)
            s = s + jnp.dot(q_pe, kbuf[slot, :, t:t + chunk], preferred_element_type=jnp.float32)
            pos = lax.broadcasted_iota(jnp.int32, (1, chunk), 1) + t
            scores.append(jnp.where(pos <= last, s * cfg["scale"], NEG_FILL))
        peak = functools.reduce(jnp.maximum, [jnp.max(s, axis=1, keepdims=True) for s in scores])
        denom = jnp.zeros_like(peak)
        lat_sum = None
        for k, t in enumerate(range(0, shard_len, chunk)):
            w = jnp.exp(scores[k] - peak)
            denom = denom + jnp.sum(w, axis=1, keepdims=True)
            term = jnp.dot(w.astype(jnp.bfloat16), cbuf[slot, t:t + chunk, :], preferred_element_type=jnp.float32)
            lat_sum = term if lat_sum is None else lat_sum + term
        for c in copies_out(b, slot):
            c.start()
        terms[:, b // per, b % per] = lat_sum.reshape(terms.shape[0], *terms.shape[3:])
        lane = lax.broadcasted_iota(jnp.int32, peaks.shape, 1)
        peaks[...] = jnp.where(lane == b, peak, peaks[...])
        denoms[...] = jnp.where(lane == b, denom, denoms[...])
        return carry

    lax.fori_loop(0, n_seqs, step, 0)
    for part in range(2):
        terms[:, part, per, :, :128] = peaks[...].reshape(terms.shape[0], terms.shape[3], 128)
        terms[:, part, per, :, 128:256] = denoms[...].reshape(terms.shape[0], terms.shape[3], 128)
    for i in range(n_seqs - lag, n_seqs):
        for c in copies_out(i, i % n_buf):
            c.wait()


def attend(q, kvn, cache_len, ckv_blk, kpe_blk_t, n_dev, qk_dim):
    n_seqs, shard_len, lat_dim = ckv_blk.shape
    rope_dim = kpe_blk_t.shape[1]
    n_heads = q.shape[1]
    cfg = dict(n_buf=8, lag=3, chunk=512, scale=qk_dim ** -0.5)
    terms_shape = (n_dev, 2, n_seqs // 2 + 1, n_heads // n_dev, lat_dim)
    return pl.pallas_call(
        functools.partial(attend_kernel, cfg),
        out_shape=(
            jax.ShapeDtypeStruct(ckv_blk.shape, ckv_blk.dtype),
            jax.ShapeDtypeStruct(kpe_blk_t.shape, kpe_blk_t.dtype),
            jax.ShapeDtypeStruct(terms_shape, jnp.float32),
            jax.ShapeDtypeStruct((n_seqs, lat_dim + rope_dim), ckv_blk.dtype),
        ),
        in_specs=[SMEM, VMEM, VMEM, HBM, HBM],
        out_specs=(HBM, HBM, VMEM, VMEM),
        scratch_shapes=[
            pltpu.VMEM((cfg["n_buf"], shard_len, lat_dim), ckv_blk.dtype),
            pltpu.VMEM((cfg["n_buf"], rope_dim, shard_len), kpe_blk_t.dtype),
            pltpu.VMEM((n_heads, 128), jnp.float32),
            pltpu.VMEM((n_heads, 128), jnp.float32),
            pltpu.SemaphoreType.DMA((cfg["n_buf"], 2)),
            pltpu.SemaphoreType.DMA((cfg["n_buf"], 2)),
        ],
        compiler_params=pltpu.CompilerParams(vmem_limit_bytes=36 * 1024 * 1024),
        name="attend",
    )(cache_len, q, kvn, ckv_blk, kpe_blk_t)


def finish_kernel(terms, w_uv, w_out, out_ref, own, pair, from_x, from_y, uv, wo, merged, oheads, psend, precv, isend, irecv, fin, agr, agp,
                  lsem, d_ss, d_rs, x_ss, x_rs, y_ss, y_rs, p_ss, p_rs, i_ss, i_rs, a_ss, a_rs, f_ss, f_rs):
    n_seqs, width = fin.shape
    heads = uv.shape[0]
    depth = wo.shape[0]
    me = lax.axis_index('sp')
    y, x, c = me // 4, (me // 2) % 2, me % 2

    def device(q, jc):
        return ((y + q // 2) % 2) * 4 + ((x + q % 2) % 2) * 2 + (c + jc) % 2

    def send(src, dst, ss, rs, dev):
        return pltpu.make_async_remote_copy(src_ref=src, dst_ref=dst, send_sem=ss, recv_sem=rs, device_id={'sp': dev}, device_id_type=MESH)

    load_uv = pltpu.make_async_copy(w_uv.at[pl.ds(me * heads, heads)], uv, lsem.at[0])
    load_wo = pltpu.make_async_copy(w_out.at[pl.ds(me * depth, depth)], wo, lsem.at[1])
    order = ((3, 0), (3, 1), (1, 0), (2, 1), (2, 0), (1, 1), (0, 0), (0, 1))
    per = n_seqs // 2
    load_uv.start()

    others = ((0, 1), (1, 0), (2, 0), (3, 0))
    barrier = pltpu.get_barrier_semaphore()
    for q, jc in others:
        pl.semaphore_signal(barrier, inc=1, device_id={'sp': device(q, jc)}, device_id_type=MESH)
    pl.semaphore_wait(barrier, len(others))

    d_sends = {(q, h): send(terms.at[device(q, 1), h], pair.at[q, h], d_ss.at[q, h], d_rs.at[q, h], device(0, 1)) for q, h in order}
    for k in order:
        d_sends[k].start()

    def merge(dst, src, h, first=None):
        base = dst if first is None else first
        old, new = base[per, :, :128], src[per, :, :128]
        peak = jnp.maximum(old, new)
        f_old, f_new = jnp.exp(old - peak), jnp.exp(new - peak)
        dst[per, :, :128] = peak
        dst[per, :, 128:256] = f_old * base[per, :, 128:256] + f_new * src[per, :, 128:256]
        for i in range(per):
            b = h * per + i
            dst[i] = f_old[:, b:b + 1] * base[i] + f_new[:, b:b + 1] * src[i]

    def merge_pair(q, h):
        d_sends[q, h].wait_recv()
        merge(own.at[q, h], pair.at[q, h], h, terms.at[device(q, 0), h])

    x_dev, y_dev = device(1, 0), device(2, 0)

    class Both:
        def __init__(self, src, dst, ss, rs, dev):
            body, tail = pl.ds(0, per), pl.ds(0, 256)
            self.copies = (send(src.at[body], dst.at[body], ss.at[0], rs.at[0], dev), send(src.at[per, :, tail], dst.at[per, :, tail], ss.at[1], rs.at[1], dev))

        def start(self):
            for copy in self.copies:
                copy.start()

        def wait_recv(self):
            for copy in self.copies:
                copy.wait_recv()

        def wait_send(self):
            for copy in self.copies:
                copy.wait_send()

    x_sends = [Both(own.at[k], from_x.at[i], x_ss.at[i], x_rs.at[i], x_dev) for i, k in enumerate(((3, 0), (1, 0), (1, 1)))]
    y_sends = [Both(own.at[k], from_y.at[i], y_ss.at[i], y_rs.at[i], y_dev) for i, k in enumerate(((3, 1), (2, 1), (2, 0)))]
    merge_pair(3, 0)
    merge_pair(3, 1)
    x_sends[0].start()
    merge_pair(1, 0)
    y_sends[0].start()
    merge_pair(2, 1)
    x_sends[1].start()
    merge_pair(2, 0)
    y_sends[1].start()
    merge_pair(1, 1)
    merge_pair(0, 0)
    merge_pair(0, 1)
    load_wo.start()
    x_sends[0].wait_recv()
    merge(own.at[2, 0], from_x.at[0], 0)
    y_sends[0].wait_recv()
    merge(own.at[1, 1], from_y.at[0], 1)
    y_sends[2].start()
    x_sends[2].start()
    x_sends[1].wait_recv()
    merge(own.at[0, 0], from_x.at[1], 0)
    y_sends[1].wait_recv()
    merge(own.at[0, 1], from_y.at[1], 1)
    y_sends[2].wait_recv()
    merge(own.at[0, 0], from_y.at[2], 0)
    x_sends[2].wait_recv()
    merge(own.at[0, 1], from_x.at[2], 1)
    for h in range(2):
        inv = 1.0 / own[0, h, per, :, 128:256]
        for i in range(per):
            b = h * per + i
            acc = inv[:, b:b + 1] * own[0, h, i]
            for k in range(merged.shape[0]):
                merged[k, b * heads:(b + 1) * heads, :] = acc[:, k * 128:(k + 1) * 128]
    load_uv.wait()
    for h in range(heads):
        o_lat = jnp.concatenate([merged[k, pl.ds(h, n_seqs, stride=heads), :] for k in range(merged.shape[0])], axis=1).astype(jnp.bfloat16)
        o_h = lax.dot_general(o_lat, uv[h], (((1,), (1,)), ((), ())), preferred_element_type=jnp.float32)
        oheads[:, h * o_h.shape[1]:(h + 1) * o_h.shape[1]] = o_h.astype(jnp.bfloat16)
    load_wo.wait()

    def columns(dev, part):
        at, size = parts[part]
        return pl.ds(pl.multiple_of(dev * width + at, 128), size)

    def partial_out(dev, part):
        return jnp.dot(oheads[...], wo[:, columns(dev, part)], preferred_element_type=jnp.float32)

    parts = ((0, width // 256 * 128), (width // 256 * 128, width - width // 256 * 128))
    far = (3, 1, 2)
    p_sends, i_sends, a_sends, f_sends = {}, {}, {}, {}

    def start(waiting):
        while waiting:
            waiting.pop().start()

    def put(ref, part, value):
        ref[:, parts[part][0]:sum(parts[part])] = value

    def get(ref, part):
        return ref[:, parts[part][0]:sum(parts[part])]

    def cut(ref, part):
        return ref.at[:, pl.ds(*parts[part])]

    mine = []
    waiting = []
    for part in range(2):
        for q in far + (0,):
            put(psend.at[q], part, partial_out(device(q, 1), part))
            start(waiting)
            p_sends[q, part] = send(cut(psend.at[q], part), cut(precv.at[q], part), p_ss.at[q, part], p_rs.at[q, part], device(0, 1))
            waiting.append(p_sends[q, part])
        for q in far + (0,):
            value = partial_out(device(q, 0), part)
            start(waiting)
            p_sends[q, part].wait_recv()
            value = value + get(precv.at[q], part)
            if q:
                put(isend.at[q - 1], part, value)
                i_sends[q, part] = send(cut(isend.at[q - 1], part), cut(irecv.at[q - 1], part), i_ss.at[q - 1, part], i_rs.at[q - 1, part], device(q, 0))
                waiting.append(i_sends[q, part])
            else:
                mine.append(value)
        start(waiting)
    for part in range(2):
        for q in far:
            i_sends[q, part].wait_recv()
        result = mine[part] + get(irecv.at[0], part) + get(irecv.at[1], part) + get(irecv.at[2], part)
        put(fin, part, result)
        out_ref[:, columns(me, part)] = result
        for q in far:
            a_sends[q, part] = send(cut(fin, part), cut(agr.at[q - 1], part), a_ss.at[q - 1, part], a_rs.at[q - 1, part], device(q, 0))
            a_sends[q, part].start()
        f_sends[0, part] = send(cut(fin, part), cut(agp.at[0], part), f_ss.at[0, part], f_rs.at[0, part], device(0, 1))
        f_sends[0, part].start()
    for part in range(2):
        for q in (1, 2, 3):
            a_sends[q, part].wait_recv()
            f_sends[q, part] = send(cut(agr.at[q - 1], part), cut(agp.at[q], part), f_ss.at[q, part], f_rs.at[q, part], device(0, 1))
            f_sends[q, part].start()
            out_ref[:, columns(device(q, 0), part)] = get(agr.at[q - 1], part)
    for part in range(2):
        for q in range(4):
            f_sends[q, part].wait_recv()
            out_ref[:, columns(device(q, 1), part)] = get(agp.at[q], part)
    for s in list(d_sends.values()) + x_sends + y_sends + list(p_sends.values()) + list(i_sends.values()) + list(a_sends.values()) + list(f_sends.values()):
        s.wait_send()


def finish(terms, w_uv, w_out):
    n_dev, _, rows, heads, lat_dim = terms.shape
    n_seqs = 2 * (rows - 1)
    d_model = w_out.shape[1]
    depth = w_out.shape[0] // n_dev
    width = d_model // n_dev
    f32 = jnp.float32
    return pl.pallas_call(
        finish_kernel,
        out_shape=jax.ShapeDtypeStruct((n_seqs, d_model), f32),
        in_specs=[VMEM, HBM, HBM],
        out_specs=VMEM,
        scratch_shapes=[
            pltpu.VMEM((4, 2, rows, heads, lat_dim), f32),
            pltpu.VMEM((4, 2, rows, heads, lat_dim), f32),
            pltpu.VMEM((3, rows, heads, lat_dim), f32),
            pltpu.VMEM((3, rows, heads, lat_dim), f32),
            pltpu.VMEM((heads,) + w_uv.shape[1:], w_uv.dtype),
            pltpu.VMEM((depth, d_model), w_out.dtype),
            pltpu.VMEM((lat_dim // 128, n_seqs * heads, 128), f32),
            pltpu.VMEM((n_seqs, depth), jnp.bfloat16),
            pltpu.VMEM((4, n_seqs, width), f32),
            pltpu.VMEM((4, n_seqs, width), f32),
            pltpu.VMEM((3, n_seqs, width), f32),
            pltpu.VMEM((3, n_seqs, width), f32),
            pltpu.VMEM((n_seqs, width), f32),
            pltpu.VMEM((3, n_seqs, width), f32),
            pltpu.VMEM((4, n_seqs, width), f32),
            pltpu.SemaphoreType.DMA((2,)),
            pltpu.SemaphoreType.DMA((4, 2)),
            pltpu.SemaphoreType.DMA((4, 2)),
            pltpu.SemaphoreType.DMA((3, 2)),
            pltpu.SemaphoreType.DMA((3, 2)),
            pltpu.SemaphoreType.DMA((3, 2)),
            pltpu.SemaphoreType.DMA((3, 2)),
            pltpu.SemaphoreType.DMA((4, 2)),
            pltpu.SemaphoreType.DMA((4, 2)),
            pltpu.SemaphoreType.DMA((3, 2)),
            pltpu.SemaphoreType.DMA((3, 2)),
            pltpu.SemaphoreType.DMA((3, 2)),
            pltpu.SemaphoreType.DMA((3, 2)),
            pltpu.SemaphoreType.DMA((4, 2)),
            pltpu.SemaphoreType.DMA((4, 2)),
        ],
        compiler_params=pltpu.CompilerParams(collective_id=0, has_side_effects=True, vmem_limit_bytes=48 * 1024 * 1024),
        name="finish",
    )(terms, w_uv, w_out)


def solution(mesh):
    n_dev = mesh.shape['sp']

    def local_step(hidden, ckv_blk, kpe_blk, cache_len, w_dq, q_gain, w_uq, w_dkv, kv_gain, w_uk, w_uv, w_out):
        q, kvn = project(hidden, cache_len, w_dq, q_gain, w_uq, w_dkv, kv_gain, w_uk)
        qk_dim = w_uk.shape[1] + kpe_blk.shape[2]
        ckv_out, kpe_out_t, terms, kv_new = attend(q, kvn, cache_len, ckv_blk, jnp.swapaxes(kpe_blk, 1, 2), n_dev, qk_dim)
        out = finish(terms, w_uv, w_out).astype(jnp.bfloat16)
        return out, ckv_out, jnp.swapaxes(kpe_out_t, 1, 2), kv_new

    cache_spec = P('dp', 'sp', None)
    return jax.shard_map(local_step, mesh=mesh, in_specs=(P('dp', None), cache_spec, cache_spec, P('dp'), P(), P(), P(), P(), P(), P(), P(), P()), out_specs=(P('dp', None), cache_spec, cache_spec, P('dp', None)), check_vma=False)
```

```python
import functools

import jax
import jax.numpy as jnp
import numpy as np
from jax import lax
from jax.experimental import pallas as pl
from jax.experimental.pallas import tpu as pltpu
from jax.sharding import PartitionSpec as P

EPS = 1e-6
ROPE_THETA = 10000.0
NEG_FILL = -1e30
MESH = pl.DeviceIdType.MESH
VMEM = pl.BlockSpec(memory_space=pltpu.VMEM)
SMEM = pl.BlockSpec(memory_space=pltpu.SMEM)
HBM = pl.BlockSpec(memory_space=pltpu.HBM)


def project_kernel(cfg, small_ref, hidden, w_dq, w_dkv_t, w_uq, w_uk, q_out, kvn_out,
                   dq, dkv, uq, uk, halves, q_mine, q_theirs, turn, dq_sem, dkv_sem, uq_sem, uk_sem, h_ss, h_rs, q_ss, q_rs):
    n_seqs = hidden.shape[0]
    n_k, k_rows, dq_cols = dq.shape
    n_blk, _, blk = uq.shape
    dkv_cols = dkv.shape[0]
    n_kt = cfg["n_kt"]
    k_tile = dkv.shape[1] // n_kt
    lat_dim = cfg["lat_dim"]
    nope_dim = uk.shape[1]
    heads = uk.shape[0]
    half_heads = heads // 2
    group, pitch = cfg["group"], cfg["pitch"]
    me = lax.axis_index('sp')
    c = me % 2
    partner = me - c + (1 - c)
    f32 = jnp.float32

    def load_dq(k):
        return pltpu.make_async_copy(w_dq.at[pl.ds(k * k_rows, k_rows), pl.ds(pl.multiple_of(c * dq_cols, 128), dq_cols)], dq.at[k], dq_sem.at[k])

    def load_dkv(k):
        return pltpu.make_async_copy(w_dkv_t.at[pl.ds(pl.multiple_of(c * (lat_dim // 2), 16), dkv_cols), pl.ds(k * k_tile, k_tile)], dkv.at[:, pl.ds(k * k_tile, k_tile)], dkv_sem.at[k])

    def load_uq(k):
        return pltpu.make_async_copy(w_uq.at[:, pl.ds(pl.multiple_of((c * n_blk + k) * blk, 128), blk)], uq.at[k], uq_sem.at[k])

    def load_uk(k):
        first = (c * half_heads + k * group) % heads
        return pltpu.make_async_copy(w_uk.at[pl.ds(first, group)], uk.at[pl.ds(k * group, group)], uk_sem.at[k])

    n_grp = heads // group
    per_kt = n_k // n_kt
    per_grp = n_blk // (n_grp // 2)
    loads = []
    for k in range(n_k):
        loads.append(load_dq(k))
        if k % per_kt == 0:
            loads.append(load_dkv(k // per_kt))
    for k in range(n_blk):
        loads.append(load_uq(k))
        if k % per_grp == 0:
            loads.append(load_uk(k // per_grp))
        if k >= cfg["behind"] and (k - cfg["behind"]) % per_grp == 0:
            loads.append(load_uk(n_grp // 2 + (k - cfg["behind"]) // per_grp))
    in_flight = cfg["in_flight"]
    for load in loads[:in_flight]:
        load.start()
    queue = loads[in_flight:]

    def wait_load(load):
        load.wait()
        if queue:
            queue.pop(0).start()

    barrier = pltpu.get_barrier_semaphore()
    pl.semaphore_signal(barrier, inc=1, device_id={'sp': partner}, device_id_type=MESH)
    pl.semaphore_wait(barrier, 1)

    lane = lax.broadcasted_iota(jnp.int32, (n_seqs, 128), 1)
    row = lax.broadcasted_iota(jnp.int32, (n_seqs, 128), 0)
    small = small_ref[...].reshape(1, -1)
    q_gain, kv_gain, lengths = small[:, :2 * dq_cols], small[:, 2 * dq_cols:2 * dq_cols + lat_dim], small[:, 2 * dq_cols + lat_dim:]
    position = jnp.sum(jnp.where(lane == row, lengths, 0.0), axis=1, keepdims=True)
    freq = jnp.zeros((n_seqs, 128), f32)
    for i, value in enumerate(cfg["freqs"]):
        freq = jnp.where(lane % 32 == i, value, freq)
    angle = position * freq
    cos_t = jnp.cos(angle)
    sin_t = jnp.where(lane % 64 < 32, -jnp.sin(angle), jnp.sin(angle))

    acc_q = jnp.zeros((n_seqs, dq_cols), f32)
    acc_kv = jnp.zeros((n_seqs, dkv_cols), f32)
    for k in range(n_k):
        wait_load(load_dq(k))
        acc_q = acc_q + jnp.dot(hidden[:, k * k_rows:(k + 1) * k_rows], dq[k], preferred_element_type=f32)
        if k % per_kt == per_kt - 1:
            t = k // per_kt
            wait_load(load_dkv(t))
            cols = slice(t * k_tile, (t + 1) * k_tile)
            acc_kv = acc_kv + lax.dot_general(hidden[:, cols], dkv[:, cols], (((1,), (1,)), ((), ())), preferred_element_type=f32)
    halves[c, :, dq_cols + lat_dim // 2:] = jnp.zeros((n_seqs, 128), f32)
    halves[c, :, :dq_cols] = acc_q
    halves[c, :, dq_cols:dq_cols + dkv_cols] = acc_kv
    swap = pltpu.make_async_remote_copy(src_ref=halves.at[c], dst_ref=halves.at[c], send_sem=h_ss, recv_sem=h_rs, device_id={'sp': partner}, device_id_type=MESH)
    swap.start()
    swap.wait_recv()

    lo, hi = halves[0], halves[1]
    raw_q = [lo[:, :dq_cols], hi[:, :dq_cols]]
    mean_sq = sum(jnp.sum(r * r, axis=1, keepdims=True) for r in raw_q) / (2 * dq_cols)
    inv = lax.rsqrt(mean_sq + EPS)
    c_q = jnp.concatenate([r * inv * q_gain[:, i * dq_cols:(i + 1) * dq_cols] for i, r in enumerate(raw_q)], axis=1).astype(jnp.bfloat16)

    def rotate_pair(pair):
        other = jnp.where(lane % 64 < 32, pltpu.roll(pair, 96, 1), pltpu.roll(pair, 32, 1))
        return pair * cos_t + other * sin_t

    def emit(q_blk, k, side):
        for p in range(blk // 384):
            t0, t1, t2 = (q_blk[:, p * 384 + i * 128:p * 384 + (i + 1) * 128] for i in range(3))
            odd = jnp.where(lane < 64, pltpu.roll(t1, 64, 1), pltpu.roll(t2, 64, 1))
            pe = rotate_pair(jnp.where(lane < 64, t1, t2))
            for i, (nope, rope) in enumerate(((t0, pe), (odd, pltpu.roll(pe, 64, 1)))):
                h = k * (blk // 192) + p * 2 + i
                lat = jnp.dot(nope.astype(jnp.bfloat16), uk[side * half_heads + h], preferred_element_type=f32)
                first = (h % group) * pitch
                for j in range(lat_dim // 128):
                    turn[side, j, first:first + n_seqs, :] = lat[:, j * 128:(j + 1) * 128]
                turn[side, lat_dim // 128, first:first + n_seqs, :] = rope

    def flush(first, side):
        rows = pl.ds(pl.multiple_of(first, group), group)
        for b in range(n_seqs):
            for j in range(lat_dim // 128 + 1):
                q_out[b, rows, j * 128:(j + 1) * 128] = turn[side, j, pl.ds(b, group, stride=pitch), :].astype(q_out.dtype)

    sends = []

    def own_block(k):
        wait_load(load_uq(k))
        q_blk = jnp.dot(c_q, uq[k], preferred_element_type=f32).astype(jnp.bfloat16).astype(f32)
        q_mine[k] = q_blk
        sends.append(pltpu.make_async_remote_copy(src_ref=q_mine.at[k], dst_ref=q_theirs.at[k], send_sem=q_ss.at[k], recv_sem=q_rs.at[k], device_id={'sp': partner}, device_id_type=MESH))
        if k % per_grp == 0:
            wait_load(load_uk(k // per_grp))
        emit(q_blk, k, 0)
        sends[k].start()
        if k % per_grp == per_grp - 1:
            flush(c * half_heads + (k // per_grp) * group, 0)

    def their_block(k):
        sends[k].wait_recv()
        if k % per_grp == 0:
            wait_load(load_uk(n_grp // 2 + k // per_grp))
        emit(q_theirs[k], k, 1)
        if k % per_grp == per_grp - 1:
            flush((1 - c) * half_heads + (k // per_grp) * group, 1)

    behind = cfg["behind"]
    for k in range(n_blk):
        own_block(k)
        if k >= behind:
            their_block(k - behind)
    raw_kv = [lo[:, dq_cols:dq_cols + lat_dim // 2], hi[:, dq_cols:dq_cols + lat_dim // 2]]
    mean_sq = sum(jnp.sum(r * r, axis=1, keepdims=True) for r in raw_kv) / lat_dim
    inv = lax.rsqrt(mean_sq + EPS)
    c_kv = jnp.concatenate([r * inv * kv_gain[:, i * (lat_dim // 2):(i + 1) * (lat_dim // 2)] for i, r in enumerate(raw_kv)], axis=1).astype(jnp.bfloat16)
    k_pe = rotate_pair(hi[:, dq_cols + lat_dim // 2:]).astype(jnp.bfloat16)
    kvn_out[:, :lat_dim] = c_kv.astype(f32)
    kvn_out[:, lat_dim:] = k_pe.astype(f32)

    for k in range(n_blk - behind, n_blk):
        their_block(k)
    swap.wait_send()
    for s in sends:
        s.wait_send()


def project(hidden, cache_len, w_dq, q_gain, w_uq, w_dkv, kv_gain, w_uk):
    n_seqs, d_model = hidden.shape
    heads, nope_dim, lat_dim = w_uk.shape
    q_rank = w_dq.shape[1]
    rope_dim = w_dkv.shape[1] - lat_dim
    freqs = [float(f) for f in np.power(ROPE_THETA, -2.0 * np.arange(rope_dim // 2) / rope_dim).astype(np.float32)]
    cfg = dict(n_kt=4, lat_dim=lat_dim, group=16, pitch=n_seqs + 8, in_flight=9, behind=2, freqs=freqs)
    n_k, n_blk = 8, 8
    dq_cols, dkv_cols = q_rank // 2, lat_dim // 2 + rope_dim
    blk = w_uq.shape[1] // 2 // n_blk
    f32, bf16 = jnp.float32, jnp.bfloat16
    at, small = 0, 0.0
    n_small = q_rank + lat_dim + 128
    for piece in (q_gain, kv_gain, cache_len):
        small = small + jnp.pad(piece, (at, n_small - at - piece.size)).astype(f32)
        at += piece.size
    dma = pltpu.SemaphoreType.DMA
    return pl.pallas_call(
        functools.partial(project_kernel, cfg),
        out_shape=(
            jax.ShapeDtypeStruct((n_seqs, heads, lat_dim + 128), bf16),
            jax.ShapeDtypeStruct((n_seqs, lat_dim + 128), f32),
        ),
        in_specs=[VMEM, VMEM, HBM, HBM, HBM, HBM],
        out_specs=(VMEM, VMEM),
        scratch_shapes=[
            pltpu.VMEM((n_k, d_model // n_k, dq_cols), bf16),
            pltpu.VMEM((dkv_cols, d_model), bf16),
            pltpu.VMEM((n_blk, q_rank, blk), bf16),
            pltpu.VMEM((heads, nope_dim, lat_dim), bf16),
            pltpu.VMEM((2, n_seqs, dq_cols + lat_dim // 2 + 128), f32),
            pltpu.VMEM((n_blk, n_seqs, blk), f32),
            pltpu.VMEM((n_blk, n_seqs, blk), f32),
            pltpu.VMEM((2, lat_dim // 128 + 1, cfg["group"] * cfg["pitch"], 128), f32),
            dma((n_k,)), dma((cfg["n_kt"],)), dma((n_blk,)), dma((heads // cfg["group"],)),
            dma, dma, dma((n_blk,)), dma((n_blk,)),
        ],
        compiler_params=pltpu.CompilerParams(collective_id=1, has_side_effects=True, vmem_limit_bytes=48 * 1024 * 1024),
        name="project",
    )(small, hidden, w_dq, w_dkv.T, w_uq, w_uk)


def attend_kernel(cfg, len_ref, q_ref, kvn_ref, ckv_hbm, kpe_hbm, cout_hbm, kout_hbm, terms, kv_new,
                  cbuf, kbuf, peaks, denoms, isem, osem):
    n_seqs, shard_len = ckv_hbm.shape[0], ckv_hbm.shape[1]
    lat_dim = ckv_hbm.shape[2]
    rope_dim = kpe_hbm.shape[1]
    per = terms.shape[2] - 1
    n_buf, lag, chunk = cfg["n_buf"], cfg["lag"], cfg["chunk"]
    base = lax.axis_index('sp') * shard_len

    def copies_in(b, slot):
        return (pltpu.make_async_copy(ckv_hbm.at[b], cbuf.at[slot], isem.at[slot, 0]),
                pltpu.make_async_copy(kpe_hbm.at[b], kbuf.at[slot], isem.at[slot, 1]))

    def copies_out(b, slot):
        return (pltpu.make_async_copy(cbuf.at[slot], cout_hbm.at[b], osem.at[slot, 0]),
                pltpu.make_async_copy(kbuf.at[slot], kout_hbm.at[b], osem.at[slot, 1]))

    for i in range(n_buf - lag):
        for c in copies_in(i, i):
            c.start()
    kv_new[...] = kvn_ref[:, :lat_dim + rope_dim].astype(kv_new.dtype)
    peaks[...] = jnp.zeros_like(peaks)
    denoms[...] = jnp.zeros_like(denoms)

    def step(b, carry):
        slot = lax.rem(b, n_buf)

        @pl.when(b >= lag)
        def _():
            for c in copies_out(b - lag, lax.rem(b - lag + n_buf, n_buf)):
                c.wait()

        ahead = b - lag + n_buf

        @pl.when(ahead < n_seqs)
        def _():
            for c in copies_in(ahead, lax.rem(ahead, n_buf)):
                c.start()

        for c in copies_in(b, slot):
            c.wait()
        last = len_ref[b] - base

        @pl.when((last >= 0) & (last < shard_len))
        def _():
            picked = lax.broadcasted_iota(jnp.int32, kvn_ref.shape, 0) == b
            fresh_row = jnp.sum(jnp.where(picked, kvn_ref[...], 0.0), axis=0, keepdims=True)
            r0 = pl.multiple_of((last // 16) * 16, 16)
            rows = cbuf[slot, pl.ds(r0, 16), :].astype(jnp.float32)
            row = lax.broadcasted_iota(jnp.int32, rows.shape, 0)
            cbuf[slot, pl.ds(r0, 16), :] = jnp.where(row == last - r0, fresh_row[:, :lat_dim], rows).astype(cbuf.dtype)
            c0 = pl.multiple_of((last // 128) * 128, 128)
            cols = kbuf[slot, :, pl.ds(c0, 128)].astype(jnp.float32)
            lane = lax.broadcasted_iota(jnp.int32, cols.shape, 1)
            diag = lane == lax.broadcasted_iota(jnp.int32, cols.shape, 0)
            fresh = jnp.sum(jnp.where(diag, fresh_row[:, lat_dim:], 0.0), axis=1, keepdims=True)
            kbuf[slot, :, pl.ds(c0, 128)] = jnp.where(lane == last - c0, fresh, cols).astype(kbuf.dtype)

        q_lat, q_pe = q_ref[b, :, :lat_dim], q_ref[b, :, lat_dim:lat_dim + rope_dim]
        scores = []
        for t in range(0, shard_len, chunk):
            s = lax.dot_general(q_lat, cbuf[slot, t:t + chunk, :], (((1,), (1,)), ((), ())), preferred_element_type=jnp.float32)
            s = s + jnp.dot(q_pe, kbuf[slot, :, t:t + chunk], preferred_element_type=jnp.float32)
            pos = lax.broadcasted_iota(jnp.int32, (1, chunk), 1) + t
            scores.append(jnp.where(pos <= last, s * cfg["scale"], NEG_FILL))
        peak = functools.reduce(jnp.maximum, [jnp.max(s, axis=1, keepdims=True) for s in scores])
        denom = jnp.zeros_like(peak)
        lat_sum = None
        for k, t in enumerate(range(0, shard_len, chunk)):
            w = jnp.exp(scores[k] - peak)
            denom = denom + jnp.sum(w, axis=1, keepdims=True)
            term = jnp.dot(w.astype(jnp.bfloat16), cbuf[slot, t:t + chunk, :], preferred_element_type=jnp.float32)
            lat_sum = term if lat_sum is None else lat_sum + term
        for c in copies_out(b, slot):
            c.start()
        terms[:, b // per, b % per] = lat_sum.reshape(terms.shape[0], *terms.shape[3:])
        lane = lax.broadcasted_iota(jnp.int32, peaks.shape, 1)
        peaks[...] = jnp.where(lane == b, peak, peaks[...])
        denoms[...] = jnp.where(lane == b, denom, denoms[...])
        return carry

    lax.fori_loop(0, n_seqs, step, 0)
    for part in range(2):
        terms[:, part, per, :, :128] = peaks[...].reshape(terms.shape[0], terms.shape[3], 128)
        terms[:, part, per, :, 128:256] = denoms[...].reshape(terms.shape[0], terms.shape[3], 128)
    for i in range(n_seqs - lag, n_seqs):
        for c in copies_out(i, i % n_buf):
            c.wait()


def attend(q, kvn, cache_len, ckv_blk, kpe_blk_t, n_dev, qk_dim):
    n_seqs, shard_len, lat_dim = ckv_blk.shape
    rope_dim = kpe_blk_t.shape[1]
    n_heads = q.shape[1]
    cfg = dict(n_buf=8, lag=3, chunk=512, scale=qk_dim ** -0.5)
    terms_shape = (n_dev, 2, n_seqs // 2 + 1, n_heads // n_dev, lat_dim)
    return pl.pallas_call(
        functools.partial(attend_kernel, cfg),
        out_shape=(
            jax.ShapeDtypeStruct(ckv_blk.shape, ckv_blk.dtype),
            jax.ShapeDtypeStruct(kpe_blk_t.shape, kpe_blk_t.dtype),
            jax.ShapeDtypeStruct(terms_shape, jnp.float32),
            jax.ShapeDtypeStruct((n_seqs, lat_dim + rope_dim), ckv_blk.dtype),
        ),
        in_specs=[SMEM, VMEM, VMEM, HBM, HBM],
        out_specs=(HBM, HBM, VMEM, VMEM),
        scratch_shapes=[
            pltpu.VMEM((cfg["n_buf"], shard_len, lat_dim), ckv_blk.dtype),
            pltpu.VMEM((cfg["n_buf"], rope_dim, shard_len), kpe_blk_t.dtype),
            pltpu.VMEM((n_heads, 128), jnp.float32),
            pltpu.VMEM((n_heads, 128), jnp.float32),
            pltpu.SemaphoreType.DMA((cfg["n_buf"], 2)),
            pltpu.SemaphoreType.DMA((cfg["n_buf"], 2)),
        ],
        compiler_params=pltpu.CompilerParams(vmem_limit_bytes=36 * 1024 * 1024),
        name="attend",
    )(cache_len, q, kvn, ckv_blk, kpe_blk_t)


def finish_kernel(terms, w_uv, w_out, out_ref, own, pair, from_x, from_y, uv, wo, merged, oheads, psend, precv, isend, irecv, fin, agr, agp,
                  lsem, d_ss, d_rs, x_ss, x_rs, y_ss, y_rs, p_ss, p_rs, i_ss, i_rs, a_ss, a_rs, f_ss, f_rs):
    n_seqs, width = fin.shape
    heads = uv.shape[0]
    depth = wo.shape[0]
    me = lax.axis_index('sp')
    y, x, c = me // 4, (me // 2) % 2, me % 2

    def device(q, jc):
        return ((y + q // 2) % 2) * 4 + ((x + q % 2) % 2) * 2 + (c + jc) % 2

    def send(src, dst, ss, rs, dev):
        return pltpu.make_async_remote_copy(src_ref=src, dst_ref=dst, send_sem=ss, recv_sem=rs, device_id={'sp': dev}, device_id_type=MESH)

    load_uv = pltpu.make_async_copy(w_uv.at[pl.ds(me * heads, heads)], uv, lsem.at[0])
    load_wo = pltpu.make_async_copy(w_out.at[pl.ds(me * depth, depth)], wo, lsem.at[1])
    order = ((3, 0), (3, 1), (1, 0), (2, 1), (2, 0), (1, 1), (0, 0), (0, 1))
    per = n_seqs // 2
    load_uv.start()

    others = ((0, 1), (1, 0), (2, 0), (3, 0))
    barrier = pltpu.get_barrier_semaphore()
    for q, jc in others:
        pl.semaphore_signal(barrier, inc=1, device_id={'sp': device(q, jc)}, device_id_type=MESH)
    pl.semaphore_wait(barrier, len(others))

    d_sends = {(q, h): send(terms.at[device(q, 1), h], pair.at[q, h], d_ss.at[q, h], d_rs.at[q, h], device(0, 1)) for q, h in order}
    for k in order:
        d_sends[k].start()

    def merge(dst, src, h, first=None):
        base = dst if first is None else first
        old, new = base[per, :, :128], src[per, :, :128]
        peak = jnp.maximum(old, new)
        f_old, f_new = jnp.exp(old - peak), jnp.exp(new - peak)
        dst[per, :, :128] = peak
        dst[per, :, 128:256] = f_old * base[per, :, 128:256] + f_new * src[per, :, 128:256]
        for i in range(per):
            b = h * per + i
            dst[i] = f_old[:, b:b + 1] * base[i] + f_new[:, b:b + 1] * src[i]

    def merge_pair(q, h):
        d_sends[q, h].wait_recv()
        merge(own.at[q, h], pair.at[q, h], h, terms.at[device(q, 0), h])

    x_dev, y_dev = device(1, 0), device(2, 0)

    class Both:
        def __init__(self, src, dst, ss, rs, dev):
            body, tail = pl.ds(0, per), pl.ds(0, 256)
            self.copies = (send(src.at[body], dst.at[body], ss.at[0], rs.at[0], dev), send(src.at[per, :, tail], dst.at[per, :, tail], ss.at[1], rs.at[1], dev))

        def start(self):
            for copy in self.copies:
                copy.start()

        def wait_recv(self):
            for copy in self.copies:
                copy.wait_recv()

        def wait_send(self):
            for copy in self.copies:
                copy.wait_send()

    x_sends = [Both(own.at[k], from_x.at[i], x_ss.at[i], x_rs.at[i], x_dev) for i, k in enumerate(((3, 0), (1, 0), (1, 1)))]
    y_sends = [Both(own.at[k], from_y.at[i], y_ss.at[i], y_rs.at[i], y_dev) for i, k in enumerate(((3, 1), (2, 1), (2, 0)))]
    merge_pair(3, 0)
    merge_pair(3, 1)
    x_sends[0].start()
    merge_pair(1, 0)
    y_sends[0].start()
    merge_pair(2, 1)
    x_sends[1].start()
    merge_pair(2, 0)
    y_sends[1].start()
    merge_pair(1, 1)
    merge_pair(0, 0)
    merge_pair(0, 1)
    load_wo.start()
    x_sends[0].wait_recv()
    merge(own.at[2, 0], from_x.at[0], 0)
    y_sends[0].wait_recv()
    merge(own.at[1, 1], from_y.at[0], 1)
    y_sends[2].start()
    x_sends[2].start()
    x_sends[1].wait_recv()
    merge(own.at[0, 0], from_x.at[1], 0)
    y_sends[1].wait_recv()
    merge(own.at[0, 1], from_y.at[1], 1)
    y_sends[2].wait_recv()
    merge(own.at[0, 0], from_y.at[2], 0)
    x_sends[2].wait_recv()
    merge(own.at[0, 1], from_x.at[2], 1)
    for h in range(2):
        inv = 1.0 / own[0, h, per, :, 128:256]
        for i in range(per):
            b = h * per + i
            acc = inv[:, b:b + 1] * own[0, h, i]
            for k in range(merged.shape[0]):
                merged[k, b * heads:(b + 1) * heads, :] = acc[:, k * 128:(k + 1) * 128]
    load_uv.wait()
    for h in range(heads):
        o_lat = jnp.concatenate([merged[k, pl.ds(h, n_seqs, stride=heads), :] for k in range(merged.shape[0])], axis=1).astype(jnp.bfloat16)
        o_h = lax.dot_general(o_lat, uv[h], (((1,), (1,)), ((), ())), preferred_element_type=jnp.float32)
        oheads[:, h * o_h.shape[1]:(h + 1) * o_h.shape[1]] = o_h.astype(jnp.bfloat16)
    load_wo.wait()

    def columns(dev, part):
        at, size = parts[part]
        return pl.ds(pl.multiple_of(dev * width + at, 128), size)

    def partial_out(dev, part):
        return jnp.dot(oheads[...], wo[:, columns(dev, part)], preferred_element_type=jnp.float32)

    parts = ((0, width // 256 * 128), (width // 256 * 128, width - width // 256 * 128))
    far = (3, 1, 2)
    p_sends, i_sends, a_sends, f_sends = {}, {}, {}, {}

    def start(waiting):
        while waiting:
            waiting.pop().start()

    def put(ref, part, value):
        ref[:, parts[part][0]:sum(parts[part])] = value

    def get(ref, part):
        return ref[:, parts[part][0]:sum(parts[part])]

    def cut(ref, part):
        return ref.at[:, pl.ds(*parts[part])]

    mine = []
    waiting = []
    for part in range(2):
        for q in far + (0,):
            put(psend.at[q], part, partial_out(device(q, 1), part))
            start(waiting)
            p_sends[q, part] = send(cut(psend.at[q], part), cut(precv.at[q], part), p_ss.at[q, part], p_rs.at[q, part], device(0, 1))
            waiting.append(p_sends[q, part])
        for q in far + (0,):
            value = partial_out(device(q, 0), part)
            start(waiting)
            p_sends[q, part].wait_recv()
            value = value + get(precv.at[q], part)
            if q:
                put(isend.at[q - 1], part, value)
                i_sends[q, part] = send(cut(isend.at[q - 1], part), cut(irecv.at[q - 1], part), i_ss.at[q - 1, part], i_rs.at[q - 1, part], device(q, 0))
                waiting.append(i_sends[q, part])
            else:
                mine.append(value)
        start(waiting)
    for part in range(2):
        for q in far:
            i_sends[q, part].wait_recv()
        result = mine[part] + get(irecv.at[0], part) + get(irecv.at[1], part) + get(irecv.at[2], part)
        put(fin, part, result)
        out_ref[:, columns(me, part)] = result
        for q in far:
            a_sends[q, part] = send(cut(fin, part), cut(agr.at[q - 1], part), a_ss.at[q - 1, part], a_rs.at[q - 1, part], device(q, 0))
            a_sends[q, part].start()
        f_sends[0, part] = send(cut(fin, part), cut(agp.at[0], part), f_ss.at[0, part], f_rs.at[0, part], device(0, 1))
        f_sends[0, part].start()
    for part in range(2):
        for q in (1, 2, 3):
            a_sends[q, part].wait_recv()
            f_sends[q, part] = send(cut(agr.at[q - 1], part), cut(agp.at[q], part), f_ss.at[q, part], f_rs.at[q, part], device(0, 1))
            f_sends[q, part].start()
            out_ref[:, columns(device(q, 0), part)] = get(agr.at[q - 1], part)
    for part in range(2):
        for q in range(4):
            f_sends[q, part].wait_recv()
            out_ref[:, columns(device(q, 1), part)] = get(agp.at[q], part)
    for s in list(d_sends.values()) + x_sends + y_sends + list(p_sends.values()) + list(i_sends.values()) + list(a_sends.values()) + list(f_sends.values()):
        s.wait_send()


def finish(terms, w_uv, w_out):
    n_dev, _, rows, heads, lat_dim = terms.shape
    n_seqs = 2 * (rows - 1)
    d_model = w_out.shape[1]
    depth = w_out.shape[0] // n_dev
    width = d_model // n_dev
    f32 = jnp.float32
    return pl.pallas_call(
        finish_kernel,
        out_shape=jax.ShapeDtypeStruct((n_seqs, d_model), f32),
        in_specs=[VMEM, HBM, HBM],
        out_specs=VMEM,
        scratch_shapes=[
            pltpu.VMEM((4, 2, rows, heads, lat_dim), f32),
            pltpu.VMEM((4, 2, rows, heads, lat_dim), f32),
            pltpu.VMEM((3, rows, heads, lat_dim), f32),
            pltpu.VMEM((3, rows, heads, lat_dim), f32),
            pltpu.VMEM((heads,) + w_uv.shape[1:], w_uv.dtype),
            pltpu.VMEM((depth, d_model), w_out.dtype),
            pltpu.VMEM((lat_dim // 128, n_seqs * heads, 128), f32),
            pltpu.VMEM((n_seqs, depth), jnp.bfloat16),
            pltpu.VMEM((4, n_seqs, width), f32),
            pltpu.VMEM((4, n_seqs, width), f32),
            pltpu.VMEM((3, n_seqs, width), f32),
            pltpu.VMEM((3, n_seqs, width), f32),
            pltpu.VMEM((n_seqs, width), f32),
            pltpu.VMEM((3, n_seqs, width), f32),
            pltpu.VMEM((4, n_seqs, width), f32),
            pltpu.SemaphoreType.DMA((2,)),
            pltpu.SemaphoreType.DMA((4, 2)),
            pltpu.SemaphoreType.DMA((4, 2)),
            pltpu.SemaphoreType.DMA((3, 2)),
            pltpu.SemaphoreType.DMA((3, 2)),
            pltpu.SemaphoreType.DMA((3, 2)),
            pltpu.SemaphoreType.DMA((3, 2)),
            pltpu.SemaphoreType.DMA((4, 2)),
            pltpu.SemaphoreType.DMA((4, 2)),
            pltpu.SemaphoreType.DMA((3, 2)),
            pltpu.SemaphoreType.DMA((3, 2)),
            pltpu.SemaphoreType.DMA((3, 2)),
            pltpu.SemaphoreType.DMA((3, 2)),
            pltpu.SemaphoreType.DMA((4, 2)),
            pltpu.SemaphoreType.DMA((4, 2)),
        ],
        compiler_params=pltpu.CompilerParams(collective_id=0, has_side_effects=True, vmem_limit_bytes=48 * 1024 * 1024),
        name="finish",
    )(terms, w_uv, w_out)


def solution(mesh):
    n_dev = mesh.shape['sp']

    def local_step(hidden, ckv_blk, kpe_blk, cache_len, w_dq, q_gain, w_uq, w_dkv, kv_gain, w_uk, w_uv, w_out):
        q, kvn = project(hidden, cache_len, w_dq, q_gain, w_uq, w_dkv, kv_gain, w_uk)
        qk_dim = w_uk.shape[1] + kpe_blk.shape[2]
        ckv_out, kpe_out_t, terms, kv_new = attend(q, kvn, cache_len, ckv_blk, jnp.swapaxes(kpe_blk, 1, 2), n_dev, qk_dim)
        out = finish(terms, w_uv, w_out).astype(jnp.bfloat16)
        return out, ckv_out, jnp.swapaxes(kpe_out_t, 1, 2), kv_new

    cache_spec = P('dp', 'sp', None)
    return jax.shard_map(local_step, mesh=mesh, in_specs=(P('dp', None), cache_spec, cache_spec, P('dp'), P(), P(), P(), P(), P(), P(), P(), P()), out_specs=(P('dp', None), cache_spec, cache_spec, P('dp', None)), check_vma=False)
```
